64 devices in a mesh: rep: 8 (over x, y, core), dp: 8 (over z).
Axes of the slice: x: 2, y: 2, z: 8, core: 2. Of those that a mesh axis runs over, the one named last changes fastest.
The devices are a block of a 4x4x8 slice.
Arguments:
- x: bfloat16 [64, 4096, 512], P(('rep', 'dp')), parts along dimension 0
- dy: bfloat16 [64, 4096, 512], P(('rep', 'dp')), parts along dimension 0
- w_gate: bfloat16 [2, 512, 2048], replicated
- w_up: bfloat16 [2, 512, 2048], replicated
- w_down: bfloat16 [2, 2048, 512], replicated
- m_w_gate: float32 [2, 512, 2048], P(None, 'dp')
- m_w_up: float32 [2, 512, 2048], P(None, 'dp')
- m_w_down: float32 [2, 2048, 512], P(None, 'dp')
- v_w_gate: float32 [2, 512, 2048], P(None, 'dp')
- v_w_up: float32 [2, 512, 2048], P(None, 'dp')
- v_w_down: float32 [2, 2048, 512], P(None, 'dp')
Outputs:
- output 1: bfloat16 [16, 512, 2048], P('rep'), parts along dimension 0
- output 2: bfloat16 [16, 512, 2048], P('rep'), parts along dimension 0
- output 3: bfloat16 [16, 2048, 512], P('rep'), parts along dimension 0
- output 4: float32 [16, 512, 2048], P('rep', 'dp'), parts along dimension 0
- output 5: float32 [16, 512, 2048], P('rep', 'dp'), parts along dimension 0
- output 6: float32 [16, 2048, 512], P('rep', 'dp'), parts along dimension 0
- output 7: float32 [16, 512, 2048], P('rep', 'dp'), parts along dimension 0
- output 8: float32 [16, 512, 2048], P('rep', 'dp'), parts along dimension 0
- output 9: float32 [16, 2048, 512], P('rep', 'dp'), parts along dimension 0
There are 8 independent parts. The reference program is written for one: setup_inputs(seed, part) draws one part's arguments, and reference() takes and returns one part's arrays. A program takes and returns all parts, laid end to end along the dimension named above; an argument that names none is the same for every part.
All inputs are finite; a program needn't handle non-finite values.
Results may differ from the reference program's by a relative error of at most 0.022.
Values are sent between devices in bfloat16 or wider.
A program may use at most 768 MiB of HBM per device.

```python
import jax
import jax.numpy as jnp
from jax import lax

SEQUENCES = 8
TOKENS = 4096
D = 512
FF = 2048
LAYERS = 2
NAMES = ("w_gate", "w_up", "w_down")
SHAPES = {"w_gate": (LAYERS, D, FF), "w_up": (LAYERS, D, FF), "w_down": (LAYERS, FF, D)}


def bump(key, n, height):
    away = (jnp.arange(n, dtype=jnp.int32) - jax.random.randint(key, (), 0, n, jnp.int32)) % n
    return jnp.where(away < n // 8, height, 1.0)


def together(key, own, strength):
    shared = jax.random.normal(key, own.shape[1:], jnp.float32)
    return (own + strength * shared) * lax.rsqrt(1 + strength * strength)


def setup_inputs(seed: int = 0, part: int = 0) -> dict:
    kx, kdy, ka, kb, kz, kf, kh, kl, *keys = jax.random.split(jax.random.key(seed), 8 + 3 * len(NAMES))
    kx, kdy, ka, kb = (jax.random.fold_in(k, part) for k in (kx, kdy, ka, kb))
    kw, km, kv = (keys[i::3] for i in range(3))
    shape = (SEQUENCES, TOKENS, D)
    much_x, much_dy = jax.random.uniform(kz, (2,), jnp.float32, 0.0, 1.0)
    loud = 2.0 ** jax.random.uniform(jax.random.fold_in(kz, 1), (), jnp.float32, -1.0, 2.0)
    layers = 2.0 ** jax.random.uniform(kl, (LAYERS, 1, 1), jnp.float32, -1.0, 1.0)
    x = together(ka, jax.random.normal(kx, shape, jnp.float32), much_x) * bump(kf, D, 4.0)
    dy = together(kb, jax.random.normal(kdy, shape, jnp.float32), much_dy)
    drawn = {"x": x.astype(jnp.bfloat16), "dy": (loud * dy * (SEQUENCES * TOKENS) ** -0.5).astype(jnp.bfloat16)}
    for key, name in zip(kw, NAMES, strict=True):
        w = jax.random.normal(key, SHAPES[name], jnp.float32) * SHAPES[name][1] ** -0.5
        drawn[name] = (w * {"w_gate": 1.0, "w_up": bump(kh, FF, 4.0), "w_down": layers}[name]).astype(jnp.bfloat16)
    for key, name in zip(km, NAMES, strict=True):
        drawn[f"m_{name}"] = 0.1 * jax.random.normal(key, SHAPES[name], jnp.float32)
    for key, name in zip(kv, NAMES, strict=True):
        drawn[f"v_{name}"] = jax.random.uniform(key, SHAPES[name], jnp.float32, 0.005, 0.015)
    return drawn


def matmul(a, w):
    return jnp.dot(a, w, preferred_element_type=jnp.float32).astype(jnp.bfloat16)


def normed(h):
    wide = h.astype(jnp.float32)
    scale = lax.rsqrt(jnp.mean(wide**2, -1, keepdims=True) + 1e-6)
    return (wide * scale).astype(jnp.bfloat16)


def layer(h, w):
    a = normed(h)
    gate = jnp.dot(a, w["w_gate"], preferred_element_type=jnp.float32)
    up = jnp.dot(a, w["w_up"], preferred_element_type=jnp.float32)
    return h + matmul((jax.nn.silu(gate) * up).astype(jnp.bfloat16), w["w_down"])


def adamw(w, m, v, g):
    m = 0.9 * m + 0.1 * g
    v = 0.95 * v + 0.05 * g * g
    step = m * lax.rsqrt(v + 1e-8) + 0.1 * w
    return (w - 0.02 * step).astype(jnp.bfloat16), m, v


def clipped(gradients, sum_of_squares, count):
    factor = jnp.minimum(1.0, 0.5 * lax.rsqrt(sum_of_squares / count + 1e-30))
    return [g * factor for g in gradients]


def stack(weights, h):
    return lax.scan(lambda h, w: (layer(h, w), None), h, weights)[0]


def reference(x, dy, w_gate, w_up, w_down, m_w_gate, m_w_up, m_w_down, v_w_gate, v_w_up, v_w_down):
    weights = dict(zip(NAMES, (w_gate, w_up, w_down), strict=True))

    def take(so_far, sequence):
        h, by_y = sequence
        _, back = jax.vjp(lambda w: stack(w, h), weights)
        return jax.tree.map(lambda total, term: total + term.astype(jnp.float32), so_far, back(by_y)[0]), None

    none_yet = {name: jnp.zeros(w.shape, jnp.float32) for name, w in weights.items()}
    by_weights, _ = lax.scan(take, none_yet, (x, dy))
    gradients = [by_weights[name].astype(jnp.bfloat16).astype(jnp.float32) for name in NAMES]
    gradients = clipped(gradients, sum(jnp.sum(g * g) for g in gradients), sum(g.size for g in gradients))
    new = [
        adamw(w.astype(jnp.float32), m, v, g)
        for w, m, v, g in zip((w_gate, w_up, w_down), (m_w_gate, m_w_up, m_w_down), (v_w_gate, v_w_up, v_w_down), gradients, strict=True)
    ]
    return tuple(one[which] for which in range(3) for one in new)
```

```python
import functools

import jax
import jax.numpy as jnp
from jax import lax
from jax.experimental import pallas as pl
from jax.experimental.pallas import tpu as pltpu
from jax.sharding import PartitionSpec as P

F32, BF16 = jnp.float32, jnp.bfloat16
TT = 512
LB = 128
VMEM_LIMIT = 67_043_328


def dot(a, b):
    return jnp.dot(a, b, preferred_element_type=F32)


def rms(wide):
    return lax.rsqrt(jnp.mean(wide * wide, -1, keepdims=True) + 1e-6)


def sigmoid(g):
    return 0.5 * jnp.tanh(0.5 * g) + 0.5


def grad_kernel(cfg, x_h, dy_h, wg_h, wu_h, wd_h, gg_h, gu_h, gd_h, a1_h, a1t_h,
                w1, w1d, w2, w2d, wgut, wdt, a, at, h1, dy, dyt, da, xb, hid, pg, pd, ob, od,
                sem_w, sem_x, sem_dy, sem_a, sem_at, sem_o):
    nt, nc, n = cfg
    half = nc // 2
    fc = 2 * LB

    def blocks(j):
        c = 2 * (j % half) + j // half
        return c, c + nc

    for layer, (wgu, wdn) in enumerate(((w1, w1d), (w2, w2d))):
        for j in range(nc):
            for s, b in enumerate(blocks(j)):
                cols, rows = pl.ds(b * LB, LB), pl.ds(s * LB, LB)
                pltpu.make_async_copy(wg_h.at[layer, :, cols], wgu.at[j, :, rows], sem_w.at[layer, 0]).start()
                pltpu.make_async_copy(wu_h.at[layer, :, cols], wgu.at[j, :, pl.ds(fc + s * LB, LB)], sem_w.at[layer, 0]).start()
                pltpu.make_async_copy(wd_h.at[layer, cols, :], wdn.at[j * 2 + s], sem_w.at[layer, 1]).start()

    def x_copy(t):
        return pltpu.make_async_copy(x_h.at[0, pl.ds(t * TT, TT), :], xb.at[t % 2], sem_x.at[t % 2])

    def dy_copy(t):
        return pltpu.make_async_copy(dy_h.at[0, pl.ds(t * TT, TT), :], dy.at[t], sem_dy.at[t])

    x_copy(0).start()
    for t in range(nt):
        dy_copy(t).start()
    pltpu.make_async_copy(w1, w1, sem_w.at[0, 0]).wait()
    pltpu.make_async_copy(w1d, w1d, sem_w.at[0, 1]).wait()

    @pl.loop(0, nt)
    def _(t):
        x_copy(t).wait()

        @pl.when(t + 1 < nt)
        def _():
            x_copy(t + 1).start()

        wide = xb[t % 2].astype(F32)
        a1 = (wide * rms(wide)).astype(BF16)
        a[t] = a1
        at[t] = a1.T
        pltpu.make_async_copy(a.at[t], a1_h.at[t], sem_a.at[t]).start()
        pltpu.make_async_copy(at.at[t], a1t_h.at[t], sem_at.at[t]).start()
        for j in range(nc):
            gu = dot(a1, w1[j])
            g, u = gu[:, :fc], gu[:, fc:]
            hid[:, j * fc:(j + 1) * fc] = (g * sigmoid(g) * u).astype(BF16)
        y = dot(hid[...], w1d[...].reshape(2 * nc * LB, -1))
        h1[t] = (xb[t % 2].astype(F32) + y.astype(BF16).astype(F32)).astype(BF16)
        da[t] = jnp.zeros(da.shape[1:], F32)
        dy_copy(t).wait()
        dyt[t] = dy[t].T

    pltpu.make_async_copy(w2, w2, sem_w.at[1, 0]).wait()
    pltpu.make_async_copy(w2d, w2d, sem_w.at[1, 1]).wait()

    @pl.loop(0, nt)
    def _(t):
        pltpu.make_async_copy(a.at[t], a1_h.at[t], sem_a.at[t]).wait()
        pltpu.make_async_copy(at.at[t], a1t_h.at[t], sem_at.at[t]).wait()
        wide = h1[t].astype(F32)
        a2 = (wide * rms(wide)).astype(BF16)
        a[t] = a2
        at[t] = a2.T

    def out_copies(layer, j, s):
        copies = []
        for i, b in enumerate(blocks(j)):
            cols = pl.ds(b * LB, LB)
            copies += [
                pltpu.make_async_copy(ob.at[s, :, pl.ds(i * LB, LB)], gg_h.at[layer, :, cols], sem_o.at[s, 3 * i]),
                pltpu.make_async_copy(ob.at[s, :, pl.ds(fc + i * LB, LB)], gu_h.at[layer, :, cols], sem_o.at[s, 3 * i + 1]),
                pltpu.make_async_copy(od.at[s, pl.ds(i * LB, LB), :], gd_h.at[layer, cols, :], sem_o.at[s, 3 * i + 2]),
            ]
        return copies

    def chunk(layer, j, wgu, wdn, into_states):
        s = j % 2
        wd = jnp.concatenate([wdn[2 * j], wdn[2 * j + 1]], 0)
        wdt[...] = wd.T
        if into_states:
            wgut[...] = wgu[j].T
        pg[...] = jnp.zeros_like(pg)
        pd[...] = jnp.zeros_like(pd)

        @pl.loop(0, nt)
        def _(t):
            gu = dot(a[t], wgu[j])
            dh = dot(dy[t], wdt[...]).astype(BF16).astype(F32)
            g, u = gu[:, :fc], gu[:, fc:]
            sig = sigmoid(g)
            silu = g * sig
            hd = (silu * u).astype(BF16)
            dgu = jnp.concatenate([(dh * u * (sig + silu * (1 - sig))).astype(BF16), (dh * silu).astype(BF16)], 1)
            pg[...] += dot(at[t], dgu)
            pd[...] += dot(dyt[t], hd)
            if into_states:
                da[t] += dot(dgu, wgut[...])

        @pl.when(j >= 2)
        def _():
            for copy in out_copies(layer, j, s):
                copy.wait()

        ob[s] = pg[...].astype(BF16)
        od[s] = pd[...].T.astype(BF16)
        for copy in out_copies(layer, j, s):
            copy.start()

    @pl.loop(0, nc)
    def _(j):
        chunk(1, j, w2, w2d, True)

    @pl.loop(0, nt)
    def _(t):
        copies = (pltpu.make_async_copy(a1_h.at[t], a.at[t], sem_a.at[t]), pltpu.make_async_copy(a1t_h.at[t], at.at[t], sem_at.at[t]))
        for copy in copies:
            copy.start()
        wide = h1[t].astype(F32)
        r = rms(wide)
        da_t = da[t].astype(BF16).astype(F32)
        dn = da_t * r - wide * (r * r * r * jnp.mean(da_t * wide, -1, keepdims=True))
        dh1 = (dy[t].astype(F32) + dn).astype(BF16)
        dy[t] = dh1
        dyt[t] = dh1.T
        for copy in copies:
            copy.wait()

    for s in range(2):
        for copy in out_copies(1, s, s):
            copy.wait()

    @pl.loop(0, nc)
    def _(j):
        chunk(0, j, w1, w1d, False)

    for s in range(2):
        for copy in out_copies(0, s, s):
            copy.wait()


def gradients_of(x, dy, wg, wu, wd, n):
    tokens, d = x.shape[1:]
    layers, _, f = wg.shape
    nt, nc = tokens // TT, f // (2 * LB)
    fc = 2 * LB
    hbm = pl.BlockSpec(memory_space=pl.ANY)
    shapes = [jax.ShapeDtypeStruct(wg.shape, BF16), jax.ShapeDtypeStruct(wu.shape, BF16), jax.ShapeDtypeStruct(wd.shape, BF16),
              jax.ShapeDtypeStruct((nt, TT, d), BF16), jax.ShapeDtypeStruct((nt, d, TT), BF16)]
    v = pltpu.VMEM
    dma = pltpu.SemaphoreType.DMA
    scratch = [
        v((nc, d, 2 * fc), BF16), v((2 * nc, LB, d), BF16), v((nc, d, 2 * fc), BF16), v((2 * nc, LB, d), BF16),
        v((2 * fc, d), BF16), v((d, fc), BF16),
        v((nt, TT, d), BF16), v((nt, d, TT), BF16), v((nt, TT, d), BF16), v((nt, TT, d), BF16), v((nt, d, TT), BF16), v((nt, TT, d), F32),
        v((2, TT, d), BF16), v((TT, f), BF16), v((d, 2 * fc), F32), v((d, fc), F32), v((2, d, 2 * fc), BF16), v((2, fc, d), BF16),
        dma((2, 2)), dma((2,)), dma((nt,)), dma((nt,)), dma((nt,)), dma((2, 6)),
    ]
    return pl.pallas_call(
        functools.partial(grad_kernel, (nt, nc, n)),
        name="gradients",
        out_shape=shapes,
        in_specs=[hbm] * 5,
        out_specs=[hbm] * 5,
        scratch_shapes=scratch,
        compiler_params=pltpu.CompilerParams(vmem_limit_bytes=VMEM_LIMIT),
    )(x, dy, wg, wu, wd)[:3]


def adamw(w, m, v, g):
    m = 0.9 * m + 0.1 * g
    v = 0.95 * v + 0.05 * g * g
    step = m * lax.rsqrt(v + 1e-8) + 0.1 * w
    return (w - 0.02 * step).astype(BF16), m, v


def solution(mesh):
    n = mesh.shape["dp"]

    def step(x, dy, *arrays):
        weights, m, v = (arrays[i:i + 3] for i in (0, 3, 6))
        terms = gradients_of(x, dy, *weights, n)
        g = [lax.psum_scatter(t, "dp", scatter_dimension=1, tiled=True).astype(F32) for t in terms]
        count = sum(t.size for t in terms)
        total = lax.psum(sum(jnp.sum(t * t) for t in g), "dp")
        factor = jnp.minimum(1.0, 0.5 * lax.rsqrt(total / count + 1e-30))
        me = lax.axis_index("dp")
        new = []
        for w, mm, vv, gg in zip(weights, m, v, g, strict=True):
            rows = gg.shape[1]
            own = lax.dynamic_slice_in_dim(w, me * rows, rows, 1).astype(F32)
            wn, mn, vn = adamw(own, mm, vv, gg * factor)
            new.append((lax.all_gather(wn, "dp", axis=1, tiled=True), mn, vn))
        return tuple(one[which] for which in range(3) for one in new)

    seq, rows = P(("rep", "dp"), None, None), P(None, "dp", None)
    return jax.shard_map(
        step,
        mesh=mesh,
        in_specs=(seq, seq) + (P(),) * 3 + (rows,) * 6,
        out_specs=(P("rep"),) * 3 + (P("rep", "dp"),) * 6,
        check_vma=False,
    )
```

```python
import functools

import jax
import jax.numpy as jnp
from jax import lax
from jax.experimental import pallas as pl
from jax.experimental.pallas import tpu as pltpu
from jax.sharding import PartitionSpec as P

F32, BF16 = jnp.float32, jnp.bfloat16
MESH = pl.DeviceIdType.MESH
TT = 512
LB = 128
FC = 2 * LB
UNITS_HELD = 5
VMEM_LIMIT = 67_043_328


def dot(a, b):
    return jnp.dot(a, b, preferred_element_type=F32)


def rms(wide):
    return lax.rsqrt(jnp.mean(wide * wide, -1, keepdims=True) + 1e-6)


def sigmoid(g):
    return 0.5 * jnp.tanh(0.5 * g) + 0.5


def grad_kernel(nt, nc, n, x_h, dy_h, wg_h, wu_h, wd_h, og_h, ou_h, od_h, tot_h, a1_h, a1t_h,
                w1, w1d, w2, w2d, wgut, wdt, a, at, h1, dy, dyt, da, xb, hid, hd0, hd1, dgu0, dgu1,
                pg, pd, rg, rd, sg, sd, og, ou, od, ss, tots,
                sem_w, sem_x, sem_dy, sem_a, sem_at, sem_o, rg_sem, rd_sem, sg_sem, sd_sem, ts_sem, tr_sem):
    half, far = nc // 2, n // 2
    units = 2 * nc
    rows = pg.shape[1] // n
    hds, dgus = (hd0, hd1), (dgu0, dgu1)
    me = lax.axis_index("dp")
    around = [lax.rem(me + k, n) for k in range(n)]
    towards = (around[1], around[n - 1])

    barrier = pltpu.get_barrier_semaphore()
    for k in range(1, n):
        pl.semaphore_signal(barrier, inc=1, device_id={"dp": around[k]}, device_id_type=MESH)

    def block(j):
        return 2 * lax.rem(j, half) + j // half

    for layer, (wgu, wdn) in enumerate(((w1, w1d), (w2, w2d))):
        for j in range(nc):
            for s in range(2):
                cols = pl.ds((2 * (j % half) + j // half + s * nc) * LB, LB)
                pltpu.make_async_copy(wg_h.at[layer, :, cols], wgu.at[j, :, pl.ds(s * LB, LB)], sem_w.at[layer, 0]).start()
                pltpu.make_async_copy(wu_h.at[layer, :, cols], wgu.at[j, :, pl.ds(FC + s * LB, LB)], sem_w.at[layer, 0]).start()
                pltpu.make_async_copy(wd_h.at[layer, cols, :], wdn.at[j * 2 + s], sem_w.at[layer, 1]).start()

    def x_copy(t):
        s = lax.rem(t, 3)
        return pltpu.make_async_copy(x_h.at[0, pl.ds(t * TT, TT), :], xb.at[s], sem_x.at[s])

    def dy_copy(t):
        return pltpu.make_async_copy(dy_h.at[0, pl.ds(t * TT, TT), :], dy.at[t], sem_dy.at[t])

    def a_copies(t, out):
        pairs = ((a.at[t], a1_h.at[t], sem_a.at[t]), (at.at[t], a1t_h.at[t], sem_at.at[t]))
        return [pltpu.make_async_copy(*((v, h) if out else (h, v)), s) for v, h, s in pairs]

    x_copy(0).start()
    for t in range(nt):
        dy_copy(t).start()
    pltpu.make_async_copy(w1, w1, sem_w.at[0, 0]).wait()
    pltpu.make_async_copy(w1d, w1d, sem_w.at[0, 1]).wait()
    ss[...] = jnp.zeros_like(ss)

    def forward_back(t):
        y = dot(hid[...], w1d[...].reshape(2 * nc * LB, -1))
        h1[t] = (xb[lax.rem(t, 3)].astype(F32) + y.astype(BF16).astype(F32)).astype(BF16)
        da[t] = jnp.zeros(da.shape[1:], F32)
        dyt[t] = dy[t].T

    @pl.loop(0, nt)
    def _(t):
        before = jnp.maximum(t - 1, 0)
        x_copy(t).wait()
        dy_copy(t).wait()

        @pl.when(t + 1 < nt)
        def _():
            x_copy(t + 1).start()

        forward_back(before)
        wide = xb[lax.rem(t, 3)].astype(F32)
        a1 = (wide * rms(wide)).astype(BF16)
        a[t] = a1
        at[t] = a1.T
        for j in range(nc):
            gu = dot(a1, w1[j])
            g, u = gu[:, :FC], gu[:, FC:]
            hid[:, j * FC:(j + 1) * FC] = (g * sigmoid(g) * u).astype(BF16)
        for copy in a_copies(t, True):
            copy.start()

    forward_back(nt - 1)
    pltpu.make_async_copy(w2, w2, sem_w.at[1, 0]).wait()
    pltpu.make_async_copy(w2d, w2d, sem_w.at[1, 1]).wait()

    @pl.loop(0, nt)
    def _(t):
        for copy in a_copies(t, True):
            copy.wait()
        wide = h1[t].astype(F32)
        a2 = (wide * rms(wide)).astype(BF16)
        a[t] = a2
        at[t] = a2.T

    def g_copy(u, s, way, both):
        part = (lambda ref: ref) if both else (lambda ref: ref.at[way])
        return pltpu.make_async_remote_copy(
            part(sg.at[way, s]), part(rg.at[way, lax.rem(u, 2), s]), sg_sem.at[way, s], rg_sem.at[way, lax.rem(u, 2), s],
            device_id={"dp": towards[way]}, device_id_type=MESH)

    def d_copy(j, way, both):
        k = lax.rem(j, far)
        part = (lambda ref: ref) if both else (lambda ref: ref.at[way])
        return pltpu.make_async_remote_copy(
            part(sd.at[way, k]), part(rd.at[way, k]), sd_sem.at[way, k], rd_sem.at[way, k],
            device_id={"dp": towards[way]}, device_id_type=MESH)

    def relay(u, s):
        j, slot, old = lax.rem(u, nc), lax.rem(u, UNITS_HELD), lax.rem(u, 2)
        for way in range(2):
            e = around[far - s] if way == 0 else around[n - far + s]

            @pl.when(u > 0)
            def _():
                g_copy(u - 1, s, way, s > 0).wait_send()

            if s > 0:
                g_copy(u, s - 1, way, s > 1).wait_recv()
            for h in range(2):
                if s == 0 and h != way:
                    continue
                own = pg[slot, pl.ds(pl.multiple_of(e * rows, rows), rows), h * FC:(h + 1) * FC]
                if s > 1 or (s == 1 and h == way):
                    own += rg[way, old, s - 1, h].astype(F32)
                sg[way, s, h] = own.astype(BF16)
            g_copy(u, s, way, s > 0).start()

            @pl.when(lax.rem(e, far) == lax.rem(j, far))
            def _():
                k = lax.rem(j, far)

                @pl.when(u >= far)
                def _():
                    d_copy(j, way, s > 0).wait_send()

                if s > 0:
                    d_copy(j, way, s > 1).wait_recv()
                tall = pd.shape[2] // 2
                for h in range(2):
                    if s == 0 and h != way:
                        continue
                    own = pd[slot, e // far, h * tall:(h + 1) * tall, :]
                    if s > 1 or (s == 1 and h == way):
                        own += rd[way, k, h].astype(F32)
                    sd[way, k, h] = own.astype(BF16)
                d_copy(j, way, s > 0).start()

    def square(g):
        wide = g.astype(F32)
        ss[...] += jnp.sum((wide * wide).reshape(-1, *ss.shape), 0)

    def arrive(u):
        j, slot, old, layer = lax.rem(u, nc), lax.rem(u, UNITS_HELD), lax.rem(u, 2), 1 - u // nc
        k = lax.rem(j, far)
        for way in range(2):
            g_copy(u, far - 1, way, True).wait_recv()
        for h, out in enumerate((og, ou)):
            own = pg[slot, pl.ds(pl.multiple_of(me * rows, rows), rows), h * FC:(h + 1) * FC]
            own = (own + rg[0, old, far - 1, h].astype(F32) + rg[1, old, far - 1, h].astype(F32)).astype(BF16)
            for s in range(2):
                piece = own[:, s * LB:(s + 1) * LB]
                out[layer, :, pl.ds(pl.multiple_of((block(j) + s * nc) * LB, LB), LB)] = piece
                square(piece)

        @pl.when(lax.rem(me, far) == k)
        def _():
            tall = pd.shape[2] // 2
            for way in range(2):
                d_copy(j, way, True).wait_recv()
            for h in range(2):
                own = pd[slot, me // far, h * tall:(h + 1) * tall, :]
                own = own + rd[0, k, h].astype(F32) + rd[1, k, h].astype(F32)
                own = own.T.astype(BF16)
                od[layer, pl.ds(pl.multiple_of(j // half * LB, LB), LB), h * tall:(h + 1) * tall] = own
                for s in range(tall // LB):
                    square(own[:, s * LB:(s + 1) * LB])

    def turn_round(at_step):
        p, q = at_step // far, lax.rem(at_step, far)

        @pl.when((q == 0) & (p >= 4) & (p < units + 4))
        def _():
            arrive(p - 4)

        for when, s, lag in ((0, 0, 1), (1, 3, 3), (2, 2, 2), (3, 1, 1)):
            @pl.when((q == when) & (p >= lag) & (p < units + lag))
            def _(s=s, lag=lag):
                relay(p - lag, s)

    def front(j, t, wgu, slot):
        gu = dot(a[t], wgu[j])
        dh = dot(dy[t], wdt[lax.rem(j, 2)]).astype(BF16).astype(F32)
        g, u = gu[:, :FC], gu[:, FC:]
        sig = sigmoid(g)
        silu = g * sig
        hds[slot][...] = (silu * u).astype(BF16)
        dgus[slot][:, :FC] = (dh * u * (sig + silu * (1 - sig))).astype(BF16)
        dgus[slot][:, FC:] = (dh * silu).astype(BF16)

    def back(u, t, slot, into_states, first=None):
        p, k = lax.rem(u, 2), lax.rem(u, UNITS_HELD)
        keep = (lambda old: old) if first is None else (lambda old: jnp.where(first, jnp.zeros_like(old), old))
        pg[k] = keep(pg[k]) + dot(at[t], dgus[slot][...])
        hd = dot(dyt[t], hds[slot][...])
        for s in range(2):
            pd[k, s] = keep(pd[k, s]) + hd[:, s * LB:(s + 1) * LB]
        if into_states:
            da[t] += dot(dgus[slot][...], wgut[p])

    def turn(j, t, wgu, wdn, into_states):
        p = lax.rem(j, 2)
        if into_states:
            i = pl.multiple_of(lax.rem(t, 4) * LB, LB)
            wgut[p, :, pl.ds(i, LB)] = wgu[j, pl.ds(i, LB), :].T
        s = lax.rem(t, 2)
        wdt[p, :, pl.ds(pl.multiple_of(s * LB, LB), LB)] = wdn[2 * j + s].T

    def layer_back(start, wgu, wdn, into_states):
        for t in range(4):
            turn(0, t, wgu, wdn, into_states)
        for h, g in zip(hds, dgus):
            h[...] = jnp.zeros_like(h)
            g[...] = jnp.zeros_like(g)

        @pl.loop(0, nc * nt // 2)
        def _(i):
            j, t = i // (nt // 2), 2 * lax.rem(i, nt // 2)
            k = jnp.maximum(2 * i - 1, 0)
            jn = jnp.minimum(j + 1, nc - 1)
            front(j, t, wgu, 0)
            back(start + k // nt, lax.rem(k, nt), 1, into_states)
            turn(jn, t, wgu, wdn, into_states)
            turn(jn, t + 1, wgu, wdn, into_states)
            front(j, t + 1, wgu, 1)
            back(start + j, t, 0, into_states, t == 0)
            turn_round(start * (nt // 2) + i)

        back(start + nc - 1, nt - 1, 1, into_states)

    pl.semaphore_wait(barrier, n - 1)
    layer_back(0, w2, w2d, True)

    for t in range(nt):
        for copy in a_copies(t, False):
            copy.start()

    @pl.loop(0, nt)
    def _(t):
        wide = h1[t].astype(F32)
        r = rms(wide)
        da_t = da[t].astype(BF16).astype(F32)
        dn = da_t * r - wide * (r * r * r * jnp.mean(da_t * wide, -1, keepdims=True))
        dh1 = (dy[t].astype(F32) + dn).astype(BF16)
        dy[t] = dh1
        dyt[t] = dh1.T
        for copy in a_copies(t, False):
            copy.wait()

    layer_back(nc, w1, w1d, False)

    @pl.loop(units * far, (units + 3) * far + 1)
    def _(at_step):
        turn_round(at_step)

    for way in range(2):
        for s in range(far):
            g_copy(units - 1, s, way, s > 0).wait_send()
            e = around[far - s] if way == 0 else around[n - far + s]
            d_copy(lax.rem(e, far), way, s > 0).wait_send()

    tots[pl.ds(me, 1)] = ss[...][None]
    copies = [
        pltpu.make_async_remote_copy(ss, tots.at[me], ts_sem.at[k], tr_sem.at[n - k], device_id={"dp": around[k]}, device_id_type=MESH)
        for k in range(1, n)
    ]
    for copy in copies:
        copy.start()
    outs = [pltpu.make_async_copy(*pair, sem_o.at[i]) for i, pair in enumerate(((og, og_h), (ou, ou_h), (od, od_h)))]
    for copy in outs:
        copy.start()
    for copy in copies:
        copy.wait_send()
    for k in range(1, n):
        pltpu.make_async_remote_copy(ss, tots.at[around[k]], ts_sem.at[k], tr_sem.at[k], device_id={"dp": around[k]}, device_id_type=MESH).wait_recv()
    last = pltpu.make_async_copy(tots, tot_h, sem_o.at[3])
    last.start()
    for copy in (*outs, last):
        copy.wait()


def gradients_of(x, dy, wg, wu, wd, n):
    tokens, d = x.shape[1:]
    layers, _, f = wg.shape
    nt, nc = tokens // TT, f // FC
    far = n // 2
    hbm = pl.BlockSpec(memory_space=pl.ANY)
    shape = jax.ShapeDtypeStruct
    shapes = [shape((layers, d // n, f), BF16), shape((layers, d // n, f), BF16), shape((layers, f // n, d), BF16), shape((n, 8, LB), F32),
              shape((nt, TT, d), BF16), shape((nt, d, TT), BF16)]
    v = pltpu.VMEM
    dma = pltpu.SemaphoreType.DMA
    rows = d // n
    scratch = [
        v((nc, d, 2 * FC), BF16), v((2 * nc, LB, d), BF16), v((nc, d, 2 * FC), BF16), v((2 * nc, LB, d), BF16),
        v((2, 2 * FC, d), BF16), v((2, d, FC), BF16),
        v((nt, TT, d), BF16), v((nt, d, TT), BF16), v((nt, TT, d), BF16), v((nt, TT, d), BF16), v((nt, d, TT), BF16), v((nt, TT, d), F32),
        v((3, TT, d), BF16), v((TT, f), BF16), v((TT, FC), BF16), v((TT, FC), BF16), v((TT, 2 * FC), BF16), v((TT, 2 * FC), BF16),
        v((UNITS_HELD, d, 2 * FC), F32), v((UNITS_HELD, 2, d, LB), F32),
        v((2, 2, far, 2, rows, FC), BF16), v((2, far, 2, d // 2, LB), BF16), v((2, far, 2, rows, FC), BF16), v((2, far, 2, d // 2, LB), BF16),
        v((layers, rows, f), BF16), v((layers, rows, f), BF16), v((layers, f // n, d), BF16), v((8, LB), F32), v((n, 8, LB), F32),
        dma((2, 2)), dma((3,)), dma((nt,)), dma((nt,)), dma((nt,)), dma((4,)),
        dma((2, 2, far)), dma((2, far)), dma((2, far)), dma((2, far)), dma((n,)), dma((n,)),
    ]
    return pl.pallas_call(
        functools.partial(grad_kernel, nt, nc, n),
        name="gradients",
        out_shape=shapes,
        in_specs=[hbm] * 5,
        out_specs=[hbm] * len(shapes),
        scratch_shapes=scratch,
        compiler_params=pltpu.CompilerParams(vmem_limit_bytes=VMEM_LIMIT, collective_id=0, has_side_effects=True),
    )(x, dy, wg, wu, wd)[:4]


def adamw(w, m, v, g):
    m = 0.9 * m + 0.1 * g
    v = 0.95 * v + 0.05 * g * g
    step = m * lax.rsqrt(v + 1e-8) + 0.1 * w
    return (w - 0.02 * step).astype(BF16), m, v


def solution(mesh):
    n = mesh.shape["dp"]

    def step(x, dy, *arrays):
        weights, m, v = (arrays[i:i + 3] for i in (0, 3, 6))
        *g, squares = gradients_of(x, dy, *weights, n)
        count = sum(w.size for w in weights)
        factor = jnp.minimum(1.0, 0.5 * lax.rsqrt(jnp.sum(squares) / count + 1e-30))
        me = lax.axis_index("dp")
        new = []
        for w, mm, vv, gg in zip(weights, m, v, g, strict=True):
            rows = gg.shape[1]
            own = lax.dynamic_slice_in_dim(w, me * rows, rows, 1).astype(F32)
            wn, mn, vn = adamw(own, mm, vv, gg.astype(F32) * factor)
            new.append((lax.all_gather(wn, "dp", axis=1, tiled=True), mn, vn))
        return tuple(one[which] for which in range(3) for one in new)

    seq, rows = P(("rep", "dp"), None, None), P(None, "dp", None)
    return jax.shard_map(
        step,
        mesh=mesh,
        in_specs=(seq, seq) + (P(),) * 3 + (rows,) * 6,
        out_specs=(P("rep"),) * 3 + (P("rep", "dp"),) * 6,
        check_vma=False,
    )
```

```python
import functools

import jax
import jax.numpy as jnp
from jax import lax
from jax.experimental import pallas as pl
from jax.experimental.pallas import tpu as pltpu
from jax.sharding import PartitionSpec as P

F32, BF16 = jnp.float32, jnp.bfloat16
MESH = pl.DeviceIdType.MESH
TT = 512
LB = 128
FC = 2 * LB
UNITS_HELD = 5
VMEM_LIMIT = 67_043_328


def dot(a, b):
    return jnp.dot(a, b, preferred_element_type=F32)


def rms(wide):
    return lax.rsqrt(jnp.mean(wide * wide, -1, keepdims=True) + 1e-6)


def sigmoid(g):
    return 0.5 * jnp.tanh(0.5 * g) + 0.5


def grad_kernel(nt, nc, n, x_h, dy_h, wg_h, wu_h, wd_h, og_h, ou_h, od_h, tot_h, a1_h, a1t_h,
                w1, w1d, w2, w2d, wgut, wdt, a, at, h1, dy, dyt, da, xb, hid, hd0, hd1, dgu0, dgu1,
                pg, pd, rg, rd, sg, sd, og, ou, od, ss, tots,
                sem_w, sem_x, sem_dy, sem_a, sem_at, sem_o, rg_sem, rd_sem, sg_sem, sd_sem, ts_sem, tr_sem):
    half, far = nc // 2, n // 2
    units = 2 * nc
    rows = pg.shape[1] // n
    hds, dgus = (hd0, hd1), (dgu0, dgu1)
    me = lax.axis_index("dp")
    around = [lax.rem(me + k, n) for k in range(n)]
    towards = (around[1], around[n - 1])

    barrier = pltpu.get_barrier_semaphore()
    for k in range(1, n):
        pl.semaphore_signal(barrier, inc=1, device_id={"dp": around[k]}, device_id_type=MESH)

    def block(j):
        return 2 * lax.rem(j, half) + j // half

    for layer, (wgu, wdn) in enumerate(((w1, w1d), (w2, w2d))):
        for j in range(nc):
            for s in range(2):
                cols = pl.ds((2 * (j % half) + j // half + s * nc) * LB, LB)
                pltpu.make_async_copy(wg_h.at[layer, :, cols], wgu.at[j, :, pl.ds(s * LB, LB)], sem_w.at[layer, 0]).start()
                pltpu.make_async_copy(wu_h.at[layer, :, cols], wgu.at[j, :, pl.ds(FC + s * LB, LB)], sem_w.at[layer, 0]).start()
                pltpu.make_async_copy(wd_h.at[layer, cols, :], wdn.at[j * 2 + s], sem_w.at[layer, 1]).start()

    def x_copy(t):
        s = lax.rem(t, 3)
        return pltpu.make_async_copy(x_h.at[0, pl.ds(t * TT, TT), :], xb.at[s], sem_x.at[s])

    def dy_copy(t):
        return pltpu.make_async_copy(dy_h.at[0, pl.ds(t * TT, TT), :], dy.at[t], sem_dy.at[t])

    def a_copies(t, out):
        pairs = ((a.at[t], a1_h.at[t], sem_a.at[t]), (at.at[t], a1t_h.at[t], sem_at.at[t]))
        return [pltpu.make_async_copy(*((v, h) if out else (h, v)), s) for v, h, s in pairs]

    x_copy(0).start()
    for t in range(nt):
        dy_copy(t).start()
    pltpu.make_async_copy(w1, w1, sem_w.at[0, 0]).wait()
    pltpu.make_async_copy(w1d, w1d, sem_w.at[0, 1]).wait()
    ss[...] = jnp.zeros_like(ss)

    def forward_back(t):
        y = dot(hid[...], w1d[...].reshape(2 * nc * LB, -1))
        h1[t] = (xb[lax.rem(t, 3)].astype(F32) + y.astype(BF16).astype(F32)).astype(BF16)
        da[t] = jnp.zeros(da.shape[1:], F32)
        dyt[t] = dy[t].T

    @pl.loop(0, nt)
    def _(t):
        before = jnp.maximum(t - 1, 0)
        x_copy(t).wait()
        dy_copy(t).wait()

        @pl.when(t + 1 < nt)
        def _():
            x_copy(t + 1).start()

        forward_back(before)
        wide = xb[lax.rem(t, 3)].astype(F32)
        a1 = (wide * rms(wide)).astype(BF16)
        a[t] = a1
        at[t] = a1.T
        for j in range(nc):
            gu = dot(a1, w1[j])
            g, u = gu[:, :FC], gu[:, FC:]
            hid[:, j * FC:(j + 1) * FC] = (g * sigmoid(g) * u).astype(BF16)
        for copy in a_copies(t, True):
            copy.start()

    forward_back(nt - 1)
    pltpu.make_async_copy(w2, w2, sem_w.at[1, 0]).wait()
    pltpu.make_async_copy(w2d, w2d, sem_w.at[1, 1]).wait()

    @pl.loop(0, nt)
    def _(t):
        for copy in a_copies(t, True):
            copy.wait()
        wide = h1[t].astype(F32)
        a2 = (wide * rms(wide)).astype(BF16)
        a[t] = a2
        at[t] = a2.T

    def g_copy(u, s, way, both):
        part = (lambda ref: ref) if both else (lambda ref: ref.at[way])
        return pltpu.make_async_remote_copy(
            part(sg.at[way, s]), part(rg.at[way, lax.rem(u, 2), s]), sg_sem.at[way, s], rg_sem.at[way, lax.rem(u, 2), s],
            device_id={"dp": towards[way]}, device_id_type=MESH)

    def d_copy(j, way, both):
        k = lax.rem(j, far)
        part = (lambda ref: ref) if both else (lambda ref: ref.at[way])
        return pltpu.make_async_remote_copy(
            part(sd.at[way, k]), part(rd.at[way, k]), sd_sem.at[way, k], rd_sem.at[way, k],
            device_id={"dp": towards[way]}, device_id_type=MESH)

    def relay(u, s):
        j, slot, old = lax.rem(u, nc), lax.rem(u, UNITS_HELD), lax.rem(u, 2)
        for way in range(2):
            e = around[far - s] if way == 0 else around[n - far + s]

            @pl.when(u > 0)
            def _():
                g_copy(u - 1, s, way, s > 0).wait_send()

            if s > 0:
                g_copy(u, s - 1, way, s > 1).wait_recv()
            for h in range(2):
                if s == 0 and h != way:
                    continue
                own = pg[slot, pl.ds(pl.multiple_of(e * rows, rows), rows), h * FC:(h + 1) * FC]
                if s > 1 or (s == 1 and h == way):
                    own += rg[way, old, s - 1, h].astype(F32)
                sg[way, s, h] = own.astype(BF16)
            g_copy(u, s, way, s > 0).start()

            @pl.when(lax.rem(e, far) == lax.rem(j, far))
            def _():
                k = lax.rem(j, far)

                @pl.when(u >= far)
                def _():
                    d_copy(j, way, s > 0).wait_send()

                if s > 0:
                    d_copy(j, way, s > 1).wait_recv()
                tall = pd.shape[2] // 2
                for h in range(2):
                    if s == 0 and h != way:
                        continue
                    own = pd[slot, e // far, h * tall:(h + 1) * tall, :]
                    if s > 1 or (s == 1 and h == way):
                        own += rd[way, k, h].astype(F32)
                    sd[way, k, h] = own.astype(BF16)
                d_copy(j, way, s > 0).start()

    def square(g):
        wide = g.astype(F32)
        ss[...] += jnp.sum((wide * wide).reshape(-1, *ss.shape), 0)

    def arrive(u):
        j, slot, old, layer = lax.rem(u, nc), lax.rem(u, UNITS_HELD), lax.rem(u, 2), 1 - u // nc
        k = lax.rem(j, far)
        for way in range(2):
            g_copy(u, far - 1, way, True).wait_recv()
        for h, out in enumerate((og, ou)):
            own = pg[slot, pl.ds(pl.multiple_of(me * rows, rows), rows), h * FC:(h + 1) * FC]
            own = (own + rg[0, old, far - 1, h].astype(F32) + rg[1, old, far - 1, h].astype(F32)).astype(BF16)
            for s in range(2):
                piece = own[:, s * LB:(s + 1) * LB]
                out[layer, :, pl.ds(pl.multiple_of((block(j) + s * nc) * LB, LB), LB)] = piece
                square(piece)

        @pl.when(lax.rem(me, far) == k)
        def _():
            tall = pd.shape[2] // 2
            for way in range(2):
                d_copy(j, way, True).wait_recv()
            for h in range(2):
                own = pd[slot, me // far, h * tall:(h + 1) * tall, :]
                own = own + rd[0, k, h].astype(F32) + rd[1, k, h].astype(F32)
                own = own.T.astype(BF16)
                od[layer, pl.ds(pl.multiple_of(j // half * LB, LB), LB), h * tall:(h + 1) * tall] = own
                for s in range(tall // LB):
                    square(own[:, s * LB:(s + 1) * LB])

    def turn_round(at_step):
        p, q = at_step // far, lax.rem(at_step, far)

        @pl.when((q == 0) & (p >= 4) & (p < units + 4))
        def _():
            arrive(p - 4)

        for when, s, lag in ((0, 0, 1), (1, 3, 3), (2, 2, 2), (3, 1, 1)):
            @pl.when((q == when) & (p >= lag) & (p < units + lag))
            def _(s=s, lag=lag):
                relay(p - lag, s)

    def front(j, t, wgu, slot):
        gu = dot(a[t], wgu[j])
        dh = dot(dy[t], wdt[lax.rem(j, 2)]).astype(BF16).astype(F32)
        g, u = gu[:, :FC], gu[:, FC:]
        sig = sigmoid(g)
        silu = g * sig
        hds[slot][...] = (silu * u).astype(BF16)
        dgus[slot][:, :FC] = (dh * u * (sig + silu * (1 - sig))).astype(BF16)
        dgus[slot][:, FC:] = (dh * silu).astype(BF16)

    def back(u, t, slot, into_states, first=None):
        p, k = lax.rem(u, 2), lax.rem(u, UNITS_HELD)
        keep = (lambda old: old) if first is None else (lambda old: jnp.where(first, jnp.zeros_like(old), old))
        pg[k] = keep(pg[k]) + dot(at[t], dgus[slot][...])
        hd = dot(dyt[t], hds[slot][...])
        for s in range(2):
            pd[k, s] = keep(pd[k, s]) + hd[:, s * LB:(s + 1) * LB]
        if into_states:
            da[t] += dot(dgus[slot][...], wgut[p])

    def turn(j, t, wgu, wdn, into_states):
        p = lax.rem(j, 2)
        if into_states:
            i = pl.multiple_of(lax.rem(t, 4) * LB, LB)
            wgut[p, :, pl.ds(i, LB)] = wgu[j, pl.ds(i, LB), :].T
        s = lax.rem(t, 2)
        wdt[p, :, pl.ds(pl.multiple_of(s * LB, LB), LB)] = wdn[2 * j + s].T

    def layer_back(start, wgu, wdn, into_states):
        for t in range(4):
            turn(0, t, wgu, wdn, into_states)
        for h, g in zip(hds, dgus):
            h[...] = jnp.zeros_like(h)
            g[...] = jnp.zeros_like(g)

        @pl.loop(0, nc * nt // 2)
        def _(i):
            j, t = i // (nt // 2), 2 * lax.rem(i, nt // 2)
            k = jnp.maximum(2 * i - 1, 0)
            jn = jnp.minimum(j + 1, nc - 1)
            front(j, t, wgu, 0)
            back(start + k // nt, lax.rem(k, nt), 1, into_states)
            turn(jn, t, wgu, wdn, into_states)
            turn(jn, t + 1, wgu, wdn, into_states)
            front(j, t + 1, wgu, 1)
            back(start + j, t, 0, into_states, t == 0)
            turn_round(start * (nt // 2) + i)

        back(start + nc - 1, nt - 1, 1, into_states)

    pl.semaphore_wait(barrier, n - 1)
    layer_back(0, w2, w2d, True)

    for t in range(nt):
        for copy in a_copies(t, False):
            copy.start()

    @pl.loop(0, nt)
    def _(t):
        wide = h1[t].astype(F32)
        r = rms(wide)
        da_t = da[t].astype(BF16).astype(F32)
        dn = da_t * r - wide * (r * r * r * jnp.mean(da_t * wide, -1, keepdims=True))
        dh1 = (dy[t].astype(F32) + dn).astype(BF16)
        dy[t] = dh1
        dyt[t] = dh1.T
        for copy in a_copies(t, False):
            copy.wait()

    layer_back(nc, w1, w1d, False)

    @pl.loop(units * far, (units + 3) * far + 1)
    def _(at_step):
        turn_round(at_step)

    for way in range(2):
        for s in range(far):
            g_copy(units - 1, s, way, s > 0).wait_send()
            e = around[far - s] if way == 0 else around[n - far + s]
            d_copy(lax.rem(e, far), way, s > 0).wait_send()

    tots[pl.ds(me, 1)] = ss[...][None]
    copies = [
        pltpu.make_async_remote_copy(ss, tots.at[me], ts_sem.at[k], tr_sem.at[n - k], device_id={"dp": around[k]}, device_id_type=MESH)
        for k in range(1, n)
    ]
    for copy in copies:
        copy.start()
    outs = [pltpu.make_async_copy(*pair, sem_o.at[i]) for i, pair in enumerate(((og, og_h), (ou, ou_h), (od, od_h)))]
    for copy in outs:
        copy.start()
    for copy in copies:
        copy.wait_send()
    for k in range(1, n):
        pltpu.make_async_remote_copy(ss, tots.at[around[k]], ts_sem.at[k], tr_sem.at[k], device_id={"dp": around[k]}, device_id_type=MESH).wait_recv()
    last = pltpu.make_async_copy(tots, tot_h, sem_o.at[3])
    last.start()
    for copy in (*outs, last):
        copy.wait()


def gradients_of(x, dy, wg, wu, wd, n):
    tokens, d = x.shape[1:]
    layers, _, f = wg.shape
    nt, nc = tokens // TT, f // FC
    far = n // 2
    hbm = pl.BlockSpec(memory_space=pl.ANY)
    shape = jax.ShapeDtypeStruct
    shapes = [shape((layers, d // n, f), BF16), shape((layers, d // n, f), BF16), shape((layers, f // n, d), BF16), shape((n, 8, LB), F32),
              shape((nt, TT, d), BF16), shape((nt, d, TT), BF16)]
    v = pltpu.VMEM
    dma = pltpu.SemaphoreType.DMA
    rows = d // n
    scratch = [
        v((nc, d, 2 * FC), BF16), v((2 * nc, LB, d), BF16), v((nc, d, 2 * FC), BF16), v((2 * nc, LB, d), BF16),
        v((2, 2 * FC, d), BF16), v((2, d, FC), BF16),
        v((nt, TT, d), BF16), v((nt, d, TT), BF16), v((nt, TT, d), BF16), v((nt, TT, d), BF16), v((nt, d, TT), BF16), v((nt, TT, d), F32),
        v((3, TT, d), BF16), v((TT, f), BF16), v((TT, FC), BF16), v((TT, FC), BF16), v((TT, 2 * FC), BF16), v((TT, 2 * FC), BF16),
        v((UNITS_HELD, d, 2 * FC), F32), v((UNITS_HELD, 2, d, LB), F32),
        v((2, 2, far, 2, rows, FC), BF16), v((2, far, 2, d // 2, LB), BF16), v((2, far, 2, rows, FC), BF16), v((2, far, 2, d // 2, LB), BF16),
        v((layers, rows, f), BF16), v((layers, rows, f), BF16), v((layers, f // n, d), BF16), v((8, LB), F32), v((n, 8, LB), F32),
        dma((2, 2)), dma((3,)), dma((nt,)), dma((nt,)), dma((nt,)), dma((4,)),
        dma((2, 2, far)), dma((2, far)), dma((2, far)), dma((2, far)), dma((n,)), dma((n,)),
    ]
    return pl.pallas_call(
        functools.partial(grad_kernel, nt, nc, n),
        name="gradients",
        out_shape=shapes,
        in_specs=[hbm] * 5,
        out_specs=[hbm] * len(shapes),
        scratch_shapes=scratch,
        compiler_params=pltpu.CompilerParams(vmem_limit_bytes=VMEM_LIMIT, collective_id=0, has_side_effects=True),
    )(x, dy, wg, wu, wd)[:4]


def update_kernel(n, count, *refs):
    gs, tot_h, ws, ms, vs = refs[:3], refs[3], refs[4:7], refs[7:10], refs[10:13]
    ow, om, ov = refs[13:16], refs[16:19], refs[19:22]
    full, gb, mb, vb = refs[22:25], refs[25:28], refs[28:31], refs[31:34]
    tots, in_sem, tot_sem, mv_sem, w_sem, send_sem, recv_sem = refs[34:]
    far = n // 2
    layers = full[0].shape[0]
    me = lax.axis_index("dp")
    around = [lax.rem(me + k, n) for k in range(n)]
    towards = (around[1], around[n - 1])
    pieces = [(i, layer) for layer in range(layers) for i in range(3)]

    barrier = pltpu.get_barrier_semaphore()
    for other in towards:
        pl.semaphore_signal(barrier, inc=1, device_id={"dp": other}, device_id_type=MESH)

    def block(i, origin, half=None):
        rows = full[i].shape[1] // n
        start = origin * rows
        if half is not None:
            rows //= 2
            start += half * rows
        return pl.ds(pl.multiple_of(start, rows), rows)

    loads = {}
    total = pltpu.make_async_copy(tot_h, tots, tot_sem)
    total.start()
    for k, (i, layer) in enumerate(pieces):
        own = block(i, me)
        loads[k] = [
            pltpu.make_async_copy(src, dst, in_sem.at[k, c])
            for c, (src, dst) in enumerate((
                (gs[i].at[layer], gb[i].at[layer]), (ws[i].at[layer, own, :], full[i].at[layer, own, :]),
                (ms[i].at[layer], mb[i].at[layer]), (vs[i].at[layer], vb[i].at[layer])))
        ]
        for copy in loads[k]:
            copy.start()
    total.wait()
    factor = jnp.minimum(1.0, 0.5 * lax.rsqrt(jnp.sum(tots[...], keepdims=True).reshape(1, 1) / count + 1e-30))

    def pass_on(k, s, way):
        i, layer = pieces[k]
        origin = around[(n - s) % n] if way == 0 else around[s]
        rows = block(i, origin, way if s == far - 1 else None)
        return pltpu.make_async_remote_copy(
            full[i].at[layer, rows, :], full[i].at[layer, rows, :], send_sem.at[way, s, k], recv_sem.at[way, s, k],
            device_id={"dp": towards[way]}, device_id_type=MESH)

    def came(k, s, way):
        i, layer = pieces[k]
        origin = around[n - s - 1] if way == 0 else around[s + 1]
        rows = block(i, origin, way if s == far - 1 else None)
        here = full[i].at[layer, rows, :]
        return pltpu.make_async_remote_copy(
            here, here, send_sem.at[way, s, k], recv_sem.at[way, s, k], device_id={"dp": towards[way]}, device_id_type=MESH
        ), pltpu.make_async_copy(here, ow[i].at[layer, rows, :], w_sem.at[way, s, k])

    outs = []
    for k, (i, layer) in enumerate(pieces):
        for copy in loads[k]:
            copy.wait()
        rows = mb[i].shape[1]
        some = max(16, rows // 8)
        first = me * rows

        @pl.loop(0, rows // some)
        def _(r):
            here = pl.ds(pl.multiple_of(r * some, some), some)
            there = pl.ds(pl.multiple_of(first + r * some, some), some)
            g = gb[i][layer, here, :].astype(F32) * factor
            m = 0.9 * mb[i][layer, here, :] + 0.1 * g
            v = 0.95 * vb[i][layer, here, :] + 0.05 * g * g
            w = full[i][layer, there, :].astype(F32)
            step = m * lax.rsqrt(v + 1e-8) + 0.1 * w
            mb[i][layer, here, :] = m
            vb[i][layer, here, :] = v
            full[i][layer, there, :] = (w - 0.02 * step).astype(BF16)

        if k == 0:
            pl.semaphore_wait(barrier, 2)
        for way in range(2):
            pass_on(k, 0, way).start()
        own = block(i, me)
        outs += [
            pltpu.make_async_copy(mb[i].at[layer], om[i].at[layer], mv_sem.at[k, 0]),
            pltpu.make_async_copy(vb[i].at[layer], ov[i].at[layer], mv_sem.at[k, 1]),
            pltpu.make_async_copy(full[i].at[layer, own, :], ow[i].at[layer, own, :], mv_sem.at[k, 2]),
        ]
        for copy in outs[-3:]:
            copy.start()

    for s in range(far):
        for k in range(len(pieces)):
            for way in range(2):
                arrival, out = came(k, s, way)
                arrival.wait_recv()
                if s + 1 < far:
                    pass_on(k, s + 1, way).start()
                out.start()
                outs.append(out)
    for s in range(far):
        for k in range(len(pieces)):
            for way in range(2):
                pass_on(k, s, way).wait_send()
    for copy in outs:
        copy.wait()


def update(g, squares, w, m, v, n):
    hbm = pl.BlockSpec(memory_space=pl.ANY)
    shape = lambda like: jax.ShapeDtypeStruct(like.shape, like.dtype)
    dma = pltpu.SemaphoreType.DMA
    far, pieces = n // 2, 3 * w[0].shape[0]
    scratch = [pltpu.VMEM(like.shape, like.dtype) for group in (w, g, m, v) for like in group] + [
        pltpu.VMEM(squares.shape, F32), dma((pieces, 4)), dma, dma((pieces, 3)),
        dma((2, far, pieces)), dma((2, far, pieces)), dma((2, far, pieces)),
    ]
    out = pl.pallas_call(
        functools.partial(update_kernel, n, sum(one.size for one in w)),
        name="update",
        out_shape=[shape(like) for group in (w, m, v) for like in group],
        in_specs=[hbm] * 13,
        out_specs=[hbm] * 9,
        scratch_shapes=scratch,
        compiler_params=pltpu.CompilerParams(vmem_limit_bytes=VMEM_LIMIT, collective_id=1, has_side_effects=True),
    )(*g, squares, *w, *m, *v)
    return tuple(out)


def solution(mesh):
    n = mesh.shape["dp"]

    def step(x, dy, *arrays):
        weights, m, v = (arrays[i:i + 3] for i in (0, 3, 6))
        *g, squares = gradients_of(x, dy, *weights, n)
        return update(g, squares, weights, m, v, n)

    seq, rows = P(("rep", "dp"), None, None), P(None, "dp", None)
    return jax.shard_map(
        step,
        mesh=mesh,
        in_specs=(seq, seq) + (P(),) * 3 + (rows,) * 6,
        out_specs=(P("rep"),) * 3 + (P("rep", "dp"),) * 6,
        check_vma=False,
    )
```

```python
import functools

import jax
import jax.numpy as jnp
from jax import lax
from jax.experimental import pallas as pl
from jax.experimental.pallas import tpu as pltpu
from jax.sharding import PartitionSpec as P

F32, BF16 = jnp.float32, jnp.bfloat16
MESH = pl.DeviceIdType.MESH
TT = 512
LB = 128
FC = 2 * LB
UNITS_HELD = 5
VMEM_BYTES = 67_043_328


def dot(a, b):
    return jnp.dot(a, b, preferred_element_type=F32)


def rms(wide):
    return lax.rsqrt(jnp.mean(wide * wide, -1, keepdims=True) + 1e-6)


def sigmoid(g):
    return 0.5 * jnp.tanh(0.5 * g) + 0.5


def step_kernel(nt, nc, n, count, x_h, dy_h, wg_h, wu_h, wd_h, mg_h, mu_h, md_h, vg_h, vu_h, vd_h,
                fg, fu, fd, wide_ref, gu_h, a1t_h,
                wgut, wdt, a, at, h1, dy, dyt, xb, hid, hd0, hd1, dgu0, dgu1,
                pg, pd, rg, rd, sg, sd, og, ou, od, ss, tots,
                sem_w, sem_x, sem_dy, sem_at, sem_gu, rg_sem, rd_sem, sg_sem, sd_sem, ts_sem, tr_sem, mv_sem, ag_send, ag_recv):
    half, far = nc // 2, n // 2
    units = 2 * nc
    rows = pg.shape[1] // n
    hds, dgus = (hd0, hd1), (dgu0, dgu1)
    full, own_g = (fg, fu, fd), (og, ou, od)
    da = wide_ref
    me = lax.axis_index("dp")
    around = [lax.rem(me + k, n) for k in range(n)]
    towards = (around[1], around[n - 1])

    barrier = pltpu.get_barrier_semaphore()
    for k in range(1, n):
        pl.semaphore_signal(barrier, inc=1, device_id={"dp": around[k]}, device_id_type=MESH)

    def block(j):
        return 2 * lax.rem(j, half) + j // half

    def at_block(b):
        return pl.ds(b * LB if isinstance(b, int) else pl.multiple_of(b * LB, LB), LB)

    def x_copy(t):
        s = lax.rem(t, 3)
        return pltpu.make_async_copy(x_h.at[0, pl.ds(t * TT, TT), :], xb.at[s], sem_x.at[s])

    def dy_copy(t):
        return pltpu.make_async_copy(dy_h.at[0, pl.ds(t * TT, TT), :], dy.at[t], sem_dy.at[t])

    def w_copies(layer):
        return [pltpu.make_async_copy(h.at[layer], v.at[layer], sem_w.at[layer, i]) for i, (h, v) in enumerate(zip((wg_h, wu_h, wd_h), full))]

    x_copy(0).start()
    for copy in w_copies(0):
        copy.start()
    x_copy(1).start()
    for t in range(nt):
        dy_copy(t).start()
    for copy in w_copies(1):
        copy.start()
    ss[...] = jnp.zeros_like(ss)

    def gu_out(t, j):
        return pltpu.make_async_copy(da.at[j], gu_h.at[j, t], sem_gu.at[j])

    def a1t_out(t):
        p = lax.rem(t, 2)
        return pltpu.make_async_copy(wgut.at[p], a1t_h.at[t], sem_at.at[p])

    def static_block(j):
        return 2 * (j % half) + j // half

    def down_part(part):
        some = range(part * half, (part + 1) * half)
        w = jnp.concatenate([fd[0, at_block(static_block(j) + s * nc), :] for j in some for s in range(2)], 0)
        return dot(hid[:, part * half * FC:(part + 1) * half * FC], w)

    def gate_up(j):
        cols = [at_block(static_block(j) + s * nc) for s in range(2)]
        gu = dot(dgu0[...], jnp.concatenate([f[0, :, c] for f in (fg, fu) for c in cols], 1))
        da[j] = gu
        g, u = gu[:, :FC], gu[:, FC:]
        hid[:, j * FC:(j + 1) * FC] = (g * sigmoid(g) * u).astype(BF16)

    def finish(t):
        y = pg[0] + down_part(1)
        h = (xb[lax.rem(t, 3)].astype(F32) + y.astype(BF16).astype(F32)).astype(BF16)
        h1[t] = h
        wide = h.astype(F32)
        a2 = (wide * rms(wide)).astype(BF16)
        a[t] = a2
        at[t] = a2.T
        dyt[t] = dy[t].T

    def forward(t, follows):
        x_copy(t).wait()
        dy_copy(t).wait()
        if follows:
            for j in range(half):
                gu_out(t - 1, j).wait()

            @pl.when(t >= 2)
            def _():
                a1t_out(t - 2).wait()

            pg[0] = down_part(0)
        wide = xb[lax.rem(t, 3)].astype(F32)
        a1 = (wide * rms(wide)).astype(BF16)
        dgu0[...] = a1
        wgut[lax.rem(t, 2)] = a1.T
        for j in range(half):
            gate_up(j)
        for j in range(half):
            gu_out(t, j).start()
        a1t_out(t).start()
        if follows:
            for j in range(half, nc):
                gu_out(t - 1, j).wait()
            finish(t - 1)
        for j in range(half, nc):
            gate_up(j)
        for j in range(half, nc):
            gu_out(t, j).start()

        @pl.when(t + 2 < nt)
        def _():
            x_copy(t + 2).start()

    for copy in w_copies(0):
        copy.wait()
    forward(0, False)

    @pl.loop(1, nt)
    def _(t):
        forward(t, True)

    pg[0] = down_part(0)
    finish(nt - 1)
    for j in range(nc):
        gu_out(nt - 1, j).wait()
    for t in (nt - 2, nt - 1):
        a1t_out(t).wait()
    for copy in w_copies(1):
        copy.wait()

    def g_copy(u, s, way, both):
        part = (lambda ref: ref) if both else (lambda ref: ref.at[way])
        return pltpu.make_async_remote_copy(
            part(sg.at[way, s]), part(rg.at[way, lax.rem(u, 2), s]), sg_sem.at[way, s], rg_sem.at[way, lax.rem(u, 2), s],
            device_id={"dp": towards[way]}, device_id_type=MESH)

    def d_copy(j, way, both):
        k = lax.rem(j, far)
        part = (lambda ref: ref) if both else (lambda ref: ref.at[way])
        return pltpu.make_async_remote_copy(
            part(sd.at[way, k]), part(rd.at[way, k]), sd_sem.at[way, k], rd_sem.at[way, k],
            device_id={"dp": towards[way]}, device_id_type=MESH)

    def relay(u, s):
        j, slot, old = lax.rem(u, nc), lax.rem(u, UNITS_HELD), lax.rem(u, 2)
        for way in range(2):
            e = around[far - s] if way == 0 else around[n - far + s]

            @pl.when(u > 0)
            def _():
                g_copy(u - 1, s, way, s > 0).wait_send()

            if s > 0:
                g_copy(u, s - 1, way, s > 1).wait_recv()
            for h in range(2):
                if s == 0 and h != way:
                    continue
                own = pg[slot, pl.ds(pl.multiple_of(e * rows, rows), rows), h * FC:(h + 1) * FC]
                if s > 1 or (s == 1 and h == way):
                    own += rg[way, old, s - 1, h].astype(F32)
                sg[way, s, h] = own.astype(BF16)
            g_copy(u, s, way, s > 0).start()

            @pl.when(lax.rem(e, far) == lax.rem(j, far))
            def _():
                k = lax.rem(j, far)

                @pl.when(u >= far)
                def _():
                    d_copy(j, way, s > 0).wait_send()

                if s > 0:
                    d_copy(j, way, s > 1).wait_recv()
                tall = pd.shape[2] // 2
                for h in range(2):
                    if s == 0 and h != way:
                        continue
                    own = pd[slot, e // far, h * tall:(h + 1) * tall, :]
                    if s > 1 or (s == 1 and h == way):
                        own += rd[way, k, h].astype(F32)
                    sd[way, k, h] = own.astype(BF16)
                d_copy(j, way, s > 0).start()

    def square(g):
        wide = g.astype(F32)
        ss[...] += jnp.sum((wide * wide).reshape(-1, *ss.shape), 0)

    def arrive(u):
        j, slot, old, layer = lax.rem(u, nc), lax.rem(u, UNITS_HELD), lax.rem(u, 2), 1 - u // nc
        k = lax.rem(j, far)
        for way in range(2):
            g_copy(u, far - 1, way, True).wait_recv()
        for h, out in enumerate((og, ou)):
            own = pg[slot, pl.ds(pl.multiple_of(me * rows, rows), rows), h * FC:(h + 1) * FC]
            own = (own + rg[0, old, far - 1, h].astype(F32) + rg[1, old, far - 1, h].astype(F32)).astype(BF16)
            for s in range(2):
                piece = own[:, s * LB:(s + 1) * LB]
                out[layer, :, at_block(block(j) + s * nc)] = piece
                square(piece)

        @pl.when(lax.rem(me, far) == k)
        def _():
            tall = pd.shape[2] // 2
            for way in range(2):
                d_copy(j, way, True).wait_recv()
            for h in range(2):
                own = pd[slot, me // far, h * tall:(h + 1) * tall, :]
                own = own + rd[0, k, h].astype(F32) + rd[1, k, h].astype(F32)
                own = own.T.astype(BF16)
                od[layer, at_block(j // half), h * tall:(h + 1) * tall] = own
                for s in range(tall // LB):
                    square(own[:, s * LB:(s + 1) * LB])

    def turn_round(at_step):
        p, q = at_step // far, lax.rem(at_step, far)

        @pl.when((q == 0) & (p >= 4) & (p < units + 4))
        def _():
            arrive(p - 4)

        for when, s, lag in ((0, 0, 1), (1, 3, 3), (2, 2, 2), (3, 1, 1)):
            @pl.when((q == when) & (p >= lag) & (p < units + lag))
            def _(s=s, lag=lag):
                relay(p - lag, s)

    def elementwise(gu, dh, slot):
        g, u = gu[:, :FC], gu[:, FC:]
        sig = sigmoid(g)
        silu = g * sig
        hds[slot][...] = (silu * u).astype(BF16)
        dgus[slot][:, :FC] = (dh * u * (sig + silu * (1 - sig))).astype(BF16)
        dgus[slot][:, FC:] = (dh * silu).astype(BF16)

    def back(u, t, slot, first=None):
        k = lax.rem(u, UNITS_HELD)
        keep = (lambda old: old) if first is None else (lambda old: jnp.where(first, jnp.zeros_like(old), old))
        pg[k] = keep(pg[k]) + dot(at[t], dgus[slot][...])
        hd = dot(dyt[t], hds[slot][...])
        for s in range(2):
            pd[k, s] = keep(pd[k, s]) + hd[:, s * LB:(s + 1) * LB]

    def to_states(u, t, slot):
        old = jnp.where(u == 0, jnp.zeros(da.shape[1:], F32), da[t])
        da[t] = old + dot(dgus[slot][...], wgut[lax.rem(u, 2)])

    def turn(layer, j, t):
        p = lax.rem(j, 2)
        if layer:
            for i, f in enumerate((fg, fu)):
                s = lax.rem(t, 2)
                wgut[p, pl.ds(pl.multiple_of(i * FC + s * LB, LB), LB), :] = f[layer, :, at_block(block(j) + s * nc)].T
        s = lax.rem(t, 2)
        wdt[p, :, at_block(s)] = fd[layer, at_block(block(j) + s * nc), :].T

    def clear():
        for h, g in zip(hds, dgus):
            h[...] = jnp.zeros_like(h)
            g[...] = jnp.zeros_like(g)

    per_chunk = nt // 2
    pl.semaphore_wait(barrier, n - 1)

    for t in range(2):
        turn(1, 0, t)
    clear()

    def front2(j, t, slot):
        cols = [at_block(block(j) + s * nc) for s in range(2)]
        gu = dot(a[t], jnp.concatenate([f[1, :, c] for f in (fg, fu) for c in cols], 1))
        elementwise(gu, dot(dy[t], wdt[lax.rem(j, 2)]).astype(BF16).astype(F32), slot)

    @pl.loop(0, nc * per_chunk)
    def _(i):
        j, t = i // per_chunk, 2 * lax.rem(i, per_chunk)
        k = jnp.maximum(2 * i - 1, 0)
        front2(j, t, 0)
        back(k // nt, lax.rem(k, nt), 1)
        to_states(k // nt, lax.rem(k, nt), 1)
        for s in range(2):
            turn(1, jnp.minimum(j + 1, nc - 1), t + s)
        front2(j, t + 1, 1)
        back(j, t, 0, t == 0)
        to_states(j, t, 0)
        turn_round(i)

    back(nc - 1, nt - 1, 1)
    to_states(nc - 1, nt - 1, 1)

    def a1t_in(t):
        return pltpu.make_async_copy(a1t_h.at[t], at.at[t], sem_dy.at[t])

    def gu_in(i):
        return pltpu.make_async_copy(gu_h.at[i // nt, lax.rem(i, nt)], da.at[lax.rem(i, nt)], sem_gu.at[lax.rem(i, nt)])

    for t in range(nt):
        a1t_in(t).start()

    @pl.loop(0, nt)
    def _(t):
        wide = h1[t].astype(F32)
        r = rms(wide)
        da_t = da[t].astype(BF16).astype(F32)
        dn = da_t * r - wide * (r * r * r * jnp.mean(da_t * wide, -1, keepdims=True))
        dh1 = (dy[t].astype(F32) + dn).astype(BF16)
        dy[t] = dh1
        dyt[t] = dh1.T
        gu_in(t).start()
        a1t_in(t).wait()

    for t in range(2):
        turn(0, 0, t)
    clear()

    def front1(j, t, slot):
        elementwise(da[t], dot(dy[t], wdt[lax.rem(j, 2)]).astype(BF16).astype(F32), slot)

    @pl.loop(0, nc * per_chunk)
    def _(i):
        j, t = i // per_chunk, 2 * lax.rem(i, per_chunk)
        k = jnp.maximum(2 * i - 1, 0)
        for s in range(2):
            gu_in(2 * i + s).wait()
        front1(j, t, 0)
        back(nc + k // nt, lax.rem(k, nt), 1)
        for s in range(2):
            turn(0, jnp.minimum(j + 1, nc - 1), t + s)
        front1(j, t + 1, 1)
        back(nc + j, t, 0, t == 0)

        @pl.when(j + 1 < nc)
        def _():
            for s in range(2):
                gu_in(2 * i + s + nt).start()

        turn_round(nc * per_chunk + i)

    back(2 * nc - 1, nt - 1, 1)

    pieces = [(i, layer) for layer in (1, 0) for i in range(3)]
    d = h1.shape[2]
    deep = n // 2 * rows

    def moment_copies(k):
        i, layer = pieces[k]
        made = []
        for c, h in enumerate(((mg_h, mu_h, md_h)[i], (vg_h, vu_h, vd_h)[i])):
            if i == 2:
                made.append(pltpu.make_async_copy(h.at[layer], da.at[k, pl.ds(c * deep, deep), :], mv_sem.at[k, c]))
            else:
                for b in range(far):
                    made.append(pltpu.make_async_copy(
                        h.at[layer, :, pl.ds(b * d, d)], da.at[k, pl.ds(c * deep + b * rows, rows), :], mv_sem.at[k, c * far + b]))
        return made

    for k in range(len(pieces)):
        for copy in moment_copies(k):
            copy.start()

    @pl.loop(units * far, (units + 3) * far + 1)
    def _(at_step):
        turn_round(at_step)

    tots[pl.ds(me, 1)] = ss[...][None]
    totals = [
        pltpu.make_async_remote_copy(ss, tots.at[me], ts_sem.at[k], tr_sem.at[n - k], device_id={"dp": around[k]}, device_id_type=MESH)
        for k in range(1, n)
    ]
    for copy in totals:
        copy.start()
    for way in range(2):
        for s in range(far):
            g_copy(units - 1, s, way, s > 0).wait_send()
            e = around[far - s] if way == 0 else around[n - far + s]
            d_copy(lax.rem(e, far), way, s > 0).wait_send()
    for k in range(len(pieces)):
        for copy in moment_copies(k):
            copy.wait()
    for k in range(1, n):
        pltpu.make_async_remote_copy(ss, tots.at[around[k]], ts_sem.at[k], tr_sem.at[k], device_id={"dp": around[k]}, device_id_type=MESH).wait_recv()
    factor = jnp.minimum(1.0, 0.5 * lax.rsqrt(jnp.sum(tots[...], keepdims=True).reshape(1, 1) / count + 1e-30))

    def rows_of(i, origin, part=None):
        tall = full[i].shape[1] // n
        start = origin * tall
        if part is not None:
            tall //= 2
            start += part * tall
        return pl.ds(pl.multiple_of(start, tall), tall)

    def pass_on(k, s, way, coming=False):
        i, layer = pieces[k]
        back_by = s + coming
        origin = around[(n - back_by) % n] if way == 0 else around[back_by]
        here = full[i].at[layer, rows_of(i, origin, way if s == far - 1 else None), :]
        return pltpu.make_async_remote_copy(
            here, here, ag_send.at[way, s, k], ag_recv.at[way, s, k], device_id={"dp": towards[way]}, device_id_type=MESH)

    for k, (i, layer) in enumerate(pieces):
        def adamw(here, where_g, where_w):
            m_at, v_at = here, pl.ds(here.start + deep, here.size)
            g = own_g[i][(layer, *where_g)].astype(F32) * factor
            m = 0.9 * da[k, m_at, :] + 0.1 * g
            v = 0.95 * da[k, v_at, :] + 0.05 * g * g
            w = full[i][(layer, *where_w)].astype(F32)
            step = m * lax.rsqrt(v + 1e-8) + 0.1 * w
            da[k, m_at, :] = m
            da[k, v_at, :] = v
            full[i][(layer, *where_w)] = (w - 0.02 * step).astype(BF16)

        for b in range(far):
            here = pl.ds(b * rows, rows)
            if i == 2:
                adamw(here, (here, slice(None)), (pl.ds(pl.multiple_of(me * deep + b * rows, rows), rows), slice(None)))
            else:
                cols = pl.ds(b * d, d)
                adamw(here, (slice(None), cols), (pl.ds(pl.multiple_of(me * rows, rows), rows), cols))
        for way in range(2):
            pass_on(k, 0, way).start()

    for s in range(far):
        for k in range(len(pieces)):
            for way in range(2):
                pass_on(k, s, way, True).wait_recv()
                if s + 1 < far:
                    pass_on(k, s + 1, way).start()
    for copy in totals:
        copy.wait_send()
    for s in range(far):
        for k in range(len(pieces)):
            for way in range(2):
                pass_on(k, s, way).wait_send()


def flush_kernel(n, fg, fu, fd, wide, *refs):
    outs, sem = refs[:9], refs[9]
    layers, d = fg.shape[0], fg.shape[1]
    rows, far = d // n, n // 2
    deep = far * rows
    copies = []
    for k, (i, layer) in enumerate((i, layer) for layer in (1, 0) for i in range(3)):
        for c in range(2):
            out = outs[3 + 3 * c + i]
            if i == 2:
                copies.append((wide.at[k, pl.ds(c * deep, deep), :], out.at[layer]))
            else:
                copies += [(wide.at[k, pl.ds(c * deep + b * rows, rows), :], out.at[layer, :, pl.ds(b * d, d)]) for b in range(far)]
    copies += [(f.at[layer], out.at[layer]) for layer in range(layers) for f, out in zip((fg, fu, fd), outs)]
    copies = [pltpu.make_async_copy(*pair, sem.at[i]) for i, pair in enumerate(copies)]
    for copy in copies:
        copy.start()
    for copy in copies:
        copy.wait()


def train_step(x, dy, w, m, v, n):
    wg, wu, wd = w
    tokens, d = x.shape[1:]
    layers, _, f = wg.shape
    nt, nc = tokens // TT, f // FC
    far, rows = n // 2, d // n
    pieces = 3 * layers
    hbm = pl.BlockSpec(memory_space=pl.ANY)
    vmem = pl.BlockSpec(memory_space=pltpu.VMEM)
    shape = jax.ShapeDtypeStruct
    kept = [pltpu.VMEM(one.shape, BF16) for one in w] + [pltpu.VMEM((nt, TT, d), F32)]
    v_, dma = pltpu.VMEM, pltpu.SemaphoreType.DMA
    scratch = [
        v_((2, 2 * FC, d), BF16), v_((2, d, FC), BF16),
        v_((nt, TT, d), BF16), v_((nt, d, TT), BF16), v_((nt, TT, d), BF16), v_((nt, TT, d), BF16), v_((nt, d, TT), BF16),
        v_((3, TT, d), BF16), v_((TT, f), BF16), v_((TT, FC), BF16), v_((TT, FC), BF16), v_((TT, 2 * FC), BF16), v_((TT, 2 * FC), BF16),
        v_((UNITS_HELD, d, 2 * FC), F32), v_((UNITS_HELD, 2, d, LB), F32),
        v_((2, 2, far, 2, rows, FC), BF16), v_((2, far, 2, d // 2, LB), BF16), v_((2, far, 2, rows, FC), BF16), v_((2, far, 2, d // 2, LB), BF16),
        v_((layers, rows, f), BF16), v_((layers, rows, f), BF16), v_((layers, f // n, d), BF16), v_((8, LB), F32), v_((n, 8, LB), F32),
        dma((layers, 3)), dma((3,)), dma((nt,)), dma((2,)), dma((nt,)),
        dma((2, 2, far)), dma((2, far)), dma((2, far)), dma((2, far)), dma((n,)), dma((n,)),
        dma((pieces, n)), dma((2, far, pieces)), dma((2, far, pieces)),
    ]
    kept_bytes = 2 * sum(one.size for one in w) + 4 * tokens * d
    *new, wide, _, _ = pl.pallas_call(
        functools.partial(step_kernel, nt, nc, n, sum(one.size for one in w)),
        name="train_step",
        out_shape=kept + [shape((nc, nt, TT, 2 * FC), F32), shape((nt, d, TT), BF16)],
        in_specs=[hbm] * 11,
        out_specs=[vmem] * 4 + [hbm] * 2,
        scratch_shapes=scratch,
        compiler_params=pltpu.CompilerParams(vmem_limit_bytes=VMEM_BYTES - kept_bytes, collective_id=0, has_side_effects=True),
    )(x, dy, *w, *m, *v)
    copies = layers * (2 * (2 * far + 1) + 3)
    keep = lambda one: pltpu.with_memory_space_constraint(one, pltpu.VMEM)
    return tuple(pl.pallas_call(
        functools.partial(flush_kernel, n),
        name="flush",
        out_shape=[shape(one.shape, one.dtype) for group in (w, m, v) for one in group],
        in_specs=[vmem] * 4,
        out_specs=[hbm] * 9,
        scratch_shapes=[dma((copies,))],
        compiler_params=pltpu.CompilerParams(vmem_limit_bytes=1 << 20),
    )(*(keep(one) for one in (*new, wide))))


def solution(mesh):
    n = mesh.shape["dp"]

    def step(x, dy, *arrays):
        return train_step(x, dy, *(arrays[i:i + 3] for i in (0, 3, 6)), n)

    seq, rows = P(("rep", "dp"), None, None), P(None, "dp", None)
    return jax.shard_map(
        step,
        mesh=mesh,
        in_specs=(seq, seq) + (P(),) * 3 + (rows,) * 6,
        out_specs=(P("rep"),) * 3 + (P("rep", "dp"),) * 6,
        check_vma=False,
    )
```

```python
import functools

import jax
import jax.numpy as jnp
from jax import lax
from jax.experimental import pallas as pl
from jax.experimental.pallas import tpu as pltpu
from jax.sharding import PartitionSpec as P

F32, BF16 = jnp.float32, jnp.bfloat16
MESH = pl.DeviceIdType.MESH
TT = 512
LB = 128
FC = 2 * LB
UNITS_HELD = 7
VMEM_BYTES = 67_043_328


def dot(a, b):
    return jnp.dot(a, b, preferred_element_type=F32)


def rms(wide):
    return lax.rsqrt(jnp.mean(wide * wide, -1, keepdims=True) + 1e-6)


def sigmoid(g):
    return 0.5 * jnp.tanh(0.5 * g) + 0.5


def step_kernel(nt, nc, n, count, x_h, dy_h, wg_h, wu_h, wd_h, mg_h, mu_h, md_h, vg_h, vu_h, vd_h,
                fg, fu, fd, wide_ref, gu_h, a1t_h,
                wgut, wdt, a, at, h1, dy, dyt, hid, hd0, hd1, dgu0, dgu1,
                pg, pd, rg, sg, og, ou, od, ss, tots,
                sem_w, sem_x, sem_dy, sem_at, sem_gu, rg_sem, rd_sem, sg_sem, sd_sem, ts_sem, tr_sem, mv_sem, ag_send, ag_recv):
    half, far = nc // 2, n // 2
    units = 2 * nc
    rows = pg.shape[1] // n
    hds, dgus = (hd0, hd1), (dgu0, dgu1)
    full, own_g = (fg, fu, fd), (og, ou, od)
    da = wide_ref
    me = lax.axis_index("dp")
    around = [lax.rem(me + k, n) for k in range(n)]
    towards = (around[1], around[n - 1])

    def block(j):
        return 2 * lax.rem(j, half) + j // half

    def at_block(b):
        return pl.ds(b * LB if isinstance(b, int) else pl.multiple_of(b * LB, LB), LB)

    def x_copy(t):
        return pltpu.make_async_copy(x_h.at[0, pl.ds(t * TT, TT), :], a.at[t], sem_x.at[t])

    def dy_copy(t):
        return pltpu.make_async_copy(dy_h.at[0, pl.ds(t * TT, TT), :], dy.at[t], sem_dy.at[t])

    def w_copies(layer):
        return [pltpu.make_async_copy(h.at[layer], v.at[layer], sem_w.at[layer, i]) for i, (h, v) in enumerate(zip((wg_h, wu_h, wd_h), full))]

    x_copy(0).start()
    for copy in w_copies(0):
        copy.start()
    for t in range(nt):
        if t:
            x_copy(t).start()
        dy_copy(t).start()
    for copy in w_copies(1):
        copy.start()
    ss[...] = jnp.zeros_like(ss)

    def gu_out(t, j):
        return pltpu.make_async_copy(da.at[j], gu_h.at[j, t], sem_gu.at[j])

    def a1t_out(t):
        p = lax.rem(t, 2)
        return pltpu.make_async_copy(wgut.at[p], a1t_h.at[t], sem_at.at[p])

    def static_block(j):
        return 2 * (j % half) + j // half

    def down_part(part):
        some = range(part * half, (part + 1) * half)
        w = jnp.concatenate([fd[0, at_block(static_block(j) + s * nc), :] for j in some for s in range(2)], 0)
        return dot(jnp.concatenate([hid[b] for b in range(part * nc, (part + 1) * nc)], 1), w)

    def gate_up(j):
        cols = [at_block(static_block(j) + s * nc) for s in range(2)]
        gu = dot(dgu0[...], jnp.concatenate([f[0, :, c] for f in (fg, fu) for c in cols], 1))
        da[j] = gu
        g, u = gu[:, :FC], gu[:, FC:]
        h = (g * sigmoid(g) * u).astype(BF16)
        for s in range(2):
            hid[2 * j + s] = h[:, s * LB:(s + 1) * LB]

    def finish(t):
        y = pg[0] + down_part(1)
        h = (a[t].astype(F32) + y.astype(BF16).astype(F32)).astype(BF16)
        h1[t] = h
        wide = h.astype(F32)
        a2 = (wide * rms(wide)).astype(BF16)
        a[t] = a2
        at[t] = a2.T
        dyt[t] = dy[t].T

    def forward(t, follows):
        x_copy(t).wait()
        dy_copy(t).wait()
        if follows:
            for j in range(half):
                gu_out(t - 1, j).wait()

            @pl.when(t >= 2)
            def _():
                a1t_out(t - 2).wait()

            pg[0] = down_part(0)
        wide = a[t].astype(F32)
        a1 = (wide * rms(wide)).astype(BF16)
        dgu0[...] = a1
        wgut[lax.rem(t, 2)] = a1.T
        for j in range(half):
            gate_up(j)
        for j in range(half):
            gu_out(t, j).start()
        a1t_out(t).start()
        if follows:
            for j in range(half, nc):
                gu_out(t - 1, j).wait()
            finish(t - 1)
        for j in range(half, nc):
            gate_up(j)
        for j in range(half, nc):
            gu_out(t, j).start()

    for copy in w_copies(0):
        copy.wait()
    forward(0, False)

    @pl.loop(1, nt)
    def _(t):
        forward(t, True)

    pg[0] = down_part(0)
    finish(nt - 1)
    for j in range(nc):
        gu_out(nt - 1, j).wait()
    for t in (nt - 2, nt - 1):
        a1t_out(t).wait()
    for copy in w_copies(1):
        copy.wait()

    barrier = pltpu.get_barrier_semaphore()
    for k in range(1, n):
        pl.semaphore_signal(barrier, inc=1, device_id={"dp": around[k]}, device_id_type=MESH)

    def g_copy(u, s, way, both):
        part = (lambda ref: ref) if both else (lambda ref: ref.at[way])
        old, new = lax.rem(u, 2), lax.rem(u, 4)
        return pltpu.make_async_remote_copy(
            part(sg.at[way, old, s]), part(rg.at[way, new, s]), sg_sem.at[way, old, s], rg_sem.at[way, new, s],
            device_id={"dp": towards[way]}, device_id_type=MESH)

    tall = pd.shape[2] // 2

    def d_at(way, k, sent):
        return hid.at[(2 * sent + way) * far + k]

    def d_copy(j, way, both):
        k = lax.rem(j, far)
        part = (lambda ref: ref) if both else (lambda ref: ref.at[pl.ds(way * tall, tall), :])
        return pltpu.make_async_remote_copy(
            part(d_at(way, k, 1)), part(d_at(way, k, 0)), sd_sem.at[way, k], rd_sem.at[way, k],
            device_id={"dp": towards[way]}, device_id_type=MESH)

    def relay(u, s):
        j, slot, old, new = lax.rem(u, nc), lax.rem(u, UNITS_HELD), lax.rem(u, 2), lax.rem(u, 4)
        for way in range(2):
            e = around[far - s] if way == 0 else around[n - far + s]

            @pl.when(u > 1)
            def _():
                g_copy(u - 2, s, way, s > 0).wait_send()

            if s > 0:
                g_copy(u, s - 1, way, s > 1).wait_recv()
            for h in range(2):
                if s == 0 and h != way:
                    continue
                own = pg[slot, pl.ds(pl.multiple_of(e * rows, rows), rows), h * FC:(h + 1) * FC]
                if s > 1 or (s == 1 and h == way):
                    own += rg[way, new, s - 1, h].astype(F32)
                sg[way, old, s, h] = own.astype(BF16)
            g_copy(u, s, way, s > 0).start()

            @pl.when(lax.rem(e, far) == lax.rem(j, far))
            def _():
                k = lax.rem(j, far)

                @pl.when(u >= far)
                def _():
                    d_copy(j, way, s > 0).wait_send()

                if s > 0:
                    d_copy(j, way, s > 1).wait_recv()
                for h in range(2):
                    if s == 0 and h != way:
                        continue
                    part = pl.ds(h * tall, tall)
                    own = pd[slot, e // far, part, :]
                    if s > 1 or (s == 1 and h == way):
                        own += d_at(way, k, 0)[part, :].astype(F32)
                    d_at(way, k, 1)[part, :] = own.astype(BF16)
                d_copy(j, way, s > 0).start()

    def square(g):
        wide = g.astype(F32)
        ss[...] += jnp.sum((wide * wide).reshape(-1, *ss.shape), 0)

    def arrive(u):
        j, slot, old, layer = lax.rem(u, nc), lax.rem(u, UNITS_HELD), lax.rem(u, 4), 1 - u // nc
        k = lax.rem(j, far)
        for way in range(2):
            g_copy(u, far - 1, way, True).wait_recv()
        for h, out in enumerate((og, ou)):
            own = pg[slot, pl.ds(pl.multiple_of(me * rows, rows), rows), h * FC:(h + 1) * FC]
            own = (own + rg[0, old, far - 1, h].astype(F32) + rg[1, old, far - 1, h].astype(F32)).astype(BF16)
            for s in range(2):
                piece = own[:, s * LB:(s + 1) * LB]
                out[layer, :, at_block(block(j) + s * nc)] = piece
                square(piece)

        @pl.when(lax.rem(me, far) == k)
        def _():
            for way in range(2):
                d_copy(j, way, True).wait_recv()
            for h in range(2):
                part = pl.ds(h * tall, tall)
                own = pd[slot, me // far, part, :]
                own = own + d_at(0, k, 0)[part, :].astype(F32) + d_at(1, k, 0)[part, :].astype(F32)
                own = own.T.astype(BF16)
                od[layer, at_block(j // half), h * tall:(h + 1) * tall] = own
                for s in range(tall // LB):
                    square(own[:, s * LB:(s + 1) * LB])

    def turn_round(at_step):
        p, q = at_step // far, lax.rem(at_step, far)

        @pl.when((q == 0) & (p >= 6) & (p < units + 6))
        def _():
            arrive(p - 6)

        for when, s, lag in ((0, 0, 1), (1, 1, 2), (2, 2, 3), (3, 3, 4)):
            @pl.when((q == when) & (p >= lag) & (p < units + lag))
            def _(s=s, lag=lag):
                relay(p - lag, s)

    def elementwise(gu, dh, slot):
        g, u = gu[:, :FC], gu[:, FC:]
        sig = sigmoid(g)
        silu = g * sig
        hds[slot][...] = (silu * u).astype(BF16)
        dgus[slot][:, :FC] = (dh * u * (sig + silu * (1 - sig))).astype(BF16)
        dgus[slot][:, FC:] = (dh * silu).astype(BF16)

    def back(u, t, slot, first=None):
        k = lax.rem(u, UNITS_HELD)
        keep = (lambda old: old) if first is None else (lambda old: jnp.where(first, jnp.zeros_like(old), old))
        pg[k] = keep(pg[k]) + dot(at[t], dgus[slot][...])
        hd = dot(dyt[t], hds[slot][...])
        for s in range(2):
            pd[k, s] = keep(pd[k, s]) + hd[:, s * LB:(s + 1) * LB]

    def to_states(u, t, slot):
        old = jnp.where(u == 0, jnp.zeros(da.shape[1:], F32), da[t])
        da[t] = old + dot(dgus[slot][...], wgut[lax.rem(u, 2)])

    def turn(layer, j, t):
        p = lax.rem(j, 2)
        if layer:
            for i, f in enumerate((fg, fu)):
                s = lax.rem(t, 2)
                wgut[p, pl.ds(pl.multiple_of(i * FC + s * LB, LB), LB), :] = f[layer, :, at_block(block(j) + s * nc)].T
        s = lax.rem(t, 2)
        wdt[p, :, at_block(s)] = fd[layer, at_block(block(j) + s * nc), :].T

    def clear():
        for h, g in zip(hds, dgus):
            h[...] = jnp.zeros_like(h)
            g[...] = jnp.zeros_like(g)

    per_chunk = nt // 2
    pl.semaphore_wait(barrier, n - 1)

    for t in range(2):
        turn(1, 0, t)
    clear()

    def front2(j, t, slot):
        cols = [at_block(block(j) + s * nc) for s in range(2)]
        gu = dot(a[t], jnp.concatenate([f[1, :, c] for f in (fg, fu) for c in cols], 1))
        elementwise(gu, dot(dy[t], wdt[lax.rem(j, 2)]).astype(BF16).astype(F32), slot)

    @pl.loop(0, nc * per_chunk)
    def _(i):
        j, t = i // per_chunk, 2 * lax.rem(i, per_chunk)
        k = jnp.maximum(2 * i - 1, 0)
        front2(j, t, 0)
        back(k // nt, lax.rem(k, nt), 1)
        to_states(k // nt, lax.rem(k, nt), 1)
        for s in range(2):
            turn(1, jnp.minimum(j + 1, nc - 1), t + s)
        front2(j, t + 1, 1)
        back(j, t, 0, t == 0)
        to_states(j, t, 0)
        turn_round(i)

    back(nc - 1, nt - 1, 1)
    to_states(nc - 1, nt - 1, 1)

    def a1t_in(t):
        return pltpu.make_async_copy(a1t_h.at[t], at.at[t], sem_dy.at[t])

    def gu_in(i):
        return pltpu.make_async_copy(gu_h.at[i // nt, lax.rem(i, nt)], da.at[lax.rem(i, nt)], sem_gu.at[lax.rem(i, nt)])

    for t in range(nt):
        a1t_in(t).start()

    @pl.loop(0, nt)
    def _(t):
        wide = h1[t].astype(F32)
        r = rms(wide)
        da_t = da[t].astype(BF16).astype(F32)
        dn = da_t * r - wide * (r * r * r * jnp.mean(da_t * wide, -1, keepdims=True))
        dh1 = (dy[t].astype(F32) + dn).astype(BF16)
        dy[t] = dh1
        dyt[t] = dh1.T
        gu_in(t).start()
        a1t_in(t).wait()

    for t in range(2):
        turn(0, 0, t)
    clear()

    def front1(j, t, slot):
        elementwise(da[t], dot(dy[t], wdt[lax.rem(j, 2)]).astype(BF16).astype(F32), slot)

    @pl.loop(0, nc * per_chunk)
    def _(i):
        j, t = i // per_chunk, 2 * lax.rem(i, per_chunk)
        k = jnp.maximum(2 * i - 1, 0)
        for s in range(2):
            gu_in(2 * i + s).wait()
        front1(j, t, 0)
        back(nc + k // nt, lax.rem(k, nt), 1)
        for s in range(2):
            turn(0, jnp.minimum(j + 1, nc - 1), t + s)
        front1(j, t + 1, 1)
        back(nc + j, t, 0, t == 0)

        @pl.when(j + 1 < nc)
        def _():
            for s in range(2):
                gu_in(2 * i + s + nt).start()

        turn_round(nc * per_chunk + i)

    back(2 * nc - 1, nt - 1, 1)

    pieces = [(i, layer) for layer in (1, 0) for i in range(3)]
    d = h1.shape[2]
    deep = n // 2 * rows

    def moment_copies(k):
        i, layer = pieces[k]
        made = []
        for c, h in enumerate(((mg_h, mu_h, md_h)[i], (vg_h, vu_h, vd_h)[i])):
            if i == 2:
                made.append(pltpu.make_async_copy(h.at[layer], da.at[k, pl.ds(c * deep, deep), :], mv_sem.at[k, c]))
            else:
                for b in range(far):
                    made.append(pltpu.make_async_copy(
                        h.at[layer, :, pl.ds(b * d, d)], da.at[k, pl.ds(c * deep + b * rows, rows), :], mv_sem.at[k, c * far + b]))
        return made

    for k in range(len(pieces)):
        for copy in moment_copies(k):
            copy.start()

    @pl.loop(units * far, (units + 5) * far + 1)
    def _(at_step):
        turn_round(at_step)

    tots[pl.ds(me, 1)] = ss[...][None]
    totals = [
        pltpu.make_async_remote_copy(ss, tots.at[me], ts_sem.at[k], tr_sem.at[n - k], device_id={"dp": around[k]}, device_id_type=MESH)
        for k in range(1, n)
    ]
    for copy in totals:
        copy.start()
    for way in range(2):
        for s in range(far):
            for u in (units - 2, units - 1):
                g_copy(u, s, way, s > 0).wait_send()
            e = around[far - s] if way == 0 else around[n - far + s]
            d_copy(lax.rem(e, far), way, s > 0).wait_send()
    for k in range(len(pieces)):
        for copy in moment_copies(k):
            copy.wait()
    for k in range(1, n):
        pltpu.make_async_remote_copy(ss, tots.at[around[k]], ts_sem.at[k], tr_sem.at[k], device_id={"dp": around[k]}, device_id_type=MESH).wait_recv()
    factor = jnp.minimum(1.0, 0.5 * lax.rsqrt(jnp.sum(tots[...], keepdims=True).reshape(1, 1) / count + 1e-30))

    def rows_of(i, origin, part=None):
        tall = full[i].shape[1] // n
        start = origin * tall
        if part is not None:
            tall //= 2
            start += part * tall
        return pl.ds(pl.multiple_of(start, tall), tall)

    def pass_on(k, s, way, coming=False):
        i, layer = pieces[k]
        back_by = s + coming
        origin = around[(n - back_by) % n] if way == 0 else around[back_by]
        here = full[i].at[layer, rows_of(i, origin, way if s == far - 1 else None), :]
        return pltpu.make_async_remote_copy(
            here, here, ag_send.at[way, s, k], ag_recv.at[way, s, k], device_id={"dp": towards[way]}, device_id_type=MESH)

    for k, (i, layer) in enumerate(pieces):
        def adamw(here, where_g, where_w):
            m_at, v_at = here, pl.ds(here.start + deep, here.size)
            g = own_g[i][(layer, *where_g)].astype(F32) * factor
            m = 0.9 * da[k, m_at, :] + 0.1 * g
            v = 0.95 * da[k, v_at, :] + 0.05 * g * g
            w = full[i][(layer, *where_w)].astype(F32)
            step = m * lax.rsqrt(v + 1e-8) + 0.1 * w
            da[k, m_at, :] = m
            da[k, v_at, :] = v
            full[i][(layer, *where_w)] = (w - 0.02 * step).astype(BF16)

        for b in range(far):
            here = pl.ds(b * rows, rows)
            if i == 2:
                adamw(here, (here, slice(None)), (pl.ds(pl.multiple_of(me * deep + b * rows, rows), rows), slice(None)))
            else:
                cols = pl.ds(b * d, d)
                adamw(here, (slice(None), cols), (pl.ds(pl.multiple_of(me * rows, rows), rows), cols))
        for way in range(2):
            pass_on(k, 0, way).start()

    for s in range(far):
        for k in range(len(pieces)):
            for way in range(2):
                pass_on(k, s, way, True).wait_recv()
                if s + 1 < far:
                    pass_on(k, s + 1, way).start()
    for copy in totals:
        copy.wait_send()
    for s in range(far):
        for k in range(len(pieces)):
            for way in range(2):
                pass_on(k, s, way).wait_send()


def flush_kernel(n, fg, fu, fd, wide, *refs):
    outs, sem = refs[:9], refs[9]
    layers, d = fg.shape[0], fg.shape[1]
    rows, far = d // n, n // 2
    deep = far * rows
    copies = []
    for k, (i, layer) in enumerate((i, layer) for layer in (1, 0) for i in range(3)):
        for c in range(2):
            out = outs[3 + 3 * c + i]
            if i == 2:
                copies.append((wide.at[k, pl.ds(c * deep, deep), :], out.at[layer]))
            else:
                copies += [(wide.at[k, pl.ds(c * deep + b * rows, rows), :], out.at[layer, :, pl.ds(b * d, d)]) for b in range(far)]
    copies += [(f.at[layer], out.at[layer]) for layer in range(layers) for f, out in zip((fg, fu, fd), outs)]
    copies = [pltpu.make_async_copy(*pair, sem.at[i]) for i, pair in enumerate(copies)]
    for copy in copies:
        copy.start()
    for copy in copies:
        copy.wait()


def train_step(x, dy, w, m, v, n):
    wg, wu, wd = w
    tokens, d = x.shape[1:]
    layers, _, f = wg.shape
    nt, nc = tokens // TT, f // FC
    far, rows = n // 2, d // n
    pieces = 3 * layers
    hbm = pl.BlockSpec(memory_space=pl.ANY)
    vmem = pl.BlockSpec(memory_space=pltpu.VMEM)
    shape = jax.ShapeDtypeStruct
    kept = [pltpu.VMEM(one.shape, BF16) for one in w] + [pltpu.VMEM((nt, TT, d), F32)]
    v_, dma = pltpu.VMEM, pltpu.SemaphoreType.DMA
    scratch = [
        v_((2, 2 * FC, d), BF16), v_((2, d, FC), BF16),
        v_((nt, TT, d), BF16), v_((nt, d, TT), BF16), v_((nt, TT, d), BF16), v_((nt, TT, d), BF16), v_((nt, d, TT), BF16),
        v_((2 * nc, TT, LB), BF16), v_((TT, FC), BF16), v_((TT, FC), BF16), v_((TT, 2 * FC), BF16), v_((TT, 2 * FC), BF16),
        v_((UNITS_HELD, d, 2 * FC), F32), v_((UNITS_HELD, 2, d, LB), F32),
        v_((2, 4, far, 2, rows, FC), BF16), v_((2, 2, far, 2, rows, FC), BF16),
        v_((layers, rows, f), BF16), v_((layers, rows, f), BF16), v_((layers, f // n, d), BF16), v_((8, LB), F32), v_((n, 8, LB), F32),
        dma((layers, 3)), dma((nt,)), dma((nt,)), dma((2,)), dma((nt,)),
        dma((2, 4, far)), dma((2, far)), dma((2, 2, far)), dma((2, far)), dma((n,)), dma((n,)),
        dma((pieces, n)), dma((2, far, pieces)), dma((2, far, pieces)),
    ]
    kept_bytes = 2 * sum(one.size for one in w) + 4 * tokens * d
    *new, wide, _, _ = pl.pallas_call(
        functools.partial(step_kernel, nt, nc, n, sum(one.size for one in w)),
        name="train_step",
        out_shape=kept + [shape((nc, nt, TT, 2 * FC), F32), shape((nt, d, TT), BF16)],
        in_specs=[hbm] * 11,
        out_specs=[vmem] * 4 + [hbm] * 2,
        scratch_shapes=scratch,
        compiler_params=pltpu.CompilerParams(vmem_limit_bytes=VMEM_BYTES - kept_bytes, collective_id=0, has_side_effects=True),
    )(x, dy, *w, *m, *v)
    copies = layers * (2 * (2 * far + 1) + 3)
    keep = lambda one: pltpu.with_memory_space_constraint(one, pltpu.VMEM)
    return tuple(pl.pallas_call(
        functools.partial(flush_kernel, n),
        name="flush",
        out_shape=[shape(one.shape, one.dtype) for group in (w, m, v) for one in group],
        in_specs=[vmem] * 4,
        out_specs=[hbm] * 9,
        scratch_shapes=[dma((copies,))],
        compiler_params=pltpu.CompilerParams(vmem_limit_bytes=1 << 20),
    )(*(keep(one) for one in (*new, wide))))


def solution(mesh):
    n = mesh.shape["dp"]

    def step(x, dy, *arrays):
        return train_step(x, dy, *(arrays[i:i + 3] for i in (0, 3, 6)), n)

    seq, rows = P(("rep", "dp"), None, None), P(None, "dp", None)
    return jax.shard_map(
        step,
        mesh=mesh,
        in_specs=(seq, seq) + (P(),) * 3 + (rows,) * 6,
        out_specs=(P("rep"),) * 3 + (P("rep", "dp"),) * 6,
        check_vma=False,
    )
```

```python
import functools

import jax
import jax.numpy as jnp
from jax import lax
from jax.experimental import pallas as pl
from jax.experimental.pallas import tpu as pltpu
from jax.sharding import PartitionSpec as P

F32, BF16 = jnp.float32, jnp.bfloat16
MESH = pl.DeviceIdType.MESH
TT = 512
LB = 128
FC = 2 * LB
UNITS_HELD = 7
VMEM_BYTES = 67_043_328


def dot(a, b):
    return jnp.dot(a, b, preferred_element_type=F32)


def rms(wide):
    return lax.rsqrt(jnp.mean(wide * wide, -1, keepdims=True) + 1e-6)


def sigmoid(g):
    return 0.5 * jnp.tanh(0.5 * g) + 0.5


def step_kernel(nt, nc, n, count, x_h, dy_h, wg_h, wu_h, wd_h, mg_h, mu_h, md_h, vg_h, vu_h, vd_h,
                fg, fu, fd, wide_ref, gu_h, a1t_h,
                wgut, wdt, a, at, h1, dy, dyt, hid, hd0, hd1, dgu0, dgu1,
                pg, pd, rg, sg, og, ou, od, ss, tots,
                sem_w, sem_x, sem_dy, sem_at, sem_gu, rg_sem, rd_sem, sg_sem, sd_sem, ts_sem, tr_sem, mv_sem, ag_send, ag_recv):
    half, far = nc // 2, n // 2
    units = 2 * nc
    rows = pg.shape[1] // n
    hds, dgus = (hd0, hd1), (dgu0, dgu1)
    full, own_g = (fg, fu, fd), (og, ou, od)
    da = wide_ref
    me = lax.axis_index("dp")
    around = [lax.rem(me + k, n) for k in range(n)]
    towards = (around[1], around[n - 1])

    def block(j):
        return 2 * lax.rem(j, half) + j // half

    def at_block(b):
        return pl.ds(b * LB if isinstance(b, int) else pl.multiple_of(b * LB, LB), LB)

    def x_copy(t):
        return pltpu.make_async_copy(x_h.at[0, pl.ds(t * TT, TT), :], a.at[t], sem_x.at[t])

    def dy_copy(t):
        return pltpu.make_async_copy(dy_h.at[0, pl.ds(t * TT, TT), :], dy.at[t], sem_dy.at[t])

    def w_copies(layer):
        return [pltpu.make_async_copy(h.at[layer], v.at[layer], sem_w.at[layer, i]) for i, (h, v) in enumerate(zip((wg_h, wu_h, wd_h), full))]

    x_copy(0).start()
    for copy in w_copies(0):
        copy.start()
    ss[...] = jnp.zeros_like(ss)

    def gu_out(t, j):
        return pltpu.make_async_copy(da.at[j], gu_h.at[j, t], sem_gu.at[j])

    def a1t_out(t):
        p = lax.rem(t, 2)
        return pltpu.make_async_copy(wgut.at[p], a1t_h.at[t], sem_at.at[p])

    def static_block(j):
        return 2 * (j % half) + j // half

    def down_part(part):
        some = range(part * half, (part + 1) * half)
        w = jnp.concatenate([fd[0, at_block(static_block(j) + s * nc), :] for j in some for s in range(2)], 0)
        return dot(jnp.concatenate([hid[b] for b in range(part * nc, (part + 1) * nc)], 1), w)

    def gate_up(j):
        cols = [at_block(static_block(j) + s * nc) for s in range(2)]
        gu = dot(dgu0[...], jnp.concatenate([f[0, :, c] for f in (fg, fu) for c in cols], 1))
        da[j] = gu
        g, u = gu[:, :FC], gu[:, FC:]
        h = (g * sigmoid(g) * u).astype(BF16)
        for s in range(2):
            hid[2 * j + s] = h[:, s * LB:(s + 1) * LB]

    def finish(t):
        h = (a[t].astype(F32) + pg[0].astype(BF16).astype(F32)).astype(BF16)
        h1[t] = h
        wide = h.astype(F32)
        a2 = (wide * rms(wide)).astype(BF16)
        a[t] = a2
        at[t] = a2.T

    def forward(t, follows):
        x_copy(t).wait()
        if follows:
            dy_copy(t - 1).wait()
            for j in range(half):
                gu_out(t - 1, j).wait()

            @pl.when(t >= 2)
            def _():
                a1t_out(t - 2).wait()

            pg[0] = down_part(0)
        wide = a[t].astype(F32)
        a1 = (wide * rms(wide)).astype(BF16)
        dgu0[...] = a1
        wgut[lax.rem(t, 2)] = a1.T
        if follows:
            dyt[t - 1] = dy[t - 1].T
        for j in range(half):
            gate_up(j)
        for j in range(half):
            gu_out(t, j).start()
        a1t_out(t).start()
        if follows:
            for j in range(half, nc):
                gu_out(t - 1, j).wait()
            pg[0] += down_part(1)
        for j in range(half, nc):
            gate_up(j)
        if follows:
            finish(t - 1)
        for j in range(half, nc):
            gu_out(t, j).start()

    for copy in w_copies(0):
        copy.wait()
    dy_copy(0).start()
    for t in range(1, nt):
        x_copy(t).start()
        dy_copy(t).start()
    for copy in w_copies(1):
        copy.start()
    forward(0, False)

    @pl.loop(1, nt)
    def _(t):
        forward(t, True)

    pg[0] = down_part(0) + down_part(1)
    dy_copy(nt - 1).wait()
    dyt[nt - 1] = dy[nt - 1].T
    finish(nt - 1)
    for j in range(nc):
        gu_out(nt - 1, j).wait()
    for t in (nt - 2, nt - 1):
        a1t_out(t).wait()
    for copy in w_copies(1):
        copy.wait()

    barrier = pltpu.get_barrier_semaphore()
    for k in range(1, n):
        pl.semaphore_signal(barrier, inc=1, device_id={"dp": around[k]}, device_id_type=MESH)

    def g_copy(u, s, way, both):
        part = (lambda ref: ref) if both else (lambda ref: ref.at[way])
        old, new = lax.rem(u, 2), lax.rem(u, 4)
        return pltpu.make_async_remote_copy(
            part(sg.at[way, old, s]), part(rg.at[way, new, s]), sg_sem.at[way, old, s], rg_sem.at[way, new, s],
            device_id={"dp": towards[way]}, device_id_type=MESH)

    tall = pd.shape[2] // 2

    def d_at(way, k, sent):
        return hid.at[(2 * sent + way) * far + k]

    def d_copy(j, way, both):
        k = lax.rem(j, far)
        part = (lambda ref: ref) if both else (lambda ref: ref.at[pl.ds(way * tall, tall), :])
        return pltpu.make_async_remote_copy(
            part(d_at(way, k, 1)), part(d_at(way, k, 0)), sd_sem.at[way, k], rd_sem.at[way, k],
            device_id={"dp": towards[way]}, device_id_type=MESH)

    def relay(u, s):
        j, slot, old, new = lax.rem(u, nc), lax.rem(u, UNITS_HELD), lax.rem(u, 2), lax.rem(u, 4)
        for way in range(2):
            e = around[far - s] if way == 0 else around[n - far + s]

            @pl.when(u > 1)
            def _():
                g_copy(u - 2, s, way, s > 0).wait_send()

            if s > 0:
                g_copy(u, s - 1, way, s > 1).wait_recv()
            for h in range(2):
                if s == 0 and h != way:
                    continue
                own = pg[slot, pl.ds(pl.multiple_of(e * rows, rows), rows), h * FC:(h + 1) * FC]
                if s > 1 or (s == 1 and h == way):
                    own += rg[way, new, s - 1, h].astype(F32)
                sg[way, old, s, h] = own.astype(BF16)
            g_copy(u, s, way, s > 0).start()

            @pl.when(lax.rem(e, far) == lax.rem(j, far))
            def _():
                k = lax.rem(j, far)

                @pl.when(u >= far)
                def _():
                    d_copy(j, way, s > 0).wait_send()

                if s > 0:
                    d_copy(j, way, s > 1).wait_recv()
                for h in range(2):
                    if s == 0 and h != way:
                        continue
                    part = pl.ds(h * tall, tall)
                    own = pd[slot, e // far, part, :]
                    if s > 1 or (s == 1 and h == way):
                        own += d_at(way, k, 0)[part, :].astype(F32)
                    d_at(way, k, 1)[part, :] = own.astype(BF16)
                d_copy(j, way, s > 0).start()

    def square(g):
        wide = g.astype(F32)
        ss[...] += jnp.sum((wide * wide).reshape(-1, *ss.shape), 0)

    def arrive(u):
        j, slot, old, layer = lax.rem(u, nc), lax.rem(u, UNITS_HELD), lax.rem(u, 4), 1 - u // nc
        k = lax.rem(j, far)
        for way in range(2):
            g_copy(u, far - 1, way, True).wait_recv()
        for h, out in enumerate((og, ou)):
            own = pg[slot, pl.ds(pl.multiple_of(me * rows, rows), rows), h * FC:(h + 1) * FC]
            own = (own + rg[0, old, far - 1, h].astype(F32) + rg[1, old, far - 1, h].astype(F32)).astype(BF16)
            for s in range(2):
                piece = own[:, s * LB:(s + 1) * LB]
                out[layer, :, at_block(block(j) + s * nc)] = piece
                square(piece)

        @pl.when(lax.rem(me, far) == k)
        def _():
            for way in range(2):
                d_copy(j, way, True).wait_recv()
            for h in range(2):
                part = pl.ds(h * tall, tall)
                own = pd[slot, me // far, part, :]
                own = own + d_at(0, k, 0)[part, :].astype(F32) + d_at(1, k, 0)[part, :].astype(F32)
                own = own.T.astype(BF16)
                od[layer, at_block(j // half), h * tall:(h + 1) * tall] = own
                for s in range(tall // LB):
                    square(own[:, s * LB:(s + 1) * LB])

    def turn_round(at_step):
        p, q = at_step // far, lax.rem(at_step, far)

        @pl.when((q == 0) & (p >= 6) & (p < units + 6))
        def _():
            arrive(p - 6)

        for when, s, lag in ((0, 0, 1), (1, 1, 2), (2, 2, 3), (3, 3, 4)):
            @pl.when((q == when) & (p >= lag) & (p < units + lag))
            def _(s=s, lag=lag):
                relay(p - lag, s)

    def elementwise(gu, dh, slot):
        g, u = gu[:, :FC], gu[:, FC:]
        sig = sigmoid(g)
        silu = g * sig
        hds[slot][...] = (silu * u).astype(BF16)
        dgus[slot][:, :FC] = (dh * u * (sig + silu * (1 - sig))).astype(BF16)
        dgus[slot][:, FC:] = (dh * silu).astype(BF16)

    def keep_from(first):
        return (lambda old: old) if first is None else (lambda old: jnp.where(first, jnp.zeros_like(old), old))

    def back_g(u, t, slot, first=None):
        k, keep = lax.rem(u, UNITS_HELD), keep_from(first)
        pg[k] = keep(pg[k]) + dot(at[t], dgus[slot][...])

    def back_d(u, t, slot, first=None):
        k, keep = lax.rem(u, UNITS_HELD), keep_from(first)
        hd = dot(dyt[t], hds[slot][...])
        for s in range(2):
            pd[k, s] = keep(pd[k, s]) + hd[:, s * LB:(s + 1) * LB]

    def to_states(u, t, slot):
        old = jnp.where(u == 0, jnp.zeros(da.shape[1:], F32), da[t])
        da[t] = old + dot(dgus[slot][...], wgut[lax.rem(u, 2)])

    def turn(layer, j, t):
        p = lax.rem(j, 2)
        if layer:
            for i, f in enumerate((fg, fu)):
                s = lax.rem(t, 2)
                wgut[p, pl.ds(pl.multiple_of(i * FC + s * LB, LB), LB), :] = f[layer, :, at_block(block(j) + s * nc)].T
        s = lax.rem(t, 2)
        wdt[p, :, at_block(s)] = fd[layer, at_block(block(j) + s * nc), :].T

    def clear():
        for h, g in zip(hds, dgus):
            h[...] = jnp.zeros_like(h)
            g[...] = jnp.zeros_like(g)

    per_chunk = nt // 2
    pl.semaphore_wait(barrier, n - 1)

    for t in range(2):
        turn(1, 0, t)
    clear()

    def front2(j, t, slot):
        cols = [at_block(block(j) + s * nc) for s in range(2)]
        gu = dot(a[t], jnp.concatenate([f[1, :, c] for f in (fg, fu) for c in cols], 1))
        elementwise(gu, dot(dy[t], wdt[lax.rem(j, 2)]).astype(BF16).astype(F32), slot)

    @pl.loop(0, nc * per_chunk)
    def _(i):
        j, t = i // per_chunk, 2 * lax.rem(i, per_chunk)
        k = jnp.maximum(2 * i - 1, 0)
        jk, tk, jn = k // nt, lax.rem(k, nt), jnp.minimum(j + 1, nc - 1)
        to_states(jk, tk, 1)
        back_d(jk, tk, 1)
        front2(j, t, 0)
        to_states(j, t, 0)
        back_g(jk, tk, 1)
        turn(1, jn, t + 1)
        back_d(j, t, 0, t == 0)
        turn(1, jn, t)
        front2(j, t + 1, 1)
        back_g(j, t, 0, t == 0)
        turn_round(i)

    to_states(nc - 1, nt - 1, 1)
    back_d(nc - 1, nt - 1, 1)
    back_g(nc - 1, nt - 1, 1)

    def a1t_in(t):
        return pltpu.make_async_copy(a1t_h.at[t], at.at[t], sem_dy.at[t])

    def gu_in(i):
        return pltpu.make_async_copy(gu_h.at[i // nt, lax.rem(i, nt)], da.at[lax.rem(i, nt)], sem_gu.at[lax.rem(i, nt)])

    for t in range(nt):
        a1t_in(t).start()

    @pl.loop(0, nt)
    def _(t):
        wide = h1[t].astype(F32)
        r = rms(wide)
        da_t = da[t].astype(BF16).astype(F32)
        dn = da_t * r - wide * (r * r * r * jnp.mean(da_t * wide, -1, keepdims=True))
        dh1 = (dy[t].astype(F32) + dn).astype(BF16)
        dy[t] = dh1
        dyt[t] = dh1.T
        gu_in(t).start()
        a1t_in(t).wait()

    for t in range(2):
        turn(0, 0, t)
    clear()

    def front1(j, t, slot):
        elementwise(da[t], dot(dy[t], wdt[lax.rem(j, 2)]).astype(BF16).astype(F32), slot)

    @pl.loop(0, nc * per_chunk)
    def _(i):
        j, t = i // per_chunk, 2 * lax.rem(i, per_chunk)
        k = jnp.maximum(2 * i - 1, 0)
        for s in range(2):
            gu_in(2 * i + s).wait()
        jk, tk, jn = nc + k // nt, lax.rem(k, nt), jnp.minimum(j + 1, nc - 1)
        turn(0, jn, t + 1)
        back_d(jk, tk, 1)
        turn(0, jn, t)
        back_g(jk, tk, 1)
        front1(j, t, 0)
        back_d(nc + j, t, 0, t == 0)
        front1(j, t + 1, 1)
        back_g(nc + j, t, 0, t == 0)

        @pl.when(j + 1 < nc)
        def _():
            for s in range(2):
                gu_in(2 * i + s + nt).start()

        turn_round(nc * per_chunk + i)

    back_d(2 * nc - 1, nt - 1, 1)
    back_g(2 * nc - 1, nt - 1, 1)

    pieces = [(i, layer) for layer in (1, 0) for i in range(3)]
    d = h1.shape[2]
    deep = n // 2 * rows

    def moment_copies(k):
        i, layer = pieces[k]
        made = []
        for c, h in enumerate(((mg_h, mu_h, md_h)[i], (vg_h, vu_h, vd_h)[i])):
            if i == 2:
                made.append(pltpu.make_async_copy(h.at[layer], da.at[k, pl.ds(c * deep, deep), :], mv_sem.at[k, c]))
            else:
                for b in range(far):
                    made.append(pltpu.make_async_copy(
                        h.at[layer, :, pl.ds(b * d, d)], da.at[k, pl.ds(c * deep + b * rows, rows), :], mv_sem.at[k, c * far + b]))
        return made

    for k in range(len(pieces)):
        for copy in moment_copies(k):
            copy.start()

    @pl.loop(units * far, (units + 5) * far + 1)
    def _(at_step):
        turn_round(at_step)

    tots[pl.ds(me, 1)] = ss[...][None]
    totals = [
        pltpu.make_async_remote_copy(ss, tots.at[me], ts_sem.at[k], tr_sem.at[n - k], device_id={"dp": around[k]}, device_id_type=MESH)
        for k in range(1, n)
    ]
    for copy in totals:
        copy.start()
    for way in range(2):
        for s in range(far):
            for u in (units - 2, units - 1):
                g_copy(u, s, way, s > 0).wait_send()
            e = around[far - s] if way == 0 else around[n - far + s]
            d_copy(lax.rem(e, far), way, s > 0).wait_send()
    for k in range(len(pieces)):
        for copy in moment_copies(k):
            copy.wait()
    for k in range(1, n):
        pltpu.make_async_remote_copy(ss, tots.at[around[k]], ts_sem.at[k], tr_sem.at[k], device_id={"dp": around[k]}, device_id_type=MESH).wait_recv()
    factor = jnp.minimum(1.0, 0.5 * lax.rsqrt(jnp.sum(tots[...], keepdims=True).reshape(1, 1) / count + 1e-30))

    def rows_of(i, origin, part=None):
        tall = full[i].shape[1] // n
        start = origin * tall
        if part is not None:
            tall //= 2
            start += part * tall
        return pl.ds(pl.multiple_of(start, tall), tall)

    def pass_on(k, s, way, coming=False):
        i, layer = pieces[k]
        back_by = s + coming
        origin = around[(n - back_by) % n] if way == 0 else around[back_by]
        here = full[i].at[layer, rows_of(i, origin, way if s == far - 1 else None), :]
        return pltpu.make_async_remote_copy(
            here, here, ag_send.at[way, s, k], ag_recv.at[way, s, k], device_id={"dp": towards[way]}, device_id_type=MESH)

    for k, (i, layer) in enumerate(pieces):
        def adamw(here, where_g, where_w):
            m_at, v_at = here, pl.ds(here.start + deep, here.size)
            g = own_g[i][(layer, *where_g)].astype(F32) * factor
            m = 0.9 * da[k, m_at, :] + 0.1 * g
            v = 0.95 * da[k, v_at, :] + 0.05 * g * g
            w = full[i][(layer, *where_w)].astype(F32)
            step = m * lax.rsqrt(v + 1e-8) + 0.1 * w
            da[k, m_at, :] = m
            da[k, v_at, :] = v
            full[i][(layer, *where_w)] = (w - 0.02 * step).astype(BF16)

        for b in range(far):
            here = pl.ds(b * rows, rows)
            if i == 2:
                adamw(here, (here, slice(None)), (pl.ds(pl.multiple_of(me * deep + b * rows, rows), rows), slice(None)))
            else:
                cols = pl.ds(b * d, d)
                adamw(here, (slice(None), cols), (pl.ds(pl.multiple_of(me * rows, rows), rows), cols))
        for way in range(2):
            pass_on(k, 0, way).start()

    for s in range(far):
        for k in range(len(pieces)):
            for way in range(2):
                pass_on(k, s, way, True).wait_recv()
                if s + 1 < far:
                    pass_on(k, s + 1, way).start()
    for copy in totals:
        copy.wait_send()
    for s in range(far):
        for k in range(len(pieces)):
            for way in range(2):
                pass_on(k, s, way).wait_send()


def flush_kernel(n, fg, fu, fd, wide, *refs):
    outs, sem = refs[:9], refs[9]
    layers, d = fg.shape[0], fg.shape[1]
    rows, far = d // n, n // 2
    deep = far * rows
    copies = []
    for k, (i, layer) in enumerate((i, layer) for layer in (1, 0) for i in range(3)):
        for c in range(2):
            out = outs[3 + 3 * c + i]
            if i == 2:
                copies.append((wide.at[k, pl.ds(c * deep, deep), :], out.at[layer]))
            else:
                copies += [(wide.at[k, pl.ds(c * deep + b * rows, rows), :], out.at[layer, :, pl.ds(b * d, d)]) for b in range(far)]
    copies += [(f.at[layer], out.at[layer]) for layer in range(layers) for f, out in zip((fg, fu, fd), outs)]
    copies = [pltpu.make_async_copy(*pair, sem.at[i]) for i, pair in enumerate(copies)]
    for copy in copies:
        copy.start()
    for copy in copies:
        copy.wait()


def train_step(x, dy, w, m, v, n):
    wg, wu, wd = w
    tokens, d = x.shape[1:]
    layers, _, f = wg.shape
    nt, nc = tokens // TT, f // FC
    far, rows = n // 2, d // n
    pieces = 3 * layers
    hbm = pl.BlockSpec(memory_space=pl.ANY)
    vmem = pl.BlockSpec(memory_space=pltpu.VMEM)
    shape = jax.ShapeDtypeStruct
    kept = [pltpu.VMEM(one.shape, BF16) for one in w] + [pltpu.VMEM((nt, TT, d), F32)]
    v_, dma = pltpu.VMEM, pltpu.SemaphoreType.DMA
    scratch = [
        v_((2, 2 * FC, d), BF16), v_((2, d, FC), BF16),
        v_((nt, TT, d), BF16), v_((nt, d, TT), BF16), v_((nt, TT, d), BF16), v_((nt, TT, d), BF16), v_((nt, d, TT), BF16),
        v_((2 * nc, TT, LB), BF16), v_((TT, FC), BF16), v_((TT, FC), BF16), v_((TT, 2 * FC), BF16), v_((TT, 2 * FC), BF16),
        v_((UNITS_HELD, d, 2 * FC), F32), v_((UNITS_HELD, 2, d, LB), F32),
        v_((2, 4, far, 2, rows, FC), BF16), v_((2, 2, far, 2, rows, FC), BF16),
        v_((layers, rows, f), BF16), v_((layers, rows, f), BF16), v_((layers, f // n, d), BF16), v_((8, LB), F32), v_((n, 8, LB), F32),
        dma((layers, 3)), dma((nt,)), dma((nt,)), dma((2,)), dma((nt,)),
        dma((2, 4, far)), dma((2, far)), dma((2, 2, far)), dma((2, far)), dma((n,)), dma((n,)),
        dma((pieces, n)), dma((2, far, pieces)), dma((2, far, pieces)),
    ]
    kept_bytes = 2 * sum(one.size for one in w) + 4 * tokens * d
    *new, wide, _, _ = pl.pallas_call(
        functools.partial(step_kernel, nt, nc, n, sum(one.size for one in w)),
        name="train_step",
        out_shape=kept + [shape((nc, nt, TT, 2 * FC), F32), shape((nt, d, TT), BF16)],
        in_specs=[hbm] * 11,
        out_specs=[vmem] * 4 + [hbm] * 2,
        scratch_shapes=scratch,
        compiler_params=pltpu.CompilerParams(vmem_limit_bytes=VMEM_BYTES - kept_bytes, collective_id=0, has_side_effects=True),
    )(x, dy, *w, *m, *v)
    copies = layers * (2 * (2 * far + 1) + 3)
    keep = lambda one: pltpu.with_memory_space_constraint(one, pltpu.VMEM)
    return tuple(pl.pallas_call(
        functools.partial(flush_kernel, n),
        name="flush",
        out_shape=[shape(one.shape, one.dtype) for group in (w, m, v) for one in group],
        in_specs=[vmem] * 4,
        out_specs=[hbm] * 9,
        scratch_shapes=[dma((copies,))],
        compiler_params=pltpu.CompilerParams(vmem_limit_bytes=1 << 20),
    )(*(keep(one) for one in (*new, wide))))


def solution(mesh):
    n = mesh.shape["dp"]

    def step(x, dy, *arrays):
        return train_step(x, dy, *(arrays[i:i + 3] for i in (0, 3, 6)), n)

    seq, rows = P(("rep", "dp"), None, None), P(None, "dp", None)
    return jax.shard_map(
        step,
        mesh=mesh,
        in_specs=(seq, seq) + (P(),) * 3 + (rows,) * 6,
        out_specs=(P("rep"),) * 3 + (P("rep", "dp"),) * 6,
        check_vma=False,
    )
```

```python
import functools

import jax
import jax.numpy as jnp
from jax import lax
from jax.experimental import pallas as pl
from jax.experimental.pallas import tpu as pltpu
from jax.sharding import PartitionSpec as P

F32, BF16 = jnp.float32, jnp.bfloat16
MESH = pl.DeviceIdType.MESH
TT = 512
LB = 128
FC = 2 * LB
UNITS_HELD = 7
VMEM_BYTES = 67_043_328


def dot(a, b):
    return jnp.dot(a, b, preferred_element_type=F32)


def rms(wide):
    return lax.rsqrt(jnp.mean(wide * wide, -1, keepdims=True) + 1e-6)


def sigmoid(g):
    return 0.5 * jnp.tanh(0.5 * g) + 0.5


def step_kernel(nt, nc, n, count, x_h, dy_h, wg_h, wu_h, wd_h, mg_h, mu_h, md_h, vg_h, vu_h, vd_h,
                fg, fu, fd, wide_ref, gu_h, a1t_h,
                wgut, wdt, a, at, h1, dy, dyt, hid, hd0, hd1, dgu0, dgu1,
                pg, pd, rg, sg, og, ou, od, ss, tots,
                sem_w, sem_x, sem_dy, sem_at, sem_gu, sem_gi, rg_sem, rd_sem, sg_sem, sd_sem, ts_sem, tr_sem, mv_sem, ag_send, ag_recv):
    half, far = nc // 2, n // 2
    units = 2 * nc
    rows = pg.shape[1] // n
    hds, dgus = (hd0, hd1), (dgu0, dgu1)
    full, own_g = (fg, fu, fd), (og, ou, od)
    da = wide_ref
    me = lax.axis_index("dp")
    around = [lax.rem(me + k, n) for k in range(n)]
    towards = (around[1], around[n - 1])

    def block(j):
        return 2 * lax.rem(j, half) + j // half

    def at_block(b):
        return pl.ds(b * LB if isinstance(b, int) else pl.multiple_of(b * LB, LB), LB)

    def x_copy(t):
        return pltpu.make_async_copy(x_h.at[0, pl.ds(t * TT, TT), :], a.at[t], sem_x.at[t])

    def dy_copy(t):
        return pltpu.make_async_copy(dy_h.at[0, pl.ds(t * TT, TT), :], dy.at[t], sem_dy.at[t])

    def w_copies(layer):
        return [pltpu.make_async_copy(h.at[layer], v.at[layer], sem_w.at[layer, i]) for i, (h, v) in enumerate(zip((wg_h, wu_h, wd_h), full))]

    x_copy(0).start()
    for copy in w_copies(0):
        copy.start()
    ss[...] = jnp.zeros_like(ss)

    def staged(odd, j):
        if not odd:
            return [(da.at[j], 0, 2 * FC)]
        if j < UNITS_HELD:
            return [(pg.at[j], 0, 2 * FC)]
        return [(pd.at[UNITS_HELD - 2 + i // 2, i % 2], i * LB, LB) for i in range(2 * FC // LB)]

    def gu_out(t, odd, j):
        return [pltpu.make_async_copy(ref, gu_h.at[j, t, :, pl.ds(at_, width)], sem_gu.at[odd * (nc + 3) + j + i])
                for i, (ref, at_, width) in enumerate(staged(odd, j))]

    def gu_out_all(t, odd):
        return [copy for j in range(nc) for copy in gu_out(t, odd, j)]

    def a1t_out(t):
        p = lax.rem(t, 2)
        return pltpu.make_async_copy(wgut.at[p], a1t_h.at[t], sem_at.at[p])

    def static_block(j):
        return 2 * (j % half) + j // half

    def down():
        w = jnp.concatenate([fd[0, at_block(static_block(j) + s * nc), :] for j in range(nc) for s in range(2)], 0)
        return dot(jnp.concatenate([hid[b] for b in range(2 * nc)], 1), w)

    def gate_up(odd, j):
        cols = [at_block(static_block(j) + s * nc) for s in range(2)]
        gu = dot(dgu0[...], jnp.concatenate([f[0, :, c] for f in (fg, fu) for c in cols], 1))
        for ref, at_, width in staged(odd, j):
            ref[...] = gu[:, at_:at_ + width]
        g, u = gu[:, :FC], gu[:, FC:]
        h = (g * sigmoid(g) * u).astype(BF16)
        for s in range(2):
            hid[2 * j + s] = h[:, s * LB:(s + 1) * LB]

    def finish(t, y):
        h = (a[t].astype(F32) + y.astype(BF16).astype(F32)).astype(BF16)
        h1[t] = h
        wide = h.astype(F32)
        a2 = (wide * rms(wide)).astype(BF16)
        a[t] = a2
        at[t] = a2.T
        dyt[t] = dy[t].T

    def forward(t, odd, follows):
        x_copy(t).wait()
        if follows:
            dy_copy(t - 1).wait()

        @pl.when(t >= 2)
        def _():
            a1t_out(t - 2).wait()
            for copy in gu_out_all(t - 2, odd):
                copy.wait()

        if follows:
            y = down()
        wide = a[t].astype(F32)
        a1 = (wide * rms(wide)).astype(BF16)
        dgu0[...] = a1
        wgut[lax.rem(t, 2)] = a1.T
        for j in range(nc):
            gate_up(odd, j)
            if j == half and follows:
                finish(t - 1, y)
        for copy in gu_out_all(t, odd):
            copy.start()
        a1t_out(t).start()

    for copy in w_copies(0):
        copy.wait()
    dy_copy(0).start()
    for t in range(1, nt):
        x_copy(t).start()
        dy_copy(t).start()
    for copy in w_copies(1):
        copy.start()
    forward(0, 0, False)

    @pl.loop(0, nt // 2 - 1)
    def _(i):
        forward(2 * i + 1, 1, True)
        forward(2 * i + 2, 0, True)

    forward(nt - 1, 1, True)
    dy_copy(nt - 1).wait()
    finish(nt - 1, down())
    for copy in gu_out_all(nt - 2, 0):
        copy.wait()
    for t in (nt - 2, nt - 1):
        a1t_out(t).wait()
    for copy in gu_out(nt - 1, 1, 0):
        copy.wait()
    for copy in w_copies(1):
        copy.wait()

    barrier = pltpu.get_barrier_semaphore()
    for k in range(1, n):
        pl.semaphore_signal(barrier, inc=1, device_id={"dp": around[k]}, device_id_type=MESH)

    def g_copy(u, s, way, both):
        part = (lambda ref: ref) if both else (lambda ref: ref.at[way])
        old, new = lax.rem(u, 2), lax.rem(u, 4)
        return pltpu.make_async_remote_copy(
            part(sg.at[way, old, s]), part(rg.at[way, new, s]), sg_sem.at[way, old, s], rg_sem.at[way, new, s],
            device_id={"dp": towards[way]}, device_id_type=MESH)

    tall = pd.shape[2] // 2

    def d_at(way, k, sent):
        return hid.at[(2 * sent + way) * far + k]

    def d_copy(j, way, both):
        k = lax.rem(j, far)
        part = (lambda ref: ref) if both else (lambda ref: ref.at[pl.ds(way * tall, tall), :])
        return pltpu.make_async_remote_copy(
            part(d_at(way, k, 1)), part(d_at(way, k, 0)), sd_sem.at[way, k], rd_sem.at[way, k],
            device_id={"dp": towards[way]}, device_id_type=MESH)

    def relay(u, s):
        j, slot, old, new = lax.rem(u, nc), lax.rem(u, UNITS_HELD), lax.rem(u, 2), lax.rem(u, 4)
        for way in range(2):
            e = around[far - s] if way == 0 else around[n - far + s]

            @pl.when(u > 1)
            def _():
                g_copy(u - 2, s, way, s > 0).wait_send()

            if s > 0:
                g_copy(u, s - 1, way, s > 1).wait_recv()
            for h in range(2):
                if s == 0 and h != way:
                    continue
                own = pg[slot, pl.ds(pl.multiple_of(e * rows, rows), rows), h * FC:(h + 1) * FC]
                if s > 1 or (s == 1 and h == way):
                    own += rg[way, new, s - 1, h].astype(F32)
                sg[way, old, s, h] = own.astype(BF16)
            g_copy(u, s, way, s > 0).start()

            @pl.when(lax.rem(e, far) == lax.rem(j, far))
            def _():
                k = lax.rem(j, far)

                @pl.when(u >= far)
                def _():
                    d_copy(j, way, s > 0).wait_send()

                if s > 0:
                    d_copy(j, way, s > 1).wait_recv()
                for h in range(2):
                    if s == 0 and h != way:
                        continue
                    part = pl.ds(h * tall, tall)
                    own = pd[slot, e // far, part, :]
                    if s > 1 or (s == 1 and h == way):
                        own += d_at(way, k, 0)[part, :].astype(F32)
                    d_at(way, k, 1)[part, :] = own.astype(BF16)
                d_copy(j, way, s > 0).start()

    def square(g):
        wide = g.astype(F32)
        ss[...] += jnp.sum((wide * wide).reshape(-1, *ss.shape), 0)

    def arrive(u):
        j, slot, old, layer = lax.rem(u, nc), lax.rem(u, UNITS_HELD), lax.rem(u, 4), 1 - u // nc
        k = lax.rem(j, far)
        for way in range(2):
            g_copy(u, far - 1, way, True).wait_recv()
        for h, out in enumerate((og, ou)):
            own = pg[slot, pl.ds(pl.multiple_of(me * rows, rows), rows), h * FC:(h + 1) * FC]
            own = (own + rg[0, old, far - 1, h].astype(F32) + rg[1, old, far - 1, h].astype(F32)).astype(BF16)
            for s in range(2):
                piece = own[:, s * LB:(s + 1) * LB]
                out[layer, :, at_block(block(j) + s * nc)] = piece
                square(piece)

        @pl.when(lax.rem(me, far) == k)
        def _():
            for way in range(2):
                d_copy(j, way, True).wait_recv()
            for h in range(2):
                part = pl.ds(h * tall, tall)
                own = pd[slot, me // far, part, :]
                own = own + d_at(0, k, 0)[part, :].astype(F32) + d_at(1, k, 0)[part, :].astype(F32)
                own = own.T.astype(BF16)
                od[layer, at_block(j // half), h * tall:(h + 1) * tall] = own
                for s in range(tall // LB):
                    square(own[:, s * LB:(s + 1) * LB])

    def turn_round(at_step):
        p, q = at_step // far, lax.rem(at_step, far)

        @pl.when((q == 0) & (p >= 6) & (p < units + 6))
        def _():
            arrive(p - 6)

        for when, s, lag in ((0, 0, 1), (1, 1, 2), (2, 2, 3), (3, 3, 4)):
            @pl.when((q == when) & (p >= lag) & (p < units + lag))
            def _(s=s, lag=lag):
                relay(p - lag, s)

    def elementwise(gu, dh, slot):
        g, u = gu[:, :FC], gu[:, FC:]
        sig = sigmoid(g)
        silu = g * sig
        hds[slot][...] = (silu * u).astype(BF16)
        dgus[slot][:, :FC] = (dh * u * (sig + silu * (1 - sig))).astype(BF16)
        dgus[slot][:, FC:] = (dh * silu).astype(BF16)

    def keep_from(first):
        return (lambda old: old) if first is None else (lambda old: jnp.where(first, jnp.zeros_like(old), old))

    def back_g(u, t, slot, first=None):
        k, keep = lax.rem(u, UNITS_HELD), keep_from(first)
        pg[k] = keep(pg[k]) + dot(at[t], dgus[slot][...])

    def back_d(u, t, slot, first=None):
        k, keep = lax.rem(u, UNITS_HELD), keep_from(first)
        hd = dot(dyt[t], hds[slot][...])
        for s in range(2):
            pd[k, s] = keep(pd[k, s]) + hd[:, s * LB:(s + 1) * LB]

    def to_states(u, t, slot):
        old = jnp.where(u == 0, jnp.zeros(da.shape[1:], F32), da[t])
        da[t] = old + dot(dgus[slot][...], wgut[lax.rem(u, 2)])

    def turn(layer, j, t):
        p = lax.rem(j, 2)
        if layer:
            for i, f in enumerate((fg, fu)):
                s = lax.rem(t, 2)
                wgut[p, pl.ds(pl.multiple_of(i * FC + s * LB, LB), LB), :] = f[layer, :, at_block(block(j) + s * nc)].T
        s = lax.rem(t, 2)
        wdt[p, :, at_block(s)] = fd[layer, at_block(block(j) + s * nc), :].T

    def clear():
        for h, g in zip(hds, dgus):
            h[...] = jnp.zeros_like(h)
            g[...] = jnp.zeros_like(g)

    per_chunk = nt // 2
    pl.semaphore_wait(barrier, n - 1)

    for t in range(2):
        turn(1, 0, t)
    clear()

    def front2(j, t, slot):
        cols = [at_block(block(j) + s * nc) for s in range(2)]
        gu = dot(a[t], jnp.concatenate([f[1, :, c] for f in (fg, fu) for c in cols], 1))
        elementwise(gu, dot(dy[t], wdt[lax.rem(j, 2)]).astype(BF16).astype(F32), slot)

    @pl.loop(0, nc * per_chunk)
    def _(i):
        j, t = i // per_chunk, 2 * lax.rem(i, per_chunk)
        k = jnp.maximum(2 * i - 1, 0)
        @pl.when(i == 2)
        def _():
            for copy in [c for k in range(1, nc) for c in gu_out(nt - 1, 1, k)]:
                copy.wait()

        jk, tk, jn = k // nt, lax.rem(k, nt), jnp.minimum(j + 1, nc - 1)
        to_states(jk, tk, 1)
        back_d(jk, tk, 1)
        front2(j, t, 0)
        to_states(j, t, 0)
        back_g(jk, tk, 1)
        turn(1, jn, t + 1)
        back_d(j, t, 0, t == 0)
        turn(1, jn, t)
        front2(j, t + 1, 1)
        back_g(j, t, 0, t == 0)
        turn_round(i)

    to_states(nc - 1, nt - 1, 1)
    back_d(nc - 1, nt - 1, 1)
    back_g(nc - 1, nt - 1, 1)

    def a1t_in(t):
        return pltpu.make_async_copy(a1t_h.at[t], at.at[t], sem_dy.at[t])

    def gu_in(i):
        return pltpu.make_async_copy(gu_h.at[i // nt, lax.rem(i, nt)], da.at[lax.rem(i, nt)], sem_gi.at[lax.rem(i, nt)])

    for t in range(nt):
        a1t_in(t).start()

    @pl.loop(0, nt)
    def _(t):
        wide = h1[t].astype(F32)
        r = rms(wide)
        da_t = da[t].astype(BF16).astype(F32)
        dn = da_t * r - wide * (r * r * r * jnp.mean(da_t * wide, -1, keepdims=True))
        dh1 = (dy[t].astype(F32) + dn).astype(BF16)
        dy[t] = dh1
        dyt[t] = dh1.T
        gu_in(t).start()
        a1t_in(t).wait()

    for t in range(2):
        turn(0, 0, t)
    clear()

    def front1(j, t, slot):
        elementwise(da[t], dot(dy[t], wdt[lax.rem(j, 2)]).astype(BF16).astype(F32), slot)

    @pl.loop(0, nc * per_chunk)
    def _(i):
        j, t = i // per_chunk, 2 * lax.rem(i, per_chunk)
        k = jnp.maximum(2 * i - 1, 0)
        for s in range(2):
            gu_in(2 * i + s).wait()
        jk, tk, jn = nc + k // nt, lax.rem(k, nt), jnp.minimum(j + 1, nc - 1)
        turn(0, jn, t + 1)
        back_d(jk, tk, 1)
        turn(0, jn, t)
        back_g(jk, tk, 1)
        front1(j, t, 0)
        back_d(nc + j, t, 0, t == 0)
        front1(j, t + 1, 1)
        back_g(nc + j, t, 0, t == 0)

        @pl.when(j + 1 < nc)
        def _():
            for s in range(2):
                gu_in(2 * i + s + nt).start()

        turn_round(nc * per_chunk + i)

    back_d(2 * nc - 1, nt - 1, 1)
    back_g(2 * nc - 1, nt - 1, 1)

    pieces = [(i, layer) for layer in (1, 0) for i in range(3)]
    d = h1.shape[2]
    deep = n // 2 * rows

    def moment_copies(k):
        i, layer = pieces[k]
        made = []
        for c, h in enumerate(((mg_h, mu_h, md_h)[i], (vg_h, vu_h, vd_h)[i])):
            if i == 2:
                made.append(pltpu.make_async_copy(h.at[layer], da.at[k, pl.ds(c * deep, deep), :], mv_sem.at[k, c]))
            else:
                for b in range(far):
                    made.append(pltpu.make_async_copy(
                        h.at[layer, :, pl.ds(b * d, d)], da.at[k, pl.ds(c * deep + b * rows, rows), :], mv_sem.at[k, c * far + b]))
        return made

    for k in range(len(pieces)):
        for copy in moment_copies(k):
            copy.start()

    @pl.loop(units * far, (units + 5) * far + 1)
    def _(at_step):
        turn_round(at_step)

    tots[pl.ds(me, 1)] = ss[...][None]
    totals = [
        pltpu.make_async_remote_copy(ss, tots.at[me], ts_sem.at[k], tr_sem.at[n - k], device_id={"dp": around[k]}, device_id_type=MESH)
        for k in range(1, n)
    ]
    for copy in totals:
        copy.start()
    for way in range(2):
        for s in range(far):
            for u in (units - 2, units - 1):
                g_copy(u, s, way, s > 0).wait_send()
            e = around[far - s] if way == 0 else around[n - far + s]
            d_copy(lax.rem(e, far), way, s > 0).wait_send()
    for k in range(len(pieces)):
        for copy in moment_copies(k):
            copy.wait()
    for k in range(1, n):
        pltpu.make_async_remote_copy(ss, tots.at[around[k]], ts_sem.at[k], tr_sem.at[k], device_id={"dp": around[k]}, device_id_type=MESH).wait_recv()
    factor = jnp.minimum(1.0, 0.5 * lax.rsqrt(jnp.sum(tots[...], keepdims=True).reshape(1, 1) / count + 1e-30))

    def rows_of(i, origin, part=None):
        tall = full[i].shape[1] // n
        start = origin * tall
        if part is not None:
            tall //= 2
            start += part * tall
        return pl.ds(pl.multiple_of(start, tall), tall)

    def pass_on(k, s, way, coming=False):
        i, layer = pieces[k]
        back_by = s + coming
        origin = around[(n - back_by) % n] if way == 0 else around[back_by]
        here = full[i].at[layer, rows_of(i, origin, way if s == far - 1 else None), :]
        return pltpu.make_async_remote_copy(
            here, here, ag_send.at[way, s, k], ag_recv.at[way, s, k], device_id={"dp": towards[way]}, device_id_type=MESH)

    for k, (i, layer) in enumerate(pieces):
        def adamw(here, where_g, where_w):
            m_at, v_at = here, pl.ds(here.start + deep, here.size)
            g = own_g[i][(layer, *where_g)].astype(F32) * factor
            m = 0.9 * da[k, m_at, :] + 0.1 * g
            v = 0.95 * da[k, v_at, :] + 0.05 * g * g
            w = full[i][(layer, *where_w)].astype(F32)
            step = m * lax.rsqrt(v + 1e-8) + 0.1 * w
            da[k, m_at, :] = m
            da[k, v_at, :] = v
            full[i][(layer, *where_w)] = (w - 0.02 * step).astype(BF16)

        for b in range(far):
            here = pl.ds(b * rows, rows)
            if i == 2:
                adamw(here, (here, slice(None)), (pl.ds(pl.multiple_of(me * deep + b * rows, rows), rows), slice(None)))
            else:
                cols = pl.ds(b * d, d)
                adamw(here, (slice(None), cols), (pl.ds(pl.multiple_of(me * rows, rows), rows), cols))
        for way in range(2):
            pass_on(k, 0, way).start()

    for s in range(far):
        for k in range(len(pieces)):
            for way in range(2):
                pass_on(k, s, way, True).wait_recv()
                if s + 1 < far:
                    pass_on(k, s + 1, way).start()
    for copy in totals:
        copy.wait_send()
    for s in range(far):
        for k in range(len(pieces)):
            for way in range(2):
                pass_on(k, s, way).wait_send()


def flush_kernel(n, fg, fu, fd, wide, *refs):
    outs, sem = refs[:9], refs[9]
    layers, d = fg.shape[0], fg.shape[1]
    rows, far = d // n, n // 2
    deep = far * rows
    copies = []
    for k, (i, layer) in enumerate((i, layer) for layer in (1, 0) for i in range(3)):
        for c in range(2):
            out = outs[3 + 3 * c + i]
            if i == 2:
                copies.append((wide.at[k, pl.ds(c * deep, deep), :], out.at[layer]))
            else:
                copies += [(wide.at[k, pl.ds(c * deep + b * rows, rows), :], out.at[layer, :, pl.ds(b * d, d)]) for b in range(far)]
    copies += [(f.at[layer], out.at[layer]) for layer in range(layers) for f, out in zip((fg, fu, fd), outs)]
    copies = [pltpu.make_async_copy(*pair, sem.at[i]) for i, pair in enumerate(copies)]
    for copy in copies:
        copy.start()
    for copy in copies:
        copy.wait()


def train_step(x, dy, w, m, v, n):
    wg, wu, wd = w
    tokens, d = x.shape[1:]
    layers, _, f = wg.shape
    nt, nc = tokens // TT, f // FC
    far, rows = n // 2, d // n
    pieces = 3 * layers
    hbm = pl.BlockSpec(memory_space=pl.ANY)
    vmem = pl.BlockSpec(memory_space=pltpu.VMEM)
    shape = jax.ShapeDtypeStruct
    kept = [pltpu.VMEM(one.shape, BF16) for one in w] + [pltpu.VMEM((nt, TT, d), F32)]
    v_, dma = pltpu.VMEM, pltpu.SemaphoreType.DMA
    scratch = [
        v_((2, 2 * FC, d), BF16), v_((2, d, FC), BF16),
        v_((nt, TT, d), BF16), v_((nt, d, TT), BF16), v_((nt, TT, d), BF16), v_((nt, TT, d), BF16), v_((nt, d, TT), BF16),
        v_((2 * nc, TT, LB), BF16), v_((TT, FC), BF16), v_((TT, FC), BF16), v_((TT, 2 * FC), BF16), v_((TT, 2 * FC), BF16),
        v_((UNITS_HELD, d, 2 * FC), F32), v_((UNITS_HELD, 2, d, LB), F32),
        v_((2, 4, far, 2, rows, FC), BF16), v_((2, 2, far, 2, rows, FC), BF16),
        v_((layers, rows, f), BF16), v_((layers, rows, f), BF16), v_((layers, f // n, d), BF16), v_((8, LB), F32), v_((n, 8, LB), F32),
        dma((layers, 3)), dma((nt,)), dma((nt,)), dma((2,)), dma((2 * nc + 6,)), dma((nt,)),
        dma((2, 4, far)), dma((2, far)), dma((2, 2, far)), dma((2, far)), dma((n,)), dma((n,)),
        dma((pieces, n)), dma((2, far, pieces)), dma((2, far, pieces)),
    ]
    kept_bytes = 2 * sum(one.size for one in w) + 4 * tokens * d
    *new, wide, _, _ = pl.pallas_call(
        functools.partial(step_kernel, nt, nc, n, sum(one.size for one in w)),
        name="train_step",
        out_shape=kept + [shape((nc, nt, TT, 2 * FC), F32), shape((nt, d, TT), BF16)],
        in_specs=[hbm] * 11,
        out_specs=[vmem] * 4 + [hbm] * 2,
        scratch_shapes=scratch,
        compiler_params=pltpu.CompilerParams(vmem_limit_bytes=VMEM_BYTES - kept_bytes, collective_id=0, has_side_effects=True),
    )(x, dy, *w, *m, *v)
    copies = layers * (2 * (2 * far + 1) + 3)
    keep = lambda one: pltpu.with_memory_space_constraint(one, pltpu.VMEM)
    return tuple(pl.pallas_call(
        functools.partial(flush_kernel, n),
        name="flush",
        out_shape=[shape(one.shape, one.dtype) for group in (w, m, v) for one in group],
        in_specs=[vmem] * 4,
        out_specs=[hbm] * 9,
        scratch_shapes=[dma((copies,))],
        compiler_params=pltpu.CompilerParams(vmem_limit_bytes=1 << 20),
    )(*(keep(one) for one in (*new, wide))))


def solution(mesh):
    n = mesh.shape["dp"]

    def step(x, dy, *arrays):
        return train_step(x, dy, *(arrays[i:i + 3] for i in (0, 3, 6)), n)

    seq, rows = P(("rep", "dp"), None, None), P(None, "dp", None)
    return jax.shard_map(
        step,
        mesh=mesh,
        in_specs=(seq, seq) + (P(),) * 3 + (rows,) * 6,
        out_specs=(P("rep"),) * 3 + (P("rep", "dp"),) * 6,
        check_vma=False,
    )
```

```python
import functools

import jax
import jax.numpy as jnp
from jax import lax
from jax.experimental import pallas as pl
from jax.experimental.pallas import tpu as pltpu
from jax.sharding import PartitionSpec as P

F32, BF16 = jnp.float32, jnp.bfloat16
MESH = pl.DeviceIdType.MESH
TT = 512
LB = 128
FC = 2 * LB
RECEIVED = 6
UNITS_HELD = 7
VMEM_BYTES = 67_043_328
PLACES = (
    (4, 8, 13, 16, 20, 25, 28, 33, 40, 44, 48, 52, 56, 61, 64),
    (6, 11, 16, 19, 23, 28, 35, 39, 46, 48, 54, 57, 60, 66),
    (9, 14, 18, 24, 26, 31, 41, 45, 51, 53, 59, 63, 64),
    (12, 17, 21, 29, 30, 36, 48, 50, 56, 61, 65),
    (18, 20, 31, 37, 41, 49, 53, 56, 63),
)
LAST = (
    ("g", 9, 4), ("g", 15, 0), ("g", 11, 3), ("g", 12, 3), ("d", 15, 0), ("d", 9, 4), ("d", 11, 3), ("d", 12, 3), ("d", 14, 1),
    ("d", 13, 2), ("g", 14, 1), ("g", 10, 4), ("d", 10, 4), ("g", 15, 1), ("g", 13, 2), ("g", 11, 4), ("g", 12, 4), ("d", 15, 1),
    ("d", 14, 2), ("g", 14, 2), ("d", 11, 4), ("g", 15, 2), ("d", 13, 3), ("d", 12, 4), ("g", 13, 3), ("d", 15, 2), ("d", 14, 3),
    ("g", 14, 3), ("g", 15, 3), ("d", 15, 3), ("d", 13, 4), ("g", 13, 4), ("d", 14, 4), ("g", 14, 4), ("g", 15, 4), ("d", 15, 4),
)


def dot(a, b):
    return jnp.dot(a, b, preferred_element_type=F32)


def rms(wide):
    return lax.rsqrt(jnp.mean(wide * wide, -1, keepdims=True) + 1e-6)


def sigmoid(g):
    return 0.5 * jnp.tanh(0.5 * g) + 0.5


def step_kernel(nt, nc, n, count, x_h, dy_h, wg_h, wu_h, wd_h, mg_h, mu_h, md_h, vg_h, vu_h, vd_h,
                fg, fu, fd, wide_ref, gu_h, a1t_h,
                wgut, wdt, a, at, h1, dy, dyt, hid, hd0, hd1, dgu0, dgu1,
                pg, pd, rg, sg, og, ou, od, ss, tots,
                sem_w, sem_x, sem_dy, sem_at, sem_gu, sem_gi, rg_sem, rd_sem, sg_sem, sd_sem, ts_sem, tr_sem, mv_sem, ag_send, ag_recv):
    half, far = nc // 2, n // 2
    units = 2 * nc
    rows = pg.shape[1] // n
    hds, dgus = (hd0, hd1), (dgu0, dgu1)
    full, own_g = (fg, fu, fd), (og, ou, od)
    da = wide_ref
    me = lax.axis_index("dp")
    around = [lax.rem(me + k, n) for k in range(n)]
    towards = (around[1], around[n - 1])

    def block(j):
        return 2 * lax.rem(j, half) + j // half

    def at_block(b):
        return pl.ds(b * LB if isinstance(b, int) else pl.multiple_of(b * LB, LB), LB)

    def x_copy(t):
        return pltpu.make_async_copy(x_h.at[0, pl.ds(t * TT, TT), :], a.at[t], sem_x.at[t])

    def dy_copy(t):
        return pltpu.make_async_copy(dy_h.at[0, pl.ds(t * TT, TT), :], dy.at[t], sem_dy.at[t])

    def w_copies(layer):
        return [pltpu.make_async_copy(h.at[layer], v.at[layer], sem_w.at[layer, i]) for i, (h, v) in enumerate(zip((wg_h, wu_h, wd_h), full))]

    x_copy(0).start()
    for copy in w_copies(0):
        copy.start()
    ss[...] = jnp.zeros_like(ss)

    def staged(odd, j):
        if not odd:
            return [(da.at[j], 0, 2 * FC)]
        if j < UNITS_HELD:
            return [(pg.at[j], 0, 2 * FC)]
        return [(pd.at[UNITS_HELD - 2 + i // 2, i % 2], i * LB, LB) for i in range(2 * FC // LB)]

    def gu_out(t, odd, j):
        return [pltpu.make_async_copy(ref, gu_h.at[j, t, :, pl.ds(at_, width)], sem_gu.at[odd * (nc + 3) + j + i])
                for i, (ref, at_, width) in enumerate(staged(odd, j))]

    def gu_out_all(t, odd):
        return [copy for j in range(nc) for copy in gu_out(t, odd, j)]

    def a1t_out(t):
        p = lax.rem(t, 2)
        return pltpu.make_async_copy(wgut.at[p], a1t_h.at[t], sem_at.at[p])

    def static_block(j):
        return 2 * (j % half) + j // half

    def down():
        w = jnp.concatenate([fd[0, at_block(static_block(j) + s * nc), :] for j in range(nc) for s in range(2)], 0)
        return dot(jnp.concatenate([hid[b] for b in range(2 * nc)], 1), w)

    def gate_up(odd, j):
        cols = [at_block(static_block(j) + s * nc) for s in range(2)]
        gu = dot(dgu0[...], jnp.concatenate([f[0, :, c] for f in (fg, fu) for c in cols], 1))
        for ref, at_, width in staged(odd, j):
            ref[...] = gu[:, at_:at_ + width]
        g, u = gu[:, :FC], gu[:, FC:]
        h = (g * sigmoid(g) * u).astype(BF16)
        for s in range(2):
            hid[2 * j + s] = h[:, s * LB:(s + 1) * LB]

    def finish(t, y):
        h = (a[t].astype(F32) + y.astype(BF16).astype(F32)).astype(BF16)
        h1[t] = h
        wide = h.astype(F32)
        a2 = (wide * rms(wide)).astype(BF16)
        a[t] = a2
        at[t] = a2.T
        dyt[t] = dy[t].T

    def forward(t, odd, follows):
        x_copy(t).wait()
        if follows:
            dy_copy(t - 1).wait()

        @pl.when(t >= 2)
        def _():
            a1t_out(t - 2).wait()
            for copy in gu_out_all(t - 2, odd):
                copy.wait()

        if follows:
            y = down()
        wide = a[t].astype(F32)
        a1 = (wide * rms(wide)).astype(BF16)
        dgu0[...] = a1
        wgut[lax.rem(t, 2)] = a1.T
        for j in range(nc):
            gate_up(odd, j)
            if j == half and follows:
                finish(t - 1, y)
        for copy in gu_out_all(t, odd):
            copy.start()
        a1t_out(t).start()

    for copy in w_copies(0):
        copy.wait()
    dy_copy(0).start()
    for t in range(1, nt):
        x_copy(t).start()
        dy_copy(t).start()
    for copy in w_copies(1):
        copy.start()
    forward(0, 0, False)

    @pl.loop(0, nt // 2 - 1)
    def _(i):
        forward(2 * i + 1, 1, True)
        forward(2 * i + 2, 0, True)

    forward(nt - 1, 1, True)
    dy_copy(nt - 1).wait()
    finish(nt - 1, down())
    for copy in gu_out_all(nt - 2, 0):
        copy.wait()
    for t in (nt - 2, nt - 1):
        a1t_out(t).wait()
    for copy in gu_out(nt - 1, 1, 0):
        copy.wait()
    for copy in w_copies(1):
        copy.wait()

    barrier = pltpu.get_barrier_semaphore()
    for k in range(1, n):
        pl.semaphore_signal(barrier, inc=1, device_id={"dp": around[k]}, device_id_type=MESH)

    def g_copy(u, s, way, both):
        part = (lambda ref: ref) if both else (lambda ref: ref.at[way])
        old, new = lax.rem(u, 2), lax.rem(u, RECEIVED)
        return pltpu.make_async_remote_copy(
            part(sg.at[way, old, s]), part(rg.at[way, new, s]), sg_sem.at[way, old, s], rg_sem.at[way, new, s],
            device_id={"dp": towards[way]}, device_id_type=MESH)

    tall = pd.shape[2] // 2

    def d_at(way, k, sent):
        return hid.at[(2 * sent + way) * far + k]

    def d_copy(j, way, both):
        k = lax.rem(j, far)
        part = (lambda ref: ref) if both else (lambda ref: ref.at[pl.ds(way * tall, tall), :])
        return pltpu.make_async_remote_copy(
            part(d_at(way, k, 1)), part(d_at(way, k, 0)), sd_sem.at[way, k], rd_sem.at[way, k],
            device_id={"dp": towards[way]}, device_id_type=MESH)

    def relay_g(u, s):
        slot, old, new = lax.rem(u, UNITS_HELD), lax.rem(u, 2), lax.rem(u, RECEIVED)
        for way in range(2):
            e = around[far - s] if way == 0 else around[n - far + s]

            @pl.when(u > 1)
            def _():
                g_copy(u - 2, s, way, s > 0).wait_send()

            if s > 0:
                g_copy(u, s - 1, way, s > 1).wait_recv()
            for h in range(2):
                if s == 0 and h != way:
                    continue
                own = pg[slot, pl.ds(pl.multiple_of(e * rows, rows), rows), h * FC:(h + 1) * FC]
                if s > 1 or (s == 1 and h == way):
                    own += rg[way, new, s - 1, h].astype(F32)
                sg[way, old, s, h] = own.astype(BF16)
            g_copy(u, s, way, s > 0).start()

    def relay_d(u, s):
        j, slot = lax.rem(u, nc), lax.rem(u, UNITS_HELD)
        k = lax.rem(j, far)
        for way in range(2):
            e = around[far - s] if way == 0 else around[n - far + s]

            @pl.when(lax.rem(e, far) == k)
            def _():
                @pl.when(u >= far)
                def _():
                    d_copy(j, way, s > 0).wait_send()

                if s > 0:
                    d_copy(j, way, s > 1).wait_recv()
                for h in range(2):
                    if s == 0 and h != way:
                        continue
                    part = pl.ds(h * tall, tall)
                    own = pd[slot, e // far, part, :]
                    if s > 1 or (s == 1 and h == way):
                        own += d_at(way, k, 0)[part, :].astype(F32)
                    d_at(way, k, 1)[part, :] = own.astype(BF16)
                d_copy(j, way, s > 0).start()

    def square(g):
        wide = g.astype(F32)
        ss[...] += jnp.sum((wide * wide).reshape(-1, *ss.shape), 0)

    def arrive_g(u):
        j, slot, new, layer = lax.rem(u, nc), lax.rem(u, UNITS_HELD), lax.rem(u, RECEIVED), 1 - u // nc
        for way in range(2):
            g_copy(u, far - 1, way, True).wait_recv()
        for h, out in enumerate((og, ou)):
            own = pg[slot, pl.ds(pl.multiple_of(me * rows, rows), rows), h * FC:(h + 1) * FC]
            own = (own + rg[0, new, far - 1, h].astype(F32) + rg[1, new, far - 1, h].astype(F32)).astype(BF16)
            for s in range(2):
                piece = own[:, s * LB:(s + 1) * LB]
                out[layer, :, at_block(block(j) + s * nc)] = piece
                square(piece)

    def arrive_d(u):
        j, slot, layer = lax.rem(u, nc), lax.rem(u, UNITS_HELD), 1 - u // nc
        k = lax.rem(j, far)

        @pl.when(lax.rem(me, far) == k)
        def _():
            for way in range(2):
                d_copy(j, way, True).wait_recv()
            for h in range(2):
                part = pl.ds(h * tall, tall)
                own = pd[slot, me // far, part, :]
                own = own + d_at(0, k, 0)[part, :].astype(F32) + d_at(1, k, 0)[part, :].astype(F32)
                own = own.T.astype(BF16)
                od[layer, at_block(j // half), h * tall:(h + 1) * tall] = own
                for s in range(tall // LB):
                    square(own[:, s * LB:(s + 1) * LB])

    def go_on(kind, u, s):
        if s == far:
            (arrive_g if kind == "g" else arrive_d)(u)
        else:
            (relay_g if kind == "g" else relay_d)(u, s)

    def turn_round(place, first, end):
        for s in range(far, -1, -1):
            here = [p for p in PLACES[s] if first <= p < end]
            if not here:
                continue
            u = sum((place > p).astype(jnp.int32) for p in here) + PLACES[s].index(here[0])
            due = functools.reduce(jnp.logical_or, [place == p for p in here])

            @pl.when(due)
            def _(s=s, u=u):
                go_on("g", u, s)
                go_on("d", u, s)

    def elementwise(gu, dh, slot):
        g, u = gu[:, :FC], gu[:, FC:]
        sig = sigmoid(g)
        silu = g * sig
        hds[slot][...] = (silu * u).astype(BF16)
        dgus[slot][:, :FC] = (dh * u * (sig + silu * (1 - sig))).astype(BF16)
        dgus[slot][:, FC:] = (dh * silu).astype(BF16)

    def keep_from(first):
        return (lambda old: old) if first is None else (lambda old: jnp.where(first, jnp.zeros_like(old), old))

    def back_g(u, t, slot, first=None):
        k, keep = lax.rem(u, UNITS_HELD), keep_from(first)
        pg[k] = keep(pg[k]) + dot(at[t], dgus[slot][...])

    def back_d(u, t, slot, first=None):
        k, keep = lax.rem(u, UNITS_HELD), keep_from(first)
        hd = dot(dyt[t], hds[slot][...])
        for s in range(2):
            pd[k, s] = keep(pd[k, s]) + hd[:, s * LB:(s + 1) * LB]

    def to_states(u, t, slot):
        old = jnp.where(u == 0, jnp.zeros(da.shape[1:], F32), da[t])
        da[t] = old + dot(dgus[slot][...], wgut[lax.rem(u, 2)])

    def turn(layer, j, t):
        p = lax.rem(j, 2)
        if layer:
            for i, f in enumerate((fg, fu)):
                s = lax.rem(t, 2)
                wgut[p, pl.ds(pl.multiple_of(i * FC + s * LB, LB), LB), :] = f[layer, :, at_block(block(j) + s * nc)].T
        s = lax.rem(t, 2)
        wdt[p, :, at_block(s)] = fd[layer, at_block(block(j) + s * nc), :].T

    def clear():
        for h, g in zip(hds, dgus):
            h[...] = jnp.zeros_like(h)
            g[...] = jnp.zeros_like(g)

    per_chunk = nt // 2
    steps = nc * per_chunk
    pl.semaphore_wait(barrier, n - 1)

    for t in range(2):
        turn(1, 0, t)
    clear()

    def front2(j, t, slot):
        cols = [at_block(block(j) + s * nc) for s in range(2)]
        gu = dot(a[t], jnp.concatenate([f[1, :, c] for f in (fg, fu) for c in cols], 1))
        elementwise(gu, dot(dy[t], wdt[lax.rem(j, 2)]).astype(BF16).astype(F32), slot)

    @pl.loop(0, nc * per_chunk)
    def _(i):
        j, t = i // per_chunk, 2 * lax.rem(i, per_chunk)
        k = jnp.maximum(2 * i - 1, 0)
        @pl.when(i == 2)
        def _():
            for copy in [c for k in range(1, nc) for c in gu_out(nt - 1, 1, k)]:
                copy.wait()

        jk, tk, jn = k // nt, lax.rem(k, nt), jnp.minimum(j + 1, nc - 1)
        to_states(jk, tk, 1)
        back_d(jk, tk, 1)
        front2(j, t, 0)
        to_states(j, t, 0)
        back_g(jk, tk, 1)
        turn(1, jn, t + 1)
        back_d(j, t, 0, t == 0)
        turn(1, jn, t)
        front2(j, t + 1, 1)
        back_g(j, t, 0, t == 0)
        turn_round(i, 0, steps)

    to_states(nc - 1, nt - 1, 1)
    back_d(nc - 1, nt - 1, 1)
    back_g(nc - 1, nt - 1, 1)

    def a1t_in(t):
        return pltpu.make_async_copy(a1t_h.at[t], at.at[t], sem_dy.at[t])

    def gu_in(i):
        return pltpu.make_async_copy(gu_h.at[i // nt, lax.rem(i, nt)], da.at[lax.rem(i, nt)], sem_gi.at[lax.rem(i, nt)])

    for t in range(nt):
        a1t_in(t).start()

    @pl.loop(0, nt)
    def _(t):
        wide = h1[t].astype(F32)
        r = rms(wide)
        da_t = da[t].astype(BF16).astype(F32)
        dn = da_t * r - wide * (r * r * r * jnp.mean(da_t * wide, -1, keepdims=True))
        dh1 = (dy[t].astype(F32) + dn).astype(BF16)
        dy[t] = dh1
        dyt[t] = dh1.T
        gu_in(t).start()
        a1t_in(t).wait()

        @pl.when(lax.rem(t, 2) == 1)
        def _():
            turn_round(steps + t // 2, steps, steps + far)

    for t in range(2):
        turn(0, 0, t)
    clear()

    def front1(j, t, slot):
        elementwise(da[t], dot(dy[t], wdt[lax.rem(j, 2)]).astype(BF16).astype(F32), slot)

    @pl.loop(0, nc * per_chunk)
    def _(i):
        j, t = i // per_chunk, 2 * lax.rem(i, per_chunk)
        k = jnp.maximum(2 * i - 1, 0)
        for s in range(2):
            gu_in(2 * i + s).wait()
        jk, tk, jn = nc + k // nt, lax.rem(k, nt), jnp.minimum(j + 1, nc - 1)
        turn(0, jn, t + 1)
        back_d(jk, tk, 1)
        turn(0, jn, t)
        back_g(jk, tk, 1)
        front1(j, t, 0)
        back_d(nc + j, t, 0, t == 0)
        front1(j, t + 1, 1)
        back_g(nc + j, t, 0, t == 0)

        @pl.when(j + 1 < nc)
        def _():
            for s in range(2):
                gu_in(2 * i + s + nt).start()

        turn_round(steps + far + i, steps + far, 2 * steps + far)

    back_d(2 * nc - 1, nt - 1, 1)
    back_g(2 * nc - 1, nt - 1, 1)

    pieces = [(i, layer) for layer in (1, 0) for i in range(3)]
    d = h1.shape[2]
    deep = n // 2 * rows

    def moment_copies(k):
        i, layer = pieces[k]
        made = []
        for c, h in enumerate(((mg_h, mu_h, md_h)[i], (vg_h, vu_h, vd_h)[i])):
            if i == 2:
                made.append(pltpu.make_async_copy(h.at[layer], da.at[k, pl.ds(c * deep, deep), :], mv_sem.at[k, c]))
            else:
                for b in range(far):
                    made.append(pltpu.make_async_copy(
                        h.at[layer, :, pl.ds(b * d, d)], da.at[k, pl.ds(c * deep + b * rows, rows), :], mv_sem.at[k, c * far + b]))
        return made

    for k in range(len(pieces)):
        for copy in moment_copies(k):
            copy.start()

    for kind, u, s in LAST:
        go_on(kind, jnp.int32(u), s)

    tots[pl.ds(me, 1)] = ss[...][None]
    totals = [
        pltpu.make_async_remote_copy(ss, tots.at[me], ts_sem.at[k], tr_sem.at[n - k], device_id={"dp": around[k]}, device_id_type=MESH)
        for k in range(1, n)
    ]
    for copy in totals:
        copy.start()
    for way in range(2):
        for s in range(far):
            for u in (units - 2, units - 1):
                g_copy(u, s, way, s > 0).wait_send()
            e = around[far - s] if way == 0 else around[n - far + s]
            d_copy(lax.rem(e, far), way, s > 0).wait_send()
    for k in range(len(pieces)):
        for copy in moment_copies(k):
            copy.wait()
    for k in range(1, n):
        pltpu.make_async_remote_copy(ss, tots.at[around[k]], ts_sem.at[k], tr_sem.at[k], device_id={"dp": around[k]}, device_id_type=MESH).wait_recv()
    factor = jnp.minimum(1.0, 0.5 * lax.rsqrt(jnp.sum(tots[...], keepdims=True).reshape(1, 1) / count + 1e-30))

    def rows_of(i, origin, part=None):
        tall = full[i].shape[1] // n
        start = origin * tall
        if part is not None:
            tall //= 2
            start += part * tall
        return pl.ds(pl.multiple_of(start, tall), tall)

    def pass_on(k, s, way, coming=False):
        i, layer = pieces[k]
        back_by = s + coming
        origin = around[(n - back_by) % n] if way == 0 else around[back_by]
        here = full[i].at[layer, rows_of(i, origin, way if s == far - 1 else None), :]
        return pltpu.make_async_remote_copy(
            here, here, ag_send.at[way, s, k], ag_recv.at[way, s, k], device_id={"dp": towards[way]}, device_id_type=MESH)

    for k, (i, layer) in enumerate(pieces):
        def adamw(here, where_g, where_w):
            m_at, v_at = here, pl.ds(here.start + deep, here.size)
            g = own_g[i][(layer, *where_g)].astype(F32) * factor
            m = 0.9 * da[k, m_at, :] + 0.1 * g
            v = 0.95 * da[k, v_at, :] + 0.05 * g * g
            w = full[i][(layer, *where_w)].astype(F32)
            step = m * lax.rsqrt(v + 1e-8) + 0.1 * w
            da[k, m_at, :] = m
            da[k, v_at, :] = v
            full[i][(layer, *where_w)] = (w - 0.02 * step).astype(BF16)

        for b in range(far):
            here = pl.ds(b * rows, rows)
            if i == 2:
                adamw(here, (here, slice(None)), (pl.ds(pl.multiple_of(me * deep + b * rows, rows), rows), slice(None)))
            else:
                cols = pl.ds(b * d, d)
                adamw(here, (slice(None), cols), (pl.ds(pl.multiple_of(me * rows, rows), rows), cols))
        for way in range(2):
            pass_on(k, 0, way).start()

    for s in range(far):
        for k in range(len(pieces)):
            for way in range(2):
                pass_on(k, s, way, True).wait_recv()
                if s + 1 < far:
                    pass_on(k, s + 1, way).start()
    for copy in totals:
        copy.wait_send()
    for s in range(far):
        for k in range(len(pieces)):
            for way in range(2):
                pass_on(k, s, way).wait_send()


def flush_kernel(n, fg, fu, fd, wide, *refs):
    outs, sem = refs[:9], refs[9]
    layers, d = fg.shape[0], fg.shape[1]
    rows, far = d // n, n // 2
    deep = far * rows
    copies = []
    for k, (i, layer) in enumerate((i, layer) for layer in (1, 0) for i in range(3)):
        for c in range(2):
            out = outs[3 + 3 * c + i]
            if i == 2:
                copies.append((wide.at[k, pl.ds(c * deep, deep), :], out.at[layer]))
            else:
                copies += [(wide.at[k, pl.ds(c * deep + b * rows, rows), :], out.at[layer, :, pl.ds(b * d, d)]) for b in range(far)]
    copies += [(f.at[layer], out.at[layer]) for layer in range(layers) for f, out in zip((fg, fu, fd), outs)]
    copies = [pltpu.make_async_copy(*pair, sem.at[i]) for i, pair in enumerate(copies)]
    for copy in copies:
        copy.start()
    for copy in copies:
        copy.wait()


def train_step(x, dy, w, m, v, n):
    wg, wu, wd = w
    tokens, d = x.shape[1:]
    layers, _, f = wg.shape
    nt, nc = tokens // TT, f // FC
    far, rows = n // 2, d // n
    pieces = 3 * layers
    hbm = pl.BlockSpec(memory_space=pl.ANY)
    vmem = pl.BlockSpec(memory_space=pltpu.VMEM)
    shape = jax.ShapeDtypeStruct
    kept = [pltpu.VMEM(one.shape, BF16) for one in w] + [pltpu.VMEM((nt, TT, d), F32)]
    v_, dma = pltpu.VMEM, pltpu.SemaphoreType.DMA
    scratch = [
        v_((2, 2 * FC, d), BF16), v_((2, d, FC), BF16),
        v_((nt, TT, d), BF16), v_((nt, d, TT), BF16), v_((nt, TT, d), BF16), v_((nt, TT, d), BF16), v_((nt, d, TT), BF16),
        v_((2 * nc, TT, LB), BF16), v_((TT, FC), BF16), v_((TT, FC), BF16), v_((TT, 2 * FC), BF16), v_((TT, 2 * FC), BF16),
        v_((UNITS_HELD, d, 2 * FC), F32), v_((UNITS_HELD, 2, d, LB), F32),
        v_((2, RECEIVED, far, 2, rows, FC), BF16), v_((2, 2, far, 2, rows, FC), BF16),
        v_((layers, rows, f), BF16), v_((layers, rows, f), BF16), v_((layers, f // n, d), BF16), v_((8, LB), F32), v_((n, 8, LB), F32),
        dma((layers, 3)), dma((nt,)), dma((nt,)), dma((2,)), dma((2 * nc + 6,)), dma((nt,)),
        dma((2, RECEIVED, far)), dma((2, far)), dma((2, 2, far)), dma((2, far)), dma((n,)), dma((n,)),
        dma((pieces, n)), dma((2, far, pieces)), dma((2, far, pieces)),
    ]
    kept_bytes = 2 * sum(one.size for one in w) + 4 * tokens * d
    *new, wide, _, _ = pl.pallas_call(
        functools.partial(step_kernel, nt, nc, n, sum(one.size for one in w)),
        name="train_step",
        out_shape=kept + [shape((nc, nt, TT, 2 * FC), F32), shape((nt, d, TT), BF16)],
        in_specs=[hbm] * 11,
        out_specs=[vmem] * 4 + [hbm] * 2,
        scratch_shapes=scratch,
        compiler_params=pltpu.CompilerParams(vmem_limit_bytes=VMEM_BYTES - kept_bytes, collective_id=0, has_side_effects=True),
    )(x, dy, *w, *m, *v)
    copies = layers * (2 * (2 * far + 1) + 3)
    keep = lambda one: pltpu.with_memory_space_constraint(one, pltpu.VMEM)
    return tuple(pl.pallas_call(
        functools.partial(flush_kernel, n),
        name="flush",
        out_shape=[shape(one.shape, one.dtype) for group in (w, m, v) for one in group],
        in_specs=[vmem] * 4,
        out_specs=[hbm] * 9,
        scratch_shapes=[dma((copies,))],
        compiler_params=pltpu.CompilerParams(vmem_limit_bytes=1 << 20),
    )(*(keep(one) for one in (*new, wide))))


def solution(mesh):
    n = mesh.shape["dp"]

    def step(x, dy, *arrays):
        return train_step(x, dy, *(arrays[i:i + 3] for i in (0, 3, 6)), n)

    seq, rows = P(("rep", "dp"), None, None), P(None, "dp", None)
    return jax.shard_map(
        step,
        mesh=mesh,
        in_specs=(seq, seq) + (P(),) * 3 + (rows,) * 6,
        out_specs=(P("rep"),) * 3 + (P("rep", "dp"),) * 6,
        check_vma=False,
    )
```

```python
import functools

import jax
import jax.numpy as jnp
from jax import lax
from jax.experimental import pallas as pl
from jax.experimental.pallas import tpu as pltpu
from jax.sharding import PartitionSpec as P

F32, BF16 = jnp.float32, jnp.bfloat16
MESH = pl.DeviceIdType.MESH
TT = 512
LB = 128
EARLY = 2
STAGED = 4
FC = 2 * LB
RECEIVED = 6
UNITS_HELD = 7
VMEM_BYTES = 67_043_328
PLACES = tuple(tuple(int(p) for p in line.split(",")) for line in (
    "4,8,12,17,20,24,29,33,40,44,48,52,56,60,64",
    "6,11,15,21,23,27,34,39,46,47,53,57,61,65",
    "9,14,19,25,26,30,42,45,50,56,58,62,66",
    "12,17,22,30,34,37,49,51,55,60,63",
    "15,20,30,43,46,47,54,57,62",
))
LAST = tuple((what[0], *(int(p) for p in what[1:].split("."))) for line in (
    "d9.4,d11.3,g15.0,d15.0,d14.1,g9.4,g14.1,g11.3,d13.2,g12.3",
    "d12.3,g15.1,d15.1,d10.4,g13.2,g14.2,d11.4,d14.2,g10.4,g11.4",
    "g15.2,d15.2,g13.3,d13.3,d14.3,g14.3,d12.4,g15.3,d15.3,d13.4",
    "g12.4,g13.4,g14.4,d14.4,g15.4,d15.4",
) for what in line.split(","))
EARLY_PLACES = tuple((what[0], *(int(p) for p in what[1:].split("."))) for line in (
    "m1.2.1,m0.3.4,m1.3.6,s0.0.15,s0.1.19,s1.0.20,s0.2.23,s1.1.24",
    "s1.2.28,s0.3.29,s1.3.31",
) for what in line.split(","))


def dot(a, b):
    return jnp.dot(a, b, preferred_element_type=F32)


def rms(wide):
    return lax.rsqrt(jnp.mean(wide * wide, -1, keepdims=True) + 1e-6)


def sigmoid(g):
    return 0.5 * jnp.tanh(0.5 * g) + 0.5


def step_kernel(nt, nc, n, count, x_h, dy_h, wg_h, wu_h, wd_h, mg_h, mu_h, md_h, vg_h, vu_h, vd_h,
                fg, fu, fd, wide_ref, gu_h, a1t_h, mv_h, gs_h,
                wgut, wdt, a, at, h1, dy, dyt, hid, hd0, hd1, dgu0, dgu1,
                pg, pd, rg, sg, gs, og, ou, od, ss, tots,
                sem_w, sem_x, sem_dy, sem_at, sem_gu, sem_gi, rg_sem, rd_sem, sg_sem, sd_sem, ts_sem, tr_sem, mv_sem, ag_send, ag_recv,
                free_sem, early_sem, ms_sem, mr_sem, gs_sem, gr_sem, late_sem):
    half, far = nc // 2, n // 2
    units = 2 * nc
    rows = pg.shape[1] // n
    hds, dgus = (hd0, hd1), (dgu0, dgu1)
    full, own_g = (fg, fu, fd), (og, ou, od)
    da = wide_ref
    me = lax.axis_index("dp")
    around = [lax.rem(me + k, n) for k in range(n)]
    towards = (around[1], around[n - 1])

    barrier = pltpu.get_barrier_semaphore()
    for k in range(1, n):
        pl.semaphore_signal(barrier, inc=1, device_id={"dp": around[k]}, device_id_type=MESH)

    def block(j):
        return 2 * lax.rem(j, half) + j // half

    def at_block(b):
        return pl.ds(b * LB if isinstance(b, int) else pl.multiple_of(b * LB, LB), LB)

    def x_copy(t):
        return pltpu.make_async_copy(x_h.at[0, pl.ds(t * TT, TT), :], a.at[t], sem_x.at[t])

    def dy_copy(t):
        return pltpu.make_async_copy(dy_h.at[0, pl.ds(t * TT, TT), :], dy.at[t], sem_dy.at[t])

    def w_copies(layer):
        return [pltpu.make_async_copy(h.at[layer], v.at[layer], sem_w.at[layer, i]) for i, (h, v) in enumerate(zip((wg_h, wu_h, wd_h), full))]

    x_copy(0).start()
    for copy in w_copies(0):
        copy.start()
    ss[...] = jnp.zeros_like(ss)

    def staged(odd, j):
        if not odd:
            return [(da.at[j], 0, 2 * FC)]
        if j < UNITS_HELD:
            return [(pg.at[j], 0, 2 * FC)]
        return [(pd.at[UNITS_HELD - 2 + i // 2, i % 2], i * LB, LB) for i in range(2 * FC // LB)]

    def gu_out(t, odd, j):
        return [pltpu.make_async_copy(ref, gu_h.at[j, t, :, pl.ds(at_, width)], sem_gu.at[odd * (nc + 3) + j + i])
                for i, (ref, at_, width) in enumerate(staged(odd, j))]

    def gu_out_all(t, odd):
        return [copy for j in range(nc) for copy in gu_out(t, odd, j)]

    def a1t_out(t):
        p = lax.rem(t, 2)
        return pltpu.make_async_copy(wgut.at[p], a1t_h.at[t], sem_at.at[p])

    def hand_on(own, copies_h, send, recv, j, s, way, coming=False):
        back_by = s + coming
        origin = around[(n - back_by) % n] if way == 0 else around[back_by]
        there = copies_h.at[j, origin]
        here = there if back_by else own
        if s == far - 1:
            size = there.shape[0] // 2
            there, here = there.at[pl.ds(way * size, size)], here.at[pl.ds(way * size, size)]
        return pltpu.make_async_remote_copy(
            here, there, send.at[way, s, j], recv.at[way, s, j], device_id={"dp": towards[way]}, device_id_type=MESH)

    def moments_on(j, s, way, coming=False):
        return hand_on(pd.at[STAGED, j], mv_h, ms_sem, mr_sem, j, s, way, coming)

    def sums_on(j, s, way, coming=False):
        return hand_on(gs.at[j], gs_h, gs_sem, gr_sem, j, s, way, coming)

    def forward_on(which, j, s):
        for way in range(2):
            if s > 0:
                which(j, s - 1, way, True).wait_recv()
            which(j, s, way).start()

    def early_moments():
        copies = []
        for j in range(EARLY):
            for i, pair in enumerate(((mg_h, vg_h), (mu_h, vu_h))):
                for c, h in enumerate(pair):
                    for b in range(2):
                        part = 4 * i + 2 * c + b
                        copies.append(pltpu.make_async_copy(
                            h.at[1, :, at_block(static_block(j) + b * nc)], pd.at[STAGED, j, pl.ds(part * rows, rows), :], early_sem.at[j, part]))
        return copies

    def static_block(j):
        return 2 * (j % half) + j // half

    def down():
        w = jnp.concatenate([fd[0, at_block(static_block(j) + s * nc), :] for j in range(nc) for s in range(2)], 0)
        return dot(jnp.concatenate([hid[b] for b in range(2 * nc)], 1), w)

    def gate_up(odd, j):
        cols = [at_block(static_block(j) + s * nc) for s in range(2)]
        gu = dot(dgu0[...], jnp.concatenate([f[0, :, c] for f in (fg, fu) for c in cols], 1))
        for ref, at_, width in staged(odd, j):
            ref[...] = gu[:, at_:at_ + width]
        g, u = gu[:, :FC], gu[:, FC:]
        h = (g * sigmoid(g) * u).astype(BF16)
        for s in range(2):
            hid[2 * j + s] = h[:, s * LB:(s + 1) * LB]

    def finish(t, y):
        h = (a[t].astype(F32) + y.astype(BF16).astype(F32)).astype(BF16)
        h1[t] = h
        wide = h.astype(F32)
        a2 = (wide * rms(wide)).astype(BF16)
        a[t] = a2
        at[t] = a2.T
        dyt[t] = dy[t].T

    def forward(t, odd, follows):
        x_copy(t).wait()
        if follows:
            dy_copy(t - 1).wait()

        @pl.when(t >= 2)
        def _():
            a1t_out(t - 2).wait()
            for copy in gu_out_all(t - 2, odd):
                copy.wait()

        if follows:
            y = down()
        wide = a[t].astype(F32)
        a1 = (wide * rms(wide)).astype(BF16)
        dgu0[...] = a1
        wgut[lax.rem(t, 2)] = a1.T
        for j in range(nc):
            gate_up(odd, j)
            if j == half and follows:
                finish(t - 1, y)
        for copy in gu_out_all(t, odd):
            copy.start()
        a1t_out(t).start()

    for copy in w_copies(0):
        copy.wait()
    dy_copy(0).start()
    for t in range(1, nt):
        x_copy(t).start()
        dy_copy(t).start()
    for copy in early_moments():
        copy.start()
    for copy in w_copies(1):
        copy.start()
    forward(0, 0, False)
    for copy in early_moments():
        copy.wait()
    pl.semaphore_wait(barrier, n - 1)
    for j in range(EARLY):
        forward_on(moments_on, j, 0)

    @pl.loop(0, nt // 2 - 1)
    def _(i):
        forward(2 * i + 1, 1, True)
        forward(2 * i + 2, 0, True)

        for j in range(EARLY):
            @pl.when(i == j + 1)
            def _(j=j):
                forward_on(moments_on, j, 1)

    forward(nt - 1, 1, True)
    forward_on(moments_on, 0, 2)
    dy_copy(nt - 1).wait()
    finish(nt - 1, down())
    for copy in gu_out_all(nt - 2, 0):
        copy.wait()
    for t in (nt - 2, nt - 1):
        a1t_out(t).wait()
    for copy in gu_out(nt - 1, 1, 0):
        copy.wait()
    for copy in w_copies(1):
        copy.wait()

    for other in towards:
        pl.semaphore_signal(free_sem, inc=1, device_id={"dp": other}, device_id_type=MESH)

    def g_copy(u, s, way, both):
        part = (lambda ref: ref) if both else (lambda ref: ref.at[way])
        old, new = lax.rem(u, 2), lax.rem(u, RECEIVED)
        return pltpu.make_async_remote_copy(
            part(sg.at[way, old, s]), part(rg.at[way, new, s]), sg_sem.at[way, old, s], rg_sem.at[way, new, s],
            device_id={"dp": towards[way]}, device_id_type=MESH)

    tall = pd.shape[2] // 2

    def d_at(way, k, sent):
        return hid.at[(2 * sent + way) * far + k]

    def d_copy(j, way, both):
        k = lax.rem(j, far)
        part = (lambda ref: ref) if both else (lambda ref: ref.at[pl.ds(way * tall, tall), :])
        return pltpu.make_async_remote_copy(
            part(d_at(way, k, 1)), part(d_at(way, k, 0)), sd_sem.at[way, k], rd_sem.at[way, k],
            device_id={"dp": towards[way]}, device_id_type=MESH)

    def relay_g(u, s):
        slot, old, new = lax.rem(u, UNITS_HELD), lax.rem(u, 2), lax.rem(u, RECEIVED)
        for way in range(2):
            e = around[far - s] if way == 0 else around[n - far + s]

            @pl.when(u > 1)
            def _():
                g_copy(u - 2, s, way, s > 0).wait_send()

            if s > 0:
                g_copy(u, s - 1, way, s > 1).wait_recv()
            for h in range(2):
                if s == 0 and h != way:
                    continue
                own = pg[slot, pl.ds(pl.multiple_of(e * rows, rows), rows), h * FC:(h + 1) * FC]
                if s > 1 or (s == 1 and h == way):
                    own += rg[way, new, s - 1, h].astype(F32)
                sg[way, old, s, h] = own.astype(BF16)
            g_copy(u, s, way, s > 0).start()

    def relay_d(u, s):
        j, slot = lax.rem(u, nc), lax.rem(u, UNITS_HELD)
        k = lax.rem(j, far)
        for way in range(2):
            e = around[far - s] if way == 0 else around[n - far + s]

            @pl.when(lax.rem(e, far) == k)
            def _():
                @pl.when(u >= far)
                def _():
                    d_copy(j, way, s > 0).wait_send()

                if s > 0:
                    d_copy(j, way, s > 1).wait_recv()
                for h in range(2):
                    if s == 0 and h != way:
                        continue
                    part = pl.ds(h * tall, tall)
                    own = pd[slot, e // far, part, :]
                    if s > 1 or (s == 1 and h == way):
                        own += d_at(way, k, 0)[part, :].astype(F32)
                    d_at(way, k, 1)[part, :] = own.astype(BF16)
                d_copy(j, way, s > 0).start()

    def square(g):
        wide = g.astype(F32)
        ss[...] += jnp.sum((wide * wide).reshape(-1, *ss.shape), 0)

    def arrive_g(u):
        j, slot, new, layer = lax.rem(u, nc), lax.rem(u, UNITS_HELD), lax.rem(u, RECEIVED), 1 - u // nc
        for way in range(2):
            g_copy(u, far - 1, way, True).wait_recv()
        for h, out in enumerate((og, ou)):
            own = pg[slot, pl.ds(pl.multiple_of(me * rows, rows), rows), h * FC:(h + 1) * FC]
            own = (own + rg[0, new, far - 1, h].astype(F32) + rg[1, new, far - 1, h].astype(F32)).astype(BF16)
            for s in range(2):
                piece = own[:, s * LB:(s + 1) * LB]
                out[layer, :, at_block(block(j) + s * nc)] = piece
                square(piece)

            @pl.when(u < EARLY)
            def _(own=own, h=h):
                gs[jnp.minimum(u, EARLY - 1), h] = own

    def arrive_d(u):
        j, slot, layer = lax.rem(u, nc), lax.rem(u, UNITS_HELD), 1 - u // nc
        k = lax.rem(j, far)

        @pl.when(lax.rem(me, far) == k)
        def _():
            for way in range(2):
                d_copy(j, way, True).wait_recv()
            for h in range(2):
                part = pl.ds(h * tall, tall)
                own = pd[slot, me // far, part, :]
                own = own + d_at(0, k, 0)[part, :].astype(F32) + d_at(1, k, 0)[part, :].astype(F32)
                own = own.T.astype(BF16)
                od[layer, at_block(j // half), h * tall:(h + 1) * tall] = own
                for s in range(tall // LB):
                    square(own[:, s * LB:(s + 1) * LB])

    def go_on(kind, u, s):
        if s == far:
            (arrive_g if kind == "g" else arrive_d)(u)
        else:
            (relay_g if kind == "g" else relay_d)(u, s)

    def turn_round(place, first, end):
        for s in range(far, -1, -1):
            here = [p for p in PLACES[s] if first <= p < end]
            if not here:
                continue
            u = sum((place > p).astype(jnp.int32) for p in here) + PLACES[s].index(here[0])
            due = functools.reduce(jnp.logical_or, [place == p for p in here])

            @pl.when(due)
            def _(s=s, u=u):
                go_on("g", u, s)
                go_on("d", u, s)

    def elementwise(gu, dh, slot):
        g, u = gu[:, :FC], gu[:, FC:]
        sig = sigmoid(g)
        silu = g * sig
        hds[slot][...] = (silu * u).astype(BF16)
        dgus[slot][:, :FC] = (dh * u * (sig + silu * (1 - sig))).astype(BF16)
        dgus[slot][:, FC:] = (dh * silu).astype(BF16)

    def keep_from(first):
        return (lambda old: old) if first is None else (lambda old: jnp.where(first, jnp.zeros_like(old), old))

    def back_g(u, t, slot, first=None):
        k, keep = lax.rem(u, UNITS_HELD), keep_from(first)
        pg[k] = keep(pg[k]) + dot(at[t], dgus[slot][...])

    def back_d(u, t, slot, first=None):
        k, keep = lax.rem(u, UNITS_HELD), keep_from(first)
        hd = dot(dyt[t], hds[slot][...])
        for s in range(2):
            pd[k, s] = keep(pd[k, s]) + hd[:, s * LB:(s + 1) * LB]

    def to_states(u, t, slot):
        old = jnp.where(u == 0, jnp.zeros(da.shape[1:], F32), da[t])
        da[t] = old + dot(dgus[slot][...], wgut[lax.rem(u, 2)])

    def turn(layer, j, t):
        p = lax.rem(j, 2)
        if layer:
            for i, f in enumerate((fg, fu)):
                s = lax.rem(t, 2)
                wgut[p, pl.ds(pl.multiple_of(i * FC + s * LB, LB), LB), :] = f[layer, :, at_block(block(j) + s * nc)].T
        s = lax.rem(t, 2)
        wdt[p, :, at_block(s)] = fd[layer, at_block(block(j) + s * nc), :].T

    def clear():
        for h, g in zip(hds, dgus):
            h[...] = jnp.zeros_like(h)
            g[...] = jnp.zeros_like(g)

    per_chunk = nt // 2
    steps = nc * per_chunk
    pl.semaphore_wait(free_sem, 2)

    for t in range(2):
        turn(1, 0, t)
    clear()

    def front2(j, t, slot):
        cols = [at_block(block(j) + s * nc) for s in range(2)]
        gu = dot(a[t], jnp.concatenate([f[1, :, c] for f in (fg, fu) for c in cols], 1))
        elementwise(gu, dot(dy[t], wdt[lax.rem(j, 2)]).astype(BF16).astype(F32), slot)

    @pl.loop(0, nc * per_chunk)
    def _(i):
        j, t = i // per_chunk, 2 * lax.rem(i, per_chunk)
        k = jnp.maximum(2 * i - 1, 0)
        @pl.when(i == 2)
        def _():
            for copy in [c for k in range(1, nc) for c in gu_out(nt - 1, 1, k)]:
                copy.wait()

        jk, tk, jn = k // nt, lax.rem(k, nt), jnp.minimum(j + 1, nc - 1)
        to_states(jk, tk, 1)
        back_d(jk, tk, 1)
        front2(j, t, 0)
        to_states(j, t, 0)
        back_g(jk, tk, 1)
        turn(1, jn, t + 1)
        back_d(j, t, 0, t == 0)
        turn(1, jn, t)
        front2(j, t + 1, 1)
        back_g(j, t, 0, t == 0)
        turn_round(i, 0, steps)
        @pl.when(i == STAGED * per_chunk - 1)
        def _():
            for j in range(EARLY):
                for way in range(2):
                    moments_on(j, 0, way).wait_send()

        for kind, which in (("m", moments_on), ("s", sums_on)):
            due = [what for what in EARLY_PLACES if what[0] == kind]

            @pl.when((i >= due[0][3]) & (i <= due[-1][3]))
            def _(which=which, due=due):
                for _, j, s, place in due:
                    @pl.when(i == place)
                    def _(j=j, s=s):
                        forward_on(which, j, s)

    to_states(nc - 1, nt - 1, 1)
    back_d(nc - 1, nt - 1, 1)
    back_g(nc - 1, nt - 1, 1)

    def a1t_in(t):
        return pltpu.make_async_copy(a1t_h.at[t], at.at[t], sem_dy.at[t])

    def gu_in(i):
        return pltpu.make_async_copy(gu_h.at[i // nt, lax.rem(i, nt)], da.at[lax.rem(i, nt)], sem_gi.at[lax.rem(i, nt)])

    for t in range(nt):
        a1t_in(t).start()

    @pl.loop(0, nt)
    def _(t):
        wide = h1[t].astype(F32)
        r = rms(wide)
        da_t = da[t].astype(BF16).astype(F32)
        dn = da_t * r - wide * (r * r * r * jnp.mean(da_t * wide, -1, keepdims=True))
        dh1 = (dy[t].astype(F32) + dn).astype(BF16)
        dy[t] = dh1
        dyt[t] = dh1.T
        gu_in(t).start()
        a1t_in(t).wait()

        @pl.when(lax.rem(t, 2) == 1)
        def _():
            turn_round(steps + t // 2, steps, steps + far)

    for t in range(2):
        turn(0, 0, t)
    clear()

    def front1(j, t, slot):
        elementwise(da[t], dot(dy[t], wdt[lax.rem(j, 2)]).astype(BF16).astype(F32), slot)

    @pl.loop(0, nc * per_chunk)
    def _(i):
        j, t = i // per_chunk, 2 * lax.rem(i, per_chunk)
        k = jnp.maximum(2 * i - 1, 0)
        for s in range(2):
            gu_in(2 * i + s).wait()
        jk, tk, jn = nc + k // nt, lax.rem(k, nt), jnp.minimum(j + 1, nc - 1)
        turn(0, jn, t + 1)
        back_d(jk, tk, 1)
        turn(0, jn, t)
        back_g(jk, tk, 1)
        front1(j, t, 0)
        back_d(nc + j, t, 0, t == 0)
        front1(j, t + 1, 1)
        back_g(nc + j, t, 0, t == 0)

        @pl.when(j + 1 < nc)
        def _():
            for s in range(2):
                gu_in(2 * i + s + nt).start()

        turn_round(steps + far + i, steps + far, 2 * steps + far)

    back_d(2 * nc - 1, nt - 1, 1)
    back_g(2 * nc - 1, nt - 1, 1)

    pieces = [(i, layer) for layer in (1, 0) for i in range(3)]
    d = h1.shape[2]
    deep = n // 2 * rows

    def moment_copies(k):
        i, layer = pieces[k]
        made = []
        for c, h in enumerate(((mg_h, mu_h, md_h)[i], (vg_h, vu_h, vd_h)[i])):
            if i == 2:
                made.append(pltpu.make_async_copy(h.at[layer], da.at[k, pl.ds(c * deep, deep), :], mv_sem.at[k, c]))
            else:
                for b in range(far):
                    made.append(pltpu.make_async_copy(
                        h.at[layer, :, pl.ds(b * d, d)], da.at[k, pl.ds(c * deep + b * rows, rows), :], mv_sem.at[k, c * far + b]))
        return made

    for k in range(len(pieces)):
        for copy in moment_copies(k):
            copy.start()

    for kind, u, s in LAST:
        go_on(kind, jnp.int32(u), s)

    def early_loads(k):
        made = []
        for j in range(EARLY):
            made.append(pltpu.make_async_copy(mv_h.at[j, around[k]], pd.at[k - 1, j], late_sem.at[k - 1, j, 0]))
            made.append(pltpu.make_async_copy(gs_h.at[j, around[k]], rg.at[j, (k - 1) // far, (k - 1) % far], late_sem.at[k - 1, j, 1]))
        return made

    for which in (moments_on, sums_on):
        for j in range(EARLY):
            for way in range(2):
                which(j, far - 1, way, True).wait_recv()
                for s in range(which is moments_on, far):
                    which(j, s, way).wait_send()
    for k in range(1, n):
        for copy in early_loads(k):
            copy.start()

    tots[pl.ds(me, 1)] = ss[...][None]
    totals = [
        pltpu.make_async_remote_copy(ss, tots.at[me], ts_sem.at[k], tr_sem.at[n - k], device_id={"dp": around[k]}, device_id_type=MESH)
        for k in range(1, n)
    ]
    for copy in totals:
        copy.start()
    for way in range(2):
        for s in range(far):
            for u in (units - 2, units - 1):
                g_copy(u, s, way, s > 0).wait_send()
            e = around[far - s] if way == 0 else around[n - far + s]
            d_copy(lax.rem(e, far), way, s > 0).wait_send()
    for k in range(len(pieces)):
        for copy in moment_copies(k):
            copy.wait()
    for k in range(1, n):
        pltpu.make_async_remote_copy(ss, tots.at[around[k]], ts_sem.at[k], tr_sem.at[k], device_id={"dp": around[k]}, device_id_type=MESH).wait_recv()
    factor = jnp.minimum(1.0, 0.5 * lax.rsqrt(jnp.sum(tots[...], keepdims=True).reshape(1, 1) / count + 1e-30))

    def rows_of(i, origin, part=None):
        tall = full[i].shape[1] // n
        start = origin * tall
        if part is not None:
            tall //= 2
            start += part * tall
        return pl.ds(pl.multiple_of(start, tall), tall)

    early = sorted(static_block(j) + s * nc for j in range(EARLY) for s in range(2))
    between = [(p + 1, q) for p, q in zip([-1] + early, early + [2 * nc]) if q > p + 1]
    parcels = [(k, i, layer, cols) for k, (i, layer) in enumerate(pieces)
               for cols in ([pl.ds(p * LB, (q - p) * LB) for p, q in between] if layer == 1 and i < 2 else [slice(None)])]

    def pass_on(c, s, way, coming=False):
        _, i, layer, cols = parcels[c]
        back_by = s + coming
        origin = around[(n - back_by) % n] if way == 0 else around[back_by]
        here = full[i].at[layer, rows_of(i, origin, way if s == far - 1 else None), cols]
        return pltpu.make_async_remote_copy(
            here, here, ag_send.at[way, s, c], ag_recv.at[way, s, c], device_id={"dp": towards[way]}, device_id_type=MESH)

    for k, (i, layer) in enumerate(pieces):
        def adamw(here, where_g, where_w):
            m_at, v_at = here, pl.ds(here.start + deep, here.size)
            g = own_g[i][(layer, *where_g)].astype(F32) * factor
            m = 0.9 * da[k, m_at, :] + 0.1 * g
            v = 0.95 * da[k, v_at, :] + 0.05 * g * g
            w = full[i][(layer, *where_w)].astype(F32)
            step = m * lax.rsqrt(v + 1e-8) + 0.1 * w
            da[k, m_at, :] = m
            da[k, v_at, :] = v
            full[i][(layer, *where_w)] = (w - 0.02 * step).astype(BF16)

        for b in range(far):
            here = pl.ds(b * rows, rows)
            if i == 2:
                adamw(here, (here, slice(None)), (pl.ds(pl.multiple_of(me * deep + b * rows, rows), rows), slice(None)))
            else:
                cols = pl.ds(b * d, d)
                adamw(here, (slice(None), cols), (pl.ds(pl.multiple_of(me * rows, rows), rows), cols))
        for c, parcel in enumerate(parcels):
            if parcel[0] == k:
                for way in range(2):
                    pass_on(c, 0, way).start()

    for k in range(1, n):
        for copy in early_loads(k):
            copy.wait()

    @pl.loop(1, n)
    def _(k):
        origin = lax.rem(me + k, n)
        mine = pl.ds(pl.multiple_of(origin * rows, rows), rows)
        for j in range(EARLY):
            for i, f in enumerate((fg, fu)):
                for b in range(2):
                    cols = at_block(static_block(j) + b * nc)
                    g = rg[j, (k - 1) // far, lax.rem(k - 1, far), i, :, b * LB:(b + 1) * LB].astype(F32) * factor
                    m = 0.9 * pd[k - 1, j, (4 * i + b) * rows:(4 * i + b + 1) * rows, :] + 0.1 * g
                    v = 0.95 * pd[k - 1, j, (4 * i + 2 + b) * rows:(4 * i + 3 + b) * rows, :] + 0.05 * g * g
                    w = f[1, mine, cols].astype(F32)
                    f[1, mine, cols] = (w - 0.02 * (m * lax.rsqrt(v + 1e-8) + 0.1 * w)).astype(BF16)

    for s in range(far):
        for c in range(len(parcels)):
            for way in range(2):
                pass_on(c, s, way, True).wait_recv()
                if s + 1 < far:
                    pass_on(c, s + 1, way).start()
    for copy in totals:
        copy.wait_send()
    for s in range(far):
        for c in range(len(parcels)):
            for way in range(2):
                pass_on(c, s, way).wait_send()


def flush_kernel(n, fg, fu, fd, wide, *refs):
    outs, sem = refs[:9], refs[9]
    layers, d = fg.shape[0], fg.shape[1]
    rows, far = d // n, n // 2
    deep = far * rows
    copies = []
    for k, (i, layer) in enumerate((i, layer) for layer in (1, 0) for i in range(3)):
        for c in range(2):
            out = outs[3 + 3 * c + i]
            if i == 2:
                copies.append((wide.at[k, pl.ds(c * deep, deep), :], out.at[layer]))
            else:
                copies += [(wide.at[k, pl.ds(c * deep + b * rows, rows), :], out.at[layer, :, pl.ds(b * d, d)]) for b in range(far)]
    copies += [(f.at[layer], out.at[layer]) for layer in range(layers) for f, out in zip((fg, fu, fd), outs)]
    copies = [pltpu.make_async_copy(*pair, sem.at[i]) for i, pair in enumerate(copies)]
    for copy in copies:
        copy.start()
    for copy in copies:
        copy.wait()


def train_step(x, dy, w, m, v, n):
    wg, wu, wd = w
    tokens, d = x.shape[1:]
    layers, _, f = wg.shape
    nt, nc = tokens // TT, f // FC
    far, rows = n // 2, d // n
    pieces = 3 * layers
    parcels = pieces + 2 * 2 * EARLY
    hbm = pl.BlockSpec(memory_space=pl.ANY)
    vmem = pl.BlockSpec(memory_space=pltpu.VMEM)
    shape = jax.ShapeDtypeStruct
    kept = [pltpu.VMEM(one.shape, BF16) for one in w] + [pltpu.VMEM((nt, TT, d), F32)]
    v_, dma = pltpu.VMEM, pltpu.SemaphoreType.DMA
    scratch = [
        v_((2, 2 * FC, d), BF16), v_((2, d, FC), BF16),
        v_((nt, TT, d), BF16), v_((nt, d, TT), BF16), v_((nt, TT, d), BF16), v_((nt, TT, d), BF16), v_((nt, d, TT), BF16),
        v_((2 * nc, TT, LB), BF16), v_((TT, FC), BF16), v_((TT, FC), BF16), v_((TT, 2 * FC), BF16), v_((TT, 2 * FC), BF16),
        v_((UNITS_HELD, d, 2 * FC), F32), v_((UNITS_HELD, 2, d, LB), F32),
        v_((2, RECEIVED, far, 2, rows, FC), BF16), v_((2, 2, far, 2, rows, FC), BF16), v_((EARLY, 2, rows, FC), BF16),
        v_((layers, rows, f), BF16), v_((layers, rows, f), BF16), v_((layers, f // n, d), BF16), v_((8, LB), F32), v_((n, 8, LB), F32),
        dma((layers, 3)), dma((nt,)), dma((nt,)), dma((2,)), dma((2 * nc + 6,)), dma((nt,)),
        dma((2, RECEIVED, far)), dma((2, far)), dma((2, 2, far)), dma((2, far)), dma((n,)), dma((n,)),
        dma((pieces, n)), dma((2, far, parcels)), dma((2, far, parcels)),
        pltpu.SemaphoreType.REGULAR, dma((EARLY, 8)), dma((2, far, EARLY)), dma((2, far, EARLY)), dma((2, far, EARLY)), dma((2, far, EARLY)),
        dma((n - 1, EARLY, 2)),
    ]
    kept_bytes = 2 * sum(one.size for one in w) + 4 * tokens * d
    *new, wide, _, _, _, _ = pl.pallas_call(
        functools.partial(step_kernel, nt, nc, n, sum(one.size for one in w)),
        name="train_step",
        out_shape=kept + [shape((nc, nt, TT, 2 * FC), F32), shape((nt, d, TT), BF16),
                          shape((EARLY, n, d, LB), F32), shape((EARLY, n, 2, rows, FC), BF16)],
        in_specs=[hbm] * 11,
        out_specs=[vmem] * 4 + [hbm] * 4,
        scratch_shapes=scratch,
        compiler_params=pltpu.CompilerParams(vmem_limit_bytes=VMEM_BYTES - kept_bytes, collective_id=0, has_side_effects=True),
    )(x, dy, *w, *m, *v)
    copies = layers * (2 * (2 * far + 1) + 3)
    keep = lambda one: pltpu.with_memory_space_constraint(one, pltpu.VMEM)
    return tuple(pl.pallas_call(
        functools.partial(flush_kernel, n),
        name="flush",
        out_shape=[shape(one.shape, one.dtype) for group in (w, m, v) for one in group],
        in_specs=[vmem] * 4,
        out_specs=[hbm] * 9,
        scratch_shapes=[dma((copies,))],
        compiler_params=pltpu.CompilerParams(vmem_limit_bytes=1 << 20),
    )(*(keep(one) for one in (*new, wide))))


def solution(mesh):
    n = mesh.shape["dp"]

    def step(x, dy, *arrays):
        return train_step(x, dy, *(arrays[i:i + 3] for i in (0, 3, 6)), n)

    seq, rows = P(("rep", "dp"), None, None), P(None, "dp", None)
    return jax.shard_map(
        step,
        mesh=mesh,
        in_specs=(seq, seq) + (P(),) * 3 + (rows,) * 6,
        out_specs=(P("rep"),) * 3 + (P("rep", "dp"),) * 6,
        check_vma=False,
    )
```

```python
import functools

import jax
import jax.numpy as jnp
from jax import lax
from jax.experimental import pallas as pl
from jax.experimental.pallas import tpu as pltpu
from jax.sharding import PartitionSpec as P

F32, BF16 = jnp.float32, jnp.bfloat16
MESH = pl.DeviceIdType.MESH
TT = 512
LB = 128
EARLY = 2
STAGED = 4
FC = 2 * LB
RECEIVED = 6
UNITS_HELD = 7
VMEM_BYTES = 67_043_328
PLACES = tuple(tuple(int(p) for p in line.split(",")) for line in (
    "4,8,12,16,20,24,29,33,40,44,48,52,56,60,64",
    "6,11,15,21,23,27,36,41,45,47,53,57,61,66",
    "9,14,18,25,29,30,42,45,50,54,59,63,65",
    "12,17,21,31,35,37,49,51,56,62,63",
    "15,20,27,41,46,48,54,57,61",
))
LAST = tuple((what[0], *(int(p) for p in what[1:].split("."))) for line in (
    "g15.0,g11.3,d14.1,d15.0,d9.4,d11.3,d12.3,d13.2,g14.1,g12.3",
    "d10.4,g15.1,d15.1,g13.2,g9.4,d14.2,g14.2,g10.4,d11.4,d12.4",
    "g11.4,g15.2,d15.2,g12.4,d13.3,g13.3,g14.3,d14.3,g15.3,d15.3",
    "g13.4,d13.4,d14.4,g14.4,g15.4,d15.4",
) for what in line.split(","))
EARLY_PLACES = tuple((what[0], *(int(p) for p in what[1:].split("."))) for line in (
    "m1.2.0,m0.3.4,m1.3.6,s0.0.15,s0.1.19,s1.0.20,s1.1.23,s0.2.24",
    "s1.2.28,s0.3.29,s1.3.31",
) for what in line.split(","))


def dot(a, b):
    return jnp.dot(a, b, preferred_element_type=F32)


def rms(wide):
    return lax.rsqrt(jnp.mean(wide * wide, -1, keepdims=True) + 1e-6)


def sigmoid(g):
    return 0.5 * jnp.tanh(0.5 * g) + 0.5


def step_kernel(nt, nc, n, count, x_h, dy_h, wg_h, wu_h, wd_h, mg_h, mu_h, md_h, vg_h, vu_h, vd_h,
                fg, fu, fd, wide_ref, gu_h, a1t_h, mv_h, gs_h,
                wgut, wdt, a, at, h1, dy, dyt, hid, hd0, hd1, dgu0, dgu1,
                pg, pd, rg, sg, gs, og, ou, od, ss, tots,
                sem_w, sem_x, sem_dy, sem_at, sem_gu, sem_gi, rg_sem, rd_sem, sg_sem, sd_sem, ts_sem, tr_sem, mv_sem, ag_send, ag_recv,
                free_sem, early_sem, ms_sem, mr_sem, gs_sem, gr_sem, late_sem):
    half, far = nc // 2, n // 2
    units = 2 * nc
    rows = pg.shape[1] // n
    hds, dgus = (hd0, hd1), (dgu0, dgu1)
    full, own_g = (fg, fu, fd), (og, ou, od)
    da = wide_ref
    me = lax.axis_index("dp")
    around = [lax.rem(me + k, n) for k in range(n)]
    towards = (around[1], around[n - 1])

    barrier = pltpu.get_barrier_semaphore()
    for k in range(1, n):
        pl.semaphore_signal(barrier, inc=1, device_id={"dp": around[k]}, device_id_type=MESH)

    def block(j):
        return 2 * lax.rem(j, half) + j // half

    def at_block(b):
        return pl.ds(b * LB if isinstance(b, int) else pl.multiple_of(b * LB, LB), LB)

    def x_copy(t):
        return pltpu.make_async_copy(x_h.at[0, pl.ds(t * TT, TT), :], a.at[t], sem_x.at[t])

    def dy_copy(t):
        return pltpu.make_async_copy(dy_h.at[0, pl.ds(t * TT, TT), :], dy.at[t], sem_dy.at[t])

    def w_copies(layer):
        return [pltpu.make_async_copy(h.at[layer], v.at[layer], sem_w.at[layer, i]) for i, (h, v) in enumerate(zip((wg_h, wu_h, wd_h), full))]

    x_copy(0).start()
    for copy in w_copies(0):
        copy.start()
    ss[...] = jnp.zeros_like(ss)

    def staged(odd, j):
        if not odd:
            return [(da.at[j], 0, 2 * FC)]
        if j < UNITS_HELD:
            return [(pg.at[j], 0, 2 * FC)]
        return [(pd.at[UNITS_HELD - 2 + i // 2, i % 2], i * LB, LB) for i in range(2 * FC // LB)]

    def gu_out(t, odd, j):
        return [pltpu.make_async_copy(ref, gu_h.at[j, t, :, pl.ds(at_, width)], sem_gu.at[odd * (nc + 3) + j + i])
                for i, (ref, at_, width) in enumerate(staged(odd, j))]

    def gu_out_all(t, odd):
        return [copy for j in range(nc) for copy in gu_out(t, odd, j)]

    def a1t_out(t):
        p = lax.rem(t, 2)
        return pltpu.make_async_copy(wgut.at[p], a1t_h.at[t], sem_at.at[p])

    def origin_of(s, way):
        return around[(n - s) % n] if way == 0 else around[s]

    def half_of(ref, s, way):
        size = ref.shape[0] // 2
        return ref.at[pl.ds(way * size, size)] if s == far - 1 else ref

    def kept_moments(j, s, way):
        return pd.at[2 * s + j, way] if s < 2 else mv_h.at[j, origin_of(s + 1, way)]

    def moments_on(j, s, way):
        here = kept_moments(j, s - 1, way) if s else pd.at[STAGED, j]
        there = pd.at[2 * s + j, way] if s < 2 else mv_h.at[j, origin_of(s, way)]
        return pltpu.make_async_remote_copy(
            half_of(here, s, way), half_of(there, s, way), ms_sem.at[way, s, j], mr_sem.at[way, s, j],
            device_id={"dp": towards[way]}, device_id_type=MESH)

    def moments_in(j, s, way):
        here = half_of(kept_moments(j, s, way), s, way)
        return pltpu.make_async_remote_copy(
            here, here, ms_sem.at[way, s, j], mr_sem.at[way, s, j], device_id={"dp": towards[way]}, device_id_type=MESH)

    def moments_out(j, s, way):
        return pltpu.make_async_copy(kept_moments(j, s, way), mv_h.at[j, origin_of(s + 1, way)], early_sem.at[j, 2 * s + way])

    def moments_left(j, s):
        for way in range(2):
            moments_on(j, s, way).wait_send()
            if s:
                moments_out(j, s - 1, way).wait()

    def sums_on(j, s, way, coming=False):
        back_by = s + coming
        there = gs_h.at[j, origin_of(back_by, way)]
        here = there if back_by else gs.at[j]
        return pltpu.make_async_remote_copy(
            half_of(here, s, way), half_of(there, s, way), gs_sem.at[way, s, j], gr_sem.at[way, s, j],
            device_id={"dp": towards[way]}, device_id_type=MESH)

    def sums_in(j, s, way):
        return sums_on(j, s, way, True)

    def forward_on(which, j, s):
        for way in range(2):
            moments = which is moments_on
            if s > 0:
                (moments_in if moments else sums_in)(j, s - 1, way).wait_recv()
            which(j, s, way).start()
            if moments and 0 < s < 3:
                moments_out(j, s - 1, way).start()

    def early_moments():
        copies = []
        for j in range(EARLY):
            for i, pair in enumerate(((mg_h, vg_h), (mu_h, vu_h))):
                for c, h in enumerate(pair):
                    for b in range(2):
                        part = 4 * i + 2 * c + b
                        copies.append(pltpu.make_async_copy(
                            h.at[1, :, at_block(static_block(j) + b * nc)], pd.at[STAGED, j, pl.ds(part * rows, rows), :], early_sem.at[j, part]))
        return copies

    def static_block(j):
        return 2 * (j % half) + j // half

    def down():
        w = jnp.concatenate([fd[0, at_block(static_block(j) + s * nc), :] for j in range(nc) for s in range(2)], 0)
        return dot(jnp.concatenate([hid[b] for b in range(2 * nc)], 1), w)

    def gate_up(odd, j):
        cols = [at_block(static_block(j) + s * nc) for s in range(2)]
        gu = dot(dgu0[...], jnp.concatenate([f[0, :, c] for f in (fg, fu) for c in cols], 1))
        for ref, at_, width in staged(odd, j):
            ref[...] = gu[:, at_:at_ + width]
        g, u = gu[:, :FC], gu[:, FC:]
        h = (g * sigmoid(g) * u).astype(BF16)
        for s in range(2):
            hid[2 * j + s] = h[:, s * LB:(s + 1) * LB]

    def finish(t, y):
        h = (a[t].astype(F32) + y.astype(BF16).astype(F32)).astype(BF16)
        h1[t] = h
        wide = h.astype(F32)
        a2 = (wide * rms(wide)).astype(BF16)
        a[t] = a2
        at[t] = a2.T
        dyt[t] = dy[t].T

    def forward(t, odd, follows):
        x_copy(t).wait()
        if follows:
            dy_copy(t - 1).wait()

        @pl.when(t >= 2)
        def _():
            a1t_out(t - 2).wait()
            for copy in gu_out_all(t - 2, odd):
                copy.wait()

        if follows:
            y = down()
        wide = a[t].astype(F32)
        a1 = (wide * rms(wide)).astype(BF16)
        dgu0[...] = a1
        wgut[lax.rem(t, 2)] = a1.T
        for j in range(nc):
            gate_up(odd, j)
            if j == half and follows:
                finish(t - 1, y)
        for copy in gu_out_all(t, odd):
            copy.start()
        a1t_out(t).start()

    for copy in w_copies(0):
        copy.wait()
    dy_copy(0).start()
    for t in range(1, nt):
        x_copy(t).start()
        dy_copy(t).start()
    for copy in early_moments():
        copy.start()
    for copy in w_copies(1):
        copy.start()
    forward(0, 0, False)
    for copy in early_moments():
        copy.wait()
    pl.semaphore_wait(barrier, n - 1)
    for j in range(EARLY):
        forward_on(moments_on, j, 0)

    @pl.loop(0, nt // 2 - 1)
    def _(i):
        forward(2 * i + 1, 1, True)

        @pl.when(i == 2)
        def _():
            forward_on(moments_on, 1, 1)

        forward(2 * i + 2, 0, True)

        @pl.when(i == 1)
        def _():
            forward_on(moments_on, 0, 1)

    forward(nt - 1, 1, True)
    forward_on(moments_on, 0, 2)
    dy_copy(nt - 1).wait()
    finish(nt - 1, down())
    for copy in gu_out_all(nt - 2, 0):
        copy.wait()
    for t in (nt - 2, nt - 1):
        a1t_out(t).wait()
    for copy in gu_out(nt - 1, 1, 0):
        copy.wait()
    for copy in w_copies(1):
        copy.wait()

    for other in towards:
        pl.semaphore_signal(free_sem, inc=1, device_id={"dp": other}, device_id_type=MESH)

    def g_copy(u, s, way, both):
        part = (lambda ref: ref) if both else (lambda ref: ref.at[way])
        old, new = lax.rem(u, 2), lax.rem(u, RECEIVED)
        return pltpu.make_async_remote_copy(
            part(sg.at[way, old, s]), part(rg.at[way, new, s]), sg_sem.at[way, old, s], rg_sem.at[way, new, s],
            device_id={"dp": towards[way]}, device_id_type=MESH)

    tall = pd.shape[2] // 2

    def d_at(way, k, sent):
        return hid.at[(2 * sent + way) * far + k]

    def d_copy(j, way, both):
        k = lax.rem(j, far)
        part = (lambda ref: ref) if both else (lambda ref: ref.at[pl.ds(way * tall, tall), :])
        return pltpu.make_async_remote_copy(
            part(d_at(way, k, 1)), part(d_at(way, k, 0)), sd_sem.at[way, k], rd_sem.at[way, k],
            device_id={"dp": towards[way]}, device_id_type=MESH)

    def relay_g(u, s):
        slot, old, new = lax.rem(u, UNITS_HELD), lax.rem(u, 2), lax.rem(u, RECEIVED)
        for way in range(2):
            e = around[far - s] if way == 0 else around[n - far + s]

            @pl.when(u > 1)
            def _():
                g_copy(u - 2, s, way, s > 0).wait_send()

            if s > 0:
                g_copy(u, s - 1, way, s > 1).wait_recv()
            for h in range(2):
                if s == 0 and h != way:
                    continue
                own = pg[slot, pl.ds(pl.multiple_of(e * rows, rows), rows), h * FC:(h + 1) * FC]
                if s > 1 or (s == 1 and h == way):
                    own += rg[way, new, s - 1, h].astype(F32)
                sg[way, old, s, h] = own.astype(BF16)
            g_copy(u, s, way, s > 0).start()

    def relay_d(u, s):
        j, slot = lax.rem(u, nc), lax.rem(u, UNITS_HELD)
        k = lax.rem(j, far)
        for way in range(2):
            e = around[far - s] if way == 0 else around[n - far + s]

            @pl.when(lax.rem(e, far) == k)
            def _():
                @pl.when(u >= far)
                def _():
                    d_copy(j, way, s > 0).wait_send()

                if s > 0:
                    d_copy(j, way, s > 1).wait_recv()
                for h in range(2):
                    if s == 0 and h != way:
                        continue
                    part = pl.ds(h * tall, tall)
                    own = pd[slot, e // far, part, :]
                    if s > 1 or (s == 1 and h == way):
                        own += d_at(way, k, 0)[part, :].astype(F32)
                    d_at(way, k, 1)[part, :] = own.astype(BF16)
                d_copy(j, way, s > 0).start()

    def square(g):
        wide = g.astype(F32)
        ss[...] += jnp.sum((wide * wide).reshape(-1, *ss.shape), 0)

    def arrive_g(u):
        j, slot, new, layer = lax.rem(u, nc), lax.rem(u, UNITS_HELD), lax.rem(u, RECEIVED), 1 - u // nc
        for way in range(2):
            g_copy(u, far - 1, way, True).wait_recv()
        for h, out in enumerate((og, ou)):
            own = pg[slot, pl.ds(pl.multiple_of(me * rows, rows), rows), h * FC:(h + 1) * FC]
            own = (own + rg[0, new, far - 1, h].astype(F32) + rg[1, new, far - 1, h].astype(F32)).astype(BF16)
            for s in range(2):
                piece = own[:, s * LB:(s + 1) * LB]
                out[layer, :, at_block(block(j) + s * nc)] = piece
                square(piece)

            @pl.when(u < EARLY)
            def _(own=own, h=h):
                gs[jnp.minimum(u, EARLY - 1), h] = own

    def arrive_d(u):
        j, slot, layer = lax.rem(u, nc), lax.rem(u, UNITS_HELD), 1 - u // nc
        k = lax.rem(j, far)

        @pl.when(lax.rem(me, far) == k)
        def _():
            for way in range(2):
                d_copy(j, way, True).wait_recv()
            for h in range(2):
                part = pl.ds(h * tall, tall)
                own = pd[slot, me // far, part, :]
                own = own + d_at(0, k, 0)[part, :].astype(F32) + d_at(1, k, 0)[part, :].astype(F32)
                own = own.T.astype(BF16)
                od[layer, at_block(j // half), h * tall:(h + 1) * tall] = own
                for s in range(tall // LB):
                    square(own[:, s * LB:(s + 1) * LB])

    def go_on(kind, u, s):
        if s == far:
            (arrive_g if kind == "g" else arrive_d)(u)
        else:
            (relay_g if kind == "g" else relay_d)(u, s)

    def turn_round(place, first, end):
        for s in range(far, -1, -1):
            here = [p for p in PLACES[s] if first <= p < end]
            if not here:
                continue
            u = sum((place > p).astype(jnp.int32) for p in here) + PLACES[s].index(here[0])
            due = functools.reduce(jnp.logical_or, [place == p for p in here])

            @pl.when(due)
            def _(s=s, u=u):
                go_on("g", u, s)
                go_on("d", u, s)

    def elementwise(gu, dh, slot):
        g, u = gu[:, :FC], gu[:, FC:]
        sig = sigmoid(g)
        silu = g * sig
        hds[slot][...] = (silu * u).astype(BF16)
        dgus[slot][:, :FC] = (dh * u * (sig + silu * (1 - sig))).astype(BF16)
        dgus[slot][:, FC:] = (dh * silu).astype(BF16)

    def keep_from(first):
        return (lambda old: old) if first is None else (lambda old: jnp.where(first, jnp.zeros_like(old), old))

    def back_g(u, t, slot, first=None):
        k, keep = lax.rem(u, UNITS_HELD), keep_from(first)
        pg[k] = keep(pg[k]) + dot(at[t], dgus[slot][...])

    def back_d(u, t, slot, first=None):
        k, keep = lax.rem(u, UNITS_HELD), keep_from(first)
        hd = dot(dyt[t], hds[slot][...])
        for s in range(2):
            pd[k, s] = keep(pd[k, s]) + hd[:, s * LB:(s + 1) * LB]

    def to_states(u, t, slot):
        old = jnp.where(u == 0, jnp.zeros(da.shape[1:], F32), da[t])
        da[t] = old + dot(dgus[slot][...], wgut[lax.rem(u, 2)])

    def turn(layer, j, t):
        p = lax.rem(j, 2)
        if layer:
            for i, f in enumerate((fg, fu)):
                s = lax.rem(t, 2)
                wgut[p, pl.ds(pl.multiple_of(i * FC + s * LB, LB), LB), :] = f[layer, :, at_block(block(j) + s * nc)].T
        s = lax.rem(t, 2)
        wdt[p, :, at_block(s)] = fd[layer, at_block(block(j) + s * nc), :].T

    def clear():
        for h, g in zip(hds, dgus):
            h[...] = jnp.zeros_like(h)
            g[...] = jnp.zeros_like(g)

    per_chunk = nt // 2
    steps = nc * per_chunk
    pl.semaphore_wait(free_sem, 2)
    moments_left(0, 1)

    for t in range(2):
        turn(1, 0, t)
    clear()

    def front2(j, t, slot):
        cols = [at_block(block(j) + s * nc) for s in range(2)]
        gu = dot(a[t], jnp.concatenate([f[1, :, c] for f in (fg, fu) for c in cols], 1))
        elementwise(gu, dot(dy[t], wdt[lax.rem(j, 2)]).astype(BF16).astype(F32), slot)

    @pl.loop(0, nc * per_chunk)
    def _(i):
        j, t = i // per_chunk, 2 * lax.rem(i, per_chunk)
        k = jnp.maximum(2 * i - 1, 0)
        @pl.when(i == 2)
        def _():
            for copy in [c for k in range(1, nc) for c in gu_out(nt - 1, 1, k)]:
                copy.wait()

        jk, tk, jn = k // nt, lax.rem(k, nt), jnp.minimum(j + 1, nc - 1)
        to_states(jk, tk, 1)
        back_d(jk, tk, 1)
        front2(j, t, 0)
        to_states(j, t, 0)
        back_g(jk, tk, 1)
        turn(1, jn, t + 1)
        back_d(j, t, 0, t == 0)
        turn(1, jn, t)
        front2(j, t + 1, 1)
        back_g(j, t, 0, t == 0)
        turn_round(i, 0, steps)
        for chunk, whose in ((1, ((1, 1),)), (2, ((0, 2),)), (3, ((1, 2),)), (STAGED, ((0, 0), (1, 0)))):
            @pl.when(i == chunk * per_chunk - 1)
            def _(whose=whose):
                for j, s in whose:
                    moments_left(j, s)

        for kind, which in (("m", moments_on), ("s", sums_on)):
            due = [what for what in EARLY_PLACES if what[0] == kind]

            @pl.when((i >= due[0][3]) & (i <= due[-1][3]))
            def _(which=which, due=due):
                for _, j, s, place in due:
                    @pl.when(i == place)
                    def _(j=j, s=s):
                        forward_on(which, j, s)

    to_states(nc - 1, nt - 1, 1)
    back_d(nc - 1, nt - 1, 1)
    back_g(nc - 1, nt - 1, 1)

    def a1t_in(t):
        return pltpu.make_async_copy(a1t_h.at[t], at.at[t], sem_dy.at[t])

    def gu_in(i):
        return pltpu.make_async_copy(gu_h.at[i // nt, lax.rem(i, nt)], da.at[lax.rem(i, nt)], sem_gi.at[lax.rem(i, nt)])

    for t in range(nt):
        a1t_in(t).start()

    @pl.loop(0, nt)
    def _(t):
        wide = h1[t].astype(F32)
        r = rms(wide)
        da_t = da[t].astype(BF16).astype(F32)
        dn = da_t * r - wide * (r * r * r * jnp.mean(da_t * wide, -1, keepdims=True))
        dh1 = (dy[t].astype(F32) + dn).astype(BF16)
        dy[t] = dh1
        dyt[t] = dh1.T
        gu_in(t).start()
        a1t_in(t).wait()

        @pl.when(lax.rem(t, 2) == 1)
        def _():
            turn_round(steps + t // 2, steps, steps + far)

    for t in range(2):
        turn(0, 0, t)
    clear()

    def front1(j, t, slot):
        elementwise(da[t], dot(dy[t], wdt[lax.rem(j, 2)]).astype(BF16).astype(F32), slot)

    @pl.loop(0, nc * per_chunk)
    def _(i):
        j, t = i // per_chunk, 2 * lax.rem(i, per_chunk)
        k = jnp.maximum(2 * i - 1, 0)
        for s in range(2):
            gu_in(2 * i + s).wait()
        jk, tk, jn = nc + k // nt, lax.rem(k, nt), jnp.minimum(j + 1, nc - 1)
        turn(0, jn, t + 1)
        back_d(jk, tk, 1)
        turn(0, jn, t)
        back_g(jk, tk, 1)
        front1(j, t, 0)
        back_d(nc + j, t, 0, t == 0)
        front1(j, t + 1, 1)
        back_g(nc + j, t, 0, t == 0)

        @pl.when(j + 1 < nc)
        def _():
            for s in range(2):
                gu_in(2 * i + s + nt).start()

        turn_round(steps + far + i, steps + far, 2 * steps + far)

    back_d(2 * nc - 1, nt - 1, 1)
    back_g(2 * nc - 1, nt - 1, 1)

    pieces = [(i, layer) for layer in (1, 0) for i in range(3)]
    d = h1.shape[2]
    deep = n // 2 * rows

    def moment_copies(k):
        i, layer = pieces[k]
        made = []
        for c, h in enumerate(((mg_h, mu_h, md_h)[i], (vg_h, vu_h, vd_h)[i])):
            if i == 2:
                made.append(pltpu.make_async_copy(h.at[layer], da.at[k, pl.ds(c * deep, deep), :], mv_sem.at[k, c]))
            else:
                for b in range(far):
                    made.append(pltpu.make_async_copy(
                        h.at[layer, :, pl.ds(b * d, d)], da.at[k, pl.ds(c * deep + b * rows, rows), :], mv_sem.at[k, c * far + b]))
        return made

    for k in range(len(pieces)):
        for copy in moment_copies(k):
            copy.start()

    for kind, u, s in LAST:
        go_on(kind, jnp.int32(u), s)

    def early_loads(k):
        made = []
        for j in range(EARLY):
            made.append(pltpu.make_async_copy(mv_h.at[j, around[k]], pd.at[k - 1, j], late_sem.at[k - 1, j, 0]))
            made.append(pltpu.make_async_copy(gs_h.at[j, around[k]], rg.at[j, (k - 1) // far, (k - 1) % far], late_sem.at[k - 1, j, 1]))
        return made

    for j in range(EARLY):
        for way in range(2):
            moments_in(j, far - 1, way).wait_recv()
            moments_on(j, far - 1, way).wait_send()
            sums_in(j, far - 1, way).wait_recv()
            for s in range(far):
                sums_on(j, s, way).wait_send()
    for k in range(1, n):
        for copy in early_loads(k):
            copy.start()

    tots[pl.ds(me, 1)] = ss[...][None]
    totals = [
        pltpu.make_async_remote_copy(ss, tots.at[me], ts_sem.at[k], tr_sem.at[n - k], device_id={"dp": around[k]}, device_id_type=MESH)
        for k in range(1, n)
    ]
    for copy in totals:
        copy.start()
    for way in range(2):
        for s in range(far):
            for u in (units - 2, units - 1):
                g_copy(u, s, way, s > 0).wait_send()
            e = around[far - s] if way == 0 else around[n - far + s]
            d_copy(lax.rem(e, far), way, s > 0).wait_send()
    for k in range(len(pieces)):
        for copy in moment_copies(k):
            copy.wait()
    for k in range(1, n):
        pltpu.make_async_remote_copy(ss, tots.at[around[k]], ts_sem.at[k], tr_sem.at[k], device_id={"dp": around[k]}, device_id_type=MESH).wait_recv()
    factor = jnp.minimum(1.0, 0.5 * lax.rsqrt(jnp.sum(tots[...], keepdims=True).reshape(1, 1) / count + 1e-30))

    def rows_of(i, origin, part=None):
        tall = full[i].shape[1] // n
        start = origin * tall
        if part is not None:
            tall //= 2
            start += part * tall
        return pl.ds(pl.multiple_of(start, tall), tall)

    early = sorted(static_block(j) + s * nc for j in range(EARLY) for s in range(2))
    between = [(p + 1, q) for p, q in zip([-1] + early, early + [2 * nc]) if q > p + 1]
    parcels = [(k, i, layer, cols) for k, (i, layer) in enumerate(pieces)
               for cols in ([pl.ds(p * LB, (q - p) * LB) for p, q in between] if layer == 1 and i < 2 else [slice(None)])]

    def pass_on(c, s, way, coming=False):
        _, i, layer, cols = parcels[c]
        back_by = s + coming
        origin = around[(n - back_by) % n] if way == 0 else around[back_by]
        here = full[i].at[layer, rows_of(i, origin, way if s == far - 1 else None), cols]
        return pltpu.make_async_remote_copy(
            here, here, ag_send.at[way, s, c], ag_recv.at[way, s, c], device_id={"dp": towards[way]}, device_id_type=MESH)

    for k, (i, layer) in enumerate(pieces):
        def adamw(here, where_g, where_w):
            m_at, v_at = here, pl.ds(here.start + deep, here.size)
            g = own_g[i][(layer, *where_g)].astype(F32) * factor
            m = 0.9 * da[k, m_at, :] + 0.1 * g
            v = 0.95 * da[k, v_at, :] + 0.05 * g * g
            w = full[i][(layer, *where_w)].astype(F32)
            step = m * lax.rsqrt(v + 1e-8) + 0.1 * w
            da[k, m_at, :] = m
            da[k, v_at, :] = v
            full[i][(layer, *where_w)] = (w - 0.02 * step).astype(BF16)

        for b in range(far):
            here = pl.ds(b * rows, rows)
            if i == 2:
                adamw(here, (here, slice(None)), (pl.ds(pl.multiple_of(me * deep + b * rows, rows), rows), slice(None)))
            else:
                cols = pl.ds(b * d, d)
                adamw(here, (slice(None), cols), (pl.ds(pl.multiple_of(me * rows, rows), rows), cols))
        for c, parcel in enumerate(parcels):
            if parcel[0] == k:
                for way in range(2):
                    pass_on(c, 0, way).start()

    for k in range(1, n):
        for copy in early_loads(k):
            copy.wait()

    @pl.loop(1, n)
    def _(k):
        origin = lax.rem(me + k, n)
        mine = pl.ds(pl.multiple_of(origin * rows, rows), rows)
        for j in range(EARLY):
            for i, f in enumerate((fg, fu)):
                for b in range(2):
                    cols = at_block(static_block(j) + b * nc)
                    g = rg[j, (k - 1) // far, lax.rem(k - 1, far), i, :, b * LB:(b + 1) * LB].astype(F32) * factor
                    m = 0.9 * pd[k - 1, j, (4 * i + b) * rows:(4 * i + b + 1) * rows, :] + 0.1 * g
                    v = 0.95 * pd[k - 1, j, (4 * i + 2 + b) * rows:(4 * i + 3 + b) * rows, :] + 0.05 * g * g
                    w = f[1, mine, cols].astype(F32)
                    f[1, mine, cols] = (w - 0.02 * (m * lax.rsqrt(v + 1e-8) + 0.1 * w)).astype(BF16)

    for s in range(far):
        for c in range(len(parcels)):
            for way in range(2):
                pass_on(c, s, way, True).wait_recv()
                if s + 1 < far:
                    pass_on(c, s + 1, way).start()
    for copy in totals:
        copy.wait_send()
    for s in range(far):
        for c in range(len(parcels)):
            for way in range(2):
                pass_on(c, s, way).wait_send()


def flush_kernel(n, fg, fu, fd, wide, *refs):
    outs, sem = refs[:9], refs[9]
    layers, d = fg.shape[0], fg.shape[1]
    rows, far = d // n, n // 2
    deep = far * rows
    copies = []
    for k, (i, layer) in enumerate((i, layer) for layer in (1, 0) for i in range(3)):
        for c in range(2):
            out = outs[3 + 3 * c + i]
            if i == 2:
                copies.append((wide.at[k, pl.ds(c * deep, deep), :], out.at[layer]))
            else:
                copies += [(wide.at[k, pl.ds(c * deep + b * rows, rows), :], out.at[layer, :, pl.ds(b * d, d)]) for b in range(far)]
    copies += [(f.at[layer], out.at[layer]) for layer in range(layers) for f, out in zip((fg, fu, fd), outs)]
    copies = [pltpu.make_async_copy(*pair, sem.at[i]) for i, pair in enumerate(copies)]
    for copy in copies:
        copy.start()
    for copy in copies:
        copy.wait()


def train_step(x, dy, w, m, v, n):
    wg, wu, wd = w
    tokens, d = x.shape[1:]
    layers, _, f = wg.shape
    nt, nc = tokens // TT, f // FC
    far, rows = n // 2, d // n
    pieces = 3 * layers
    parcels = pieces + 2 * 2 * EARLY
    hbm = pl.BlockSpec(memory_space=pl.ANY)
    vmem = pl.BlockSpec(memory_space=pltpu.VMEM)
    shape = jax.ShapeDtypeStruct
    kept = [pltpu.VMEM(one.shape, BF16) for one in w] + [pltpu.VMEM((nt, TT, d), F32)]
    v_, dma = pltpu.VMEM, pltpu.SemaphoreType.DMA
    scratch = [
        v_((2, 2 * FC, d), BF16), v_((2, d, FC), BF16),
        v_((nt, TT, d), BF16), v_((nt, d, TT), BF16), v_((nt, TT, d), BF16), v_((nt, TT, d), BF16), v_((nt, d, TT), BF16),
        v_((2 * nc, TT, LB), BF16), v_((TT, FC), BF16), v_((TT, FC), BF16), v_((TT, 2 * FC), BF16), v_((TT, 2 * FC), BF16),
        v_((UNITS_HELD, d, 2 * FC), F32), v_((UNITS_HELD, 2, d, LB), F32),
        v_((2, RECEIVED, far, 2, rows, FC), BF16), v_((2, 2, far, 2, rows, FC), BF16), v_((EARLY, 2, rows, FC), BF16),
        v_((layers, rows, f), BF16), v_((layers, rows, f), BF16), v_((layers, f // n, d), BF16), v_((8, LB), F32), v_((n, 8, LB), F32),
        dma((layers, 3)), dma((nt,)), dma((nt,)), dma((2,)), dma((2 * nc + 6,)), dma((nt,)),
        dma((2, RECEIVED, far)), dma((2, far)), dma((2, 2, far)), dma((2, far)), dma((n,)), dma((n,)),
        dma((pieces, n)), dma((2, far, parcels)), dma((2, far, parcels)),
        pltpu.SemaphoreType.REGULAR, dma((EARLY, 8)), dma((2, far, EARLY)), dma((2, far, EARLY)), dma((2, far, EARLY)), dma((2, far, EARLY)),
        dma((n - 1, EARLY, 2)),
    ]
    kept_bytes = 2 * sum(one.size for one in w) + 4 * tokens * d
    *new, wide, _, _, _, _ = pl.pallas_call(
        functools.partial(step_kernel, nt, nc, n, sum(one.size for one in w)),
        name="train_step",
        out_shape=kept + [shape((nc, nt, TT, 2 * FC), F32), shape((nt, d, TT), BF16),
                          shape((EARLY, n, d, LB), F32), shape((EARLY, n, 2, rows, FC), BF16)],
        in_specs=[hbm] * 11,
        out_specs=[vmem] * 4 + [hbm] * 4,
        scratch_shapes=scratch,
        compiler_params=pltpu.CompilerParams(vmem_limit_bytes=VMEM_BYTES - kept_bytes, collective_id=0, has_side_effects=True),
    )(x, dy, *w, *m, *v)
    copies = layers * (2 * (2 * far + 1) + 3)
    keep = lambda one: pltpu.with_memory_space_constraint(one, pltpu.VMEM)
    return tuple(pl.pallas_call(
        functools.partial(flush_kernel, n),
        name="flush",
        out_shape=[shape(one.shape, one.dtype) for group in (w, m, v) for one in group],
        in_specs=[vmem] * 4,
        out_specs=[hbm] * 9,
        scratch_shapes=[dma((copies,))],
        compiler_params=pltpu.CompilerParams(vmem_limit_bytes=1 << 20),
    )(*(keep(one) for one in (*new, wide))))


def solution(mesh):
    n = mesh.shape["dp"]

    def step(x, dy, *arrays):
        return train_step(x, dy, *(arrays[i:i + 3] for i in (0, 3, 6)), n)

    seq, rows = P(("rep", "dp"), None, None), P(None, "dp", None)
    return jax.shard_map(
        step,
        mesh=mesh,
        in_specs=(seq, seq) + (P(),) * 3 + (rows,) * 6,
        out_specs=(P("rep"),) * 3 + (P("rep", "dp"),) * 6,
        check_vma=False,
    )
```

```python
import functools

import jax
import jax.numpy as jnp
from jax import lax
from jax.experimental import pallas as pl
from jax.experimental.pallas import tpu as pltpu
from jax.sharding import PartitionSpec as P

F32, BF16 = jnp.float32, jnp.bfloat16
MESH = pl.DeviceIdType.MESH
TT = 512
LB = 128
EARLY = 2
STAGED = 4
FC = 2 * LB
RECEIVED = 6
UNITS_HELD = 7
VMEM_BYTES = 67_043_328
PLACES = tuple(tuple(int(p) for p in line.split(",")) for line in (
    "4,8,12,16,20,24,29,33,40,44,48,52,56,60,64",
    "6,11,15,21,23,27,36,41,45,47,53,57,61,66",
    "9,14,18,25,29,30,42,45,50,54,59,63,65",
    "12,17,21,31,35,37,49,51,56,62,63",
    "15,20,27,41,46,48,54,57,61",
))
LAST = tuple((what[0], *(int(p) for p in what[1:].split("."))) for line in (
    "g15.0,g11.3,d14.1,d15.0,d9.4,d11.3,d12.3,d13.2,g14.1,g12.3",
    "d10.4,g15.1,d15.1,g13.2,g9.4,d14.2,g14.2,g10.4,d11.4,d12.4",
    "g11.4,g15.2,d15.2,g12.4,d13.3,g13.3,g14.3,d14.3,g15.3,d15.3",
    "g13.4,d13.4,d14.4,g14.4,g15.4,d15.4",
) for what in line.split(","))
EARLY_PLACES = tuple((what[0], *(int(p) for p in what[1:].split("."))) for line in (
    "m1.2.0,m0.3.4,m1.3.6,s0.0.15,s0.1.19,s1.0.20,s1.1.23,s0.2.24",
    "s1.2.28,s0.3.29,s1.3.31",
) for what in line.split(","))


def dot(a, b):
    return jnp.dot(a, b, preferred_element_type=F32)


def rms(wide):
    return lax.rsqrt(jnp.mean(wide * wide, -1, keepdims=True) + 1e-6)


def sigmoid(g):
    return 0.5 * jnp.tanh(0.5 * g) + 0.5


def step_kernel(nt, nc, n, count, x_h, dy_h, wg_h, wu_h, wd_h, mg_h, mu_h, md_h, vg_h, vu_h, vd_h,
                fg, fu, fd, wide_ref, gu_h, a1t_h, mv_h, gs_h,
                wgut, wdt, a, at, h1, dy, dyt, hid, hd0, hd1, dgu0, dgu1,
                pg, pd, rg, sg, gs, og, ou, od, ss, tots,
                sem_w, sem_x, sem_dy, sem_at, sem_gu, sem_gi, rg_sem, rd_sem, sg_sem, sd_sem, ts_sem, tr_sem, mv_sem, ag_send, ag_recv,
                free_sem, early_sem, ms_sem, mr_sem, gs_sem, gr_sem, late_sem):
    half, far = nc // 2, n // 2
    units = 2 * nc
    rows = pg.shape[1] // n
    hds, dgus = (hd0, hd1), (dgu0, dgu1)
    full, own_g = (fg, fu, fd), (og, ou, od)
    da = wide_ref
    me = lax.axis_index("dp")
    around = [lax.rem(me + k, n) for k in range(n)]
    towards = (around[1], around[n - 1])

    barrier = pltpu.get_barrier_semaphore()
    for k in range(1, n):
        pl.semaphore_signal(barrier, inc=1, device_id={"dp": around[k]}, device_id_type=MESH)

    def block(j):
        return 2 * lax.rem(j, half) + j // half

    def at_block(b):
        return pl.ds(b * LB if isinstance(b, int) else pl.multiple_of(b * LB, LB), LB)

    def x_copy(t):
        return pltpu.make_async_copy(x_h.at[0, pl.ds(t * TT, TT), :], a.at[t], sem_x.at[t])

    def dy_copy(t):
        return pltpu.make_async_copy(dy_h.at[0, pl.ds(t * TT, TT), :], dy.at[t], sem_dy.at[t])

    def w_copies(layer):
        return [pltpu.make_async_copy(h.at[layer], v.at[layer], sem_w.at[layer, i]) for i, (h, v) in enumerate(zip((wg_h, wu_h, wd_h), full))]

    x_copy(0).start()
    for copy in w_copies(0):
        copy.start()
    ss[...] = jnp.zeros_like(ss)

    def staged(odd, j):
        if not odd:
            return [(da.at[j], 0, 2 * FC)]
        if j < UNITS_HELD:
            return [(pg.at[j], 0, 2 * FC)]
        return [(pd.at[UNITS_HELD - 2 + i // 2, i % 2], i * LB, LB) for i in range(2 * FC // LB)]

    def gu_out(t, odd, j):
        return [pltpu.make_async_copy(ref, gu_h.at[j, t, :, pl.ds(at_, width)], sem_gu.at[odd * (nc + 3) + j + i])
                for i, (ref, at_, width) in enumerate(staged(odd, j))]

    def gu_out_all(t, odd):
        return [copy for j in range(nc) for copy in gu_out(t, odd, j)]

    def a1t_out(t):
        p = lax.rem(t, 2)
        return pltpu.make_async_copy(wgut.at[p], a1t_h.at[t], sem_at.at[p])

    def origin_of(s, way):
        return around[(n - s) % n] if way == 0 else around[s]

    def half_of(ref, s, way):
        size = ref.shape[0] // 2
        return ref.at[pl.ds(way * size, size)] if s == far - 1 else ref

    def kept_moments(j, s, way):
        return pd.at[2 * s + j, way] if s < 2 else mv_h.at[j, origin_of(s + 1, way)]

    def moments_on(j, s, way):
        here = kept_moments(j, s - 1, way) if s else pd.at[STAGED, j]
        there = pd.at[2 * s + j, way] if s < 2 else mv_h.at[j, origin_of(s, way)]
        return pltpu.make_async_remote_copy(
            half_of(here, s, way), half_of(there, s, way), ms_sem.at[way, s, j], mr_sem.at[way, s, j],
            device_id={"dp": towards[way]}, device_id_type=MESH)

    def moments_in(j, s, way):
        here = half_of(kept_moments(j, s, way), s, way)
        return pltpu.make_async_remote_copy(
            here, here, ms_sem.at[way, s, j], mr_sem.at[way, s, j], device_id={"dp": towards[way]}, device_id_type=MESH)

    def moments_out(j, s, way):
        return pltpu.make_async_copy(kept_moments(j, s, way), mv_h.at[j, origin_of(s + 1, way)], early_sem.at[j, 2 * s + way])

    def moments_left(j, s):
        for way in range(2):
            moments_on(j, s, way).wait_send()
            if s:
                moments_out(j, s - 1, way).wait()

    def sums_on(j, s, way, coming=False):
        back_by = s + coming
        there = gs_h.at[j, origin_of(back_by, way)]
        here = there if back_by else gs.at[j]
        return pltpu.make_async_remote_copy(
            half_of(here, s, way), half_of(there, s, way), gs_sem.at[way, s, j], gr_sem.at[way, s, j],
            device_id={"dp": towards[way]}, device_id_type=MESH)

    def sums_in(j, s, way):
        return sums_on(j, s, way, True)

    def forward_on(which, j, s):
        for way in range(2):
            moments = which is moments_on
            if s > 0:
                (moments_in if moments else sums_in)(j, s - 1, way).wait_recv()
            which(j, s, way).start()
            if moments and 0 < s < 3:
                moments_out(j, s - 1, way).start()

    def early_moments():
        copies = []
        for j in range(EARLY):
            for i, pair in enumerate(((mg_h, vg_h), (mu_h, vu_h))):
                for c, h in enumerate(pair):
                    for b in range(2):
                        part = 4 * i + 2 * c + b
                        copies.append(pltpu.make_async_copy(
                            h.at[1, :, at_block(static_block(j) + b * nc)], pd.at[STAGED, j, pl.ds(part * rows, rows), :], early_sem.at[j, part]))
        return copies

    def static_block(j):
        return 2 * (j % half) + j // half

    def down():
        w = jnp.concatenate([fd[0, at_block(static_block(j) + s * nc), :] for j in range(nc) for s in range(2)], 0)
        return dot(jnp.concatenate([hid[b] for b in range(2 * nc)], 1), w)

    def gate_up(odd, j):
        cols = [at_block(static_block(j) + s * nc) for s in range(2)]
        gu = dot(dgu0[...], jnp.concatenate([f[0, :, c] for f in (fg, fu) for c in cols], 1))
        for ref, at_, width in staged(odd, j):
            ref[...] = gu[:, at_:at_ + width]
        g, u = gu[:, :FC], gu[:, FC:]
        h = (g * sigmoid(g) * u).astype(BF16)
        for s in range(2):
            hid[2 * j + s] = h[:, s * LB:(s + 1) * LB]

    def finish(t, y):
        h = (a[t].astype(F32) + y.astype(BF16).astype(F32)).astype(BF16)
        h1[t] = h
        wide = h.astype(F32)
        a2 = (wide * rms(wide)).astype(BF16)
        a[t] = a2
        at[t] = a2.T
        dyt[t] = dy[t].T

    def forward(t, odd, follows):
        x_copy(t).wait()
        if follows:
            dy_copy(t - 1).wait()

        @pl.when(t >= 2)
        def _():
            a1t_out(t - 2).wait()
            for copy in gu_out_all(t - 2, odd):
                copy.wait()

        if follows:
            y = down()
        wide = a[t].astype(F32)
        a1 = (wide * rms(wide)).astype(BF16)
        dgu0[...] = a1
        wgut[lax.rem(t, 2)] = a1.T
        for j in range(nc):
            gate_up(odd, j)
            if j == half and follows:
                finish(t - 1, y)
        for copy in gu_out_all(t, odd):
            copy.start()
        a1t_out(t).start()

    for copy in w_copies(0):
        copy.wait()
    dy_copy(0).start()
    for t in range(1, nt):
        x_copy(t).start()
        dy_copy(t).start()
    for copy in early_moments():
        copy.start()
    for copy in w_copies(1):
        copy.start()
    forward(0, 0, False)
    for copy in early_moments():
        copy.wait()
    pl.semaphore_wait(barrier, n - 1)
    for j in range(EARLY):
        forward_on(moments_on, j, 0)

    @pl.loop(0, nt // 2 - 1)
    def _(i):
        forward(2 * i + 1, 1, True)

        @pl.when(i == 2)
        def _():
            forward_on(moments_on, 1, 1)

        forward(2 * i + 2, 0, True)

        @pl.when(i == 1)
        def _():
            forward_on(moments_on, 0, 1)

    forward(nt - 1, 1, True)
    forward_on(moments_on, 0, 2)
    dy_copy(nt - 1).wait()
    finish(nt - 1, down())
    for copy in gu_out_all(nt - 2, 0):
        copy.wait()
    for t in (nt - 2, nt - 1):
        a1t_out(t).wait()
    for copy in gu_out(nt - 1, 1, 0):
        copy.wait()
    for copy in w_copies(1):
        copy.wait()

    for other in towards:
        pl.semaphore_signal(free_sem, inc=1, device_id={"dp": other}, device_id_type=MESH)

    def g_copy(u, s, way, both):
        part = (lambda ref: ref) if both else (lambda ref: ref.at[way])
        old, new = lax.rem(u, 2), lax.rem(u, RECEIVED)
        return pltpu.make_async_remote_copy(
            part(sg.at[way, old, s]), part(rg.at[way, new, s]), sg_sem.at[way, old, s], rg_sem.at[way, new, s],
            device_id={"dp": towards[way]}, device_id_type=MESH)

    tall = pd.shape[2] // 2

    def d_at(way, k, sent):
        return hid.at[(2 * sent + way) * far + k]

    def d_copy(j, way, both):
        k = lax.rem(j, far)
        part = (lambda ref: ref) if both else (lambda ref: ref.at[pl.ds(way * tall, tall), :])
        return pltpu.make_async_remote_copy(
            part(d_at(way, k, 1)), part(d_at(way, k, 0)), sd_sem.at[way, k], rd_sem.at[way, k],
            device_id={"dp": towards[way]}, device_id_type=MESH)

    def relay_g(u, s):
        slot, old, new = lax.rem(u, UNITS_HELD), lax.rem(u, 2), lax.rem(u, RECEIVED)
        for way in range(2):
            e = around[far - s] if way == 0 else around[n - far + s]

            @pl.when(u > 1)
            def _():
                g_copy(u - 2, s, way, s > 0).wait_send()

            if s > 0:
                g_copy(u, s - 1, way, s > 1).wait_recv()
            for h in range(2):
                if s == 0 and h != way:
                    continue
                own = pg[slot, pl.ds(pl.multiple_of(e * rows, rows), rows), h * FC:(h + 1) * FC]
                if s > 1 or (s == 1 and h == way):
                    own += rg[way, new, s - 1, h].astype(F32)
                sg[way, old, s, h] = own.astype(BF16)
            g_copy(u, s, way, s > 0).start()

    def relay_d(u, s):
        j, slot = lax.rem(u, nc), lax.rem(u, UNITS_HELD)
        k = lax.rem(j, far)
        for way in range(2):
            e = around[far - s] if way == 0 else around[n - far + s]

            @pl.when(lax.rem(e, far) == k)
            def _():
                @pl.when(u >= far)
                def _():
                    d_copy(j, way, s > 0).wait_send()

                if s > 0:
                    d_copy(j, way, s > 1).wait_recv()
                for h in range(2):
                    if s == 0 and h != way:
                        continue
                    part = pl.ds(h * tall, tall)
                    own = pd[slot, e // far, part, :]
                    if s > 1 or (s == 1 and h == way):
                        own += d_at(way, k, 0)[part, :].astype(F32)
                    d_at(way, k, 1)[part, :] = own.astype(BF16)
                d_copy(j, way, s > 0).start()

    def square(g):
        wide = g.astype(F32)
        ss[...] += jnp.sum((wide * wide).reshape(-1, *ss.shape), 0)

    def arrive_g(u):
        j, slot, new, layer = lax.rem(u, nc), lax.rem(u, UNITS_HELD), lax.rem(u, RECEIVED), 1 - u // nc
        for way in range(2):
            g_copy(u, far - 1, way, True).wait_recv()
        for h, out in enumerate((og, ou)):
            own = pg[slot, pl.ds(pl.multiple_of(me * rows, rows), rows), h * FC:(h + 1) * FC]
            own = (own + rg[0, new, far - 1, h].astype(F32) + rg[1, new, far - 1, h].astype(F32)).astype(BF16)
            for s in range(2):
                piece = own[:, s * LB:(s + 1) * LB]
                out[layer, :, at_block(block(j) + s * nc)] = piece
                square(piece)

            @pl.when(u < EARLY)
            def _(own=own, h=h):
                gs[jnp.minimum(u, EARLY - 1), h] = own

    def arrive_d(u):
        j, slot, layer = lax.rem(u, nc), lax.rem(u, UNITS_HELD), 1 - u // nc
        k = lax.rem(j, far)

        @pl.when(lax.rem(me, far) == k)
        def _():
            for way in range(2):
                d_copy(j, way, True).wait_recv()
            for h in range(2):
                part = pl.ds(h * tall, tall)
                own = pd[slot, me // far, part, :]
                own = own + d_at(0, k, 0)[part, :].astype(F32) + d_at(1, k, 0)[part, :].astype(F32)
                own = own.T.astype(BF16)
                od[layer, at_block(j // half), h * tall:(h + 1) * tall] = own
                for s in range(tall // LB):
                    square(own[:, s * LB:(s + 1) * LB])

    def go_on(kind, u, s):
        if s == far:
            (arrive_g if kind == "g" else arrive_d)(u)
        else:
            (relay_g if kind == "g" else relay_d)(u, s)

    def turn_round(place, first, end):
        for s in range(far, -1, -1):
            here = [p for p in PLACES[s] if first <= p < end]
            if not here:
                continue
            u = sum((place > p).astype(jnp.int32) for p in here) + PLACES[s].index(here[0])
            due = functools.reduce(jnp.logical_or, [place == p for p in here])

            @pl.when(due)
            def _(s=s, u=u):
                go_on("g", u, s)
                go_on("d", u, s)

    def elementwise(gu, dh, slot):
        g, u = gu[:, :FC], gu[:, FC:]
        sig = sigmoid(g)
        silu = g * sig
        hds[slot][...] = (silu * u).astype(BF16)
        dgus[slot][:, :FC] = (dh * u * (sig + silu * (1 - sig))).astype(BF16)
        dgus[slot][:, FC:] = (dh * silu).astype(BF16)

    def keep_from(first):
        return (lambda old: old) if first is None else (lambda old: jnp.where(first, jnp.zeros_like(old), old))

    def back_g(u, t, slot, first=None):
        k, keep = lax.rem(u, UNITS_HELD), keep_from(first)
        pg[k] = keep(pg[k]) + dot(at[t], dgus[slot][...])

    def back_d(u, t, slot, first=None):
        k, keep = lax.rem(u, UNITS_HELD), keep_from(first)
        hd = dot(dyt[t], hds[slot][...])
        for s in range(2):
            pd[k, s] = keep(pd[k, s]) + hd[:, s * LB:(s + 1) * LB]

    def to_states(u, t, slot):
        old = jnp.where(u == 0, jnp.zeros(da.shape[1:], F32), da[t])
        da[t] = old + dot(dgus[slot][...], wgut[lax.rem(u, 2)])

    def turn(layer, j, t):
        p = lax.rem(j, 2)
        if layer:
            for i, f in enumerate((fg, fu)):
                s = lax.rem(t, 2)
                wgut[p, pl.ds(pl.multiple_of(i * FC + s * LB, LB), LB), :] = f[layer, :, at_block(block(j) + s * nc)].T
        s = lax.rem(t, 2)
        wdt[p, :, at_block(s)] = fd[layer, at_block(block(j) + s * nc), :].T

    def clear():
        for h, g in zip(hds, dgus):
            h[...] = jnp.zeros_like(h)
            g[...] = jnp.zeros_like(g)

    per_chunk = nt // 2
    steps = nc * per_chunk
    pl.semaphore_wait(free_sem, 2)
    moments_left(0, 1)

    for t in range(2):
        turn(1, 0, t)
    clear()

    def front2(j, t, slot):
        cols = [at_block(block(j) + s * nc) for s in range(2)]
        gu = dot(a[t], jnp.concatenate([f[1, :, c] for f in (fg, fu) for c in cols], 1))
        elementwise(gu, dot(dy[t], wdt[lax.rem(j, 2)]).astype(BF16).astype(F32), slot)

    @pl.loop(0, nc * per_chunk)
    def _(i):
        j, t = i // per_chunk, 2 * lax.rem(i, per_chunk)
        k = jnp.maximum(2 * i - 1, 0)
        @pl.when(i == 2)
        def _():
            for copy in [c for k in range(1, nc) for c in gu_out(nt - 1, 1, k)]:
                copy.wait()

        jk, tk, jn = k // nt, lax.rem(k, nt), jnp.minimum(j + 1, nc - 1)
        back_g(jk, tk, 1)
        to_states(jk, tk, 1)
        back_d(jk, tk, 1)
        front2(j, t, 0)
        to_states(j, t, 0)
        turn(1, jn, t + 1)
        back_d(j, t, 0, t == 0)
        front2(j, t + 1, 1)
        turn(1, jn, t)
        back_g(j, t, 0, t == 0)
        turn_round(i, 0, steps)
        @pl.when((lax.rem(i, per_chunk) == per_chunk - 1) & (i < STAGED * per_chunk))
        def _():
            for chunk, whose in ((1, ((1, 1),)), (2, ((0, 2),)), (3, ((1, 2),)), (STAGED, ((0, 0), (1, 0)))):
                @pl.when(i == chunk * per_chunk - 1)
                def _(whose=whose):
                    for j, s in whose:
                        moments_left(j, s)

        for kind, which in (("m", moments_on), ("s", sums_on)):
            due = [what for what in EARLY_PLACES if what[0] == kind]

            @pl.when(functools.reduce(jnp.logical_or, [i == what[3] for what in due]))
            def _(which=which, due=due):
                for _, j, s, place in due:
                    @pl.when(i == place)
                    def _(j=j, s=s):
                        forward_on(which, j, s)

    to_states(nc - 1, nt - 1, 1)
    back_d(nc - 1, nt - 1, 1)
    back_g(nc - 1, nt - 1, 1)

    def a1t_in(t):
        return pltpu.make_async_copy(a1t_h.at[t], at.at[t], sem_dy.at[t])

    def gu_in(i):
        return pltpu.make_async_copy(gu_h.at[i // nt, lax.rem(i, nt)], da.at[lax.rem(i, nt)], sem_gi.at[lax.rem(i, nt)])

    for t in range(nt):
        a1t_in(t).start()

    @pl.loop(0, nt)
    def _(t):
        wide = h1[t].astype(F32)
        r = rms(wide)
        da_t = da[t].astype(BF16).astype(F32)
        dn = da_t * r - wide * (r * r * r * jnp.mean(da_t * wide, -1, keepdims=True))
        dh1 = (dy[t].astype(F32) + dn).astype(BF16)
        dy[t] = dh1
        dyt[t] = dh1.T
        gu_in(t).start()
        a1t_in(t).wait()

        @pl.when(lax.rem(t, 2) == 1)
        def _():
            turn_round(steps + t // 2, steps, steps + far)

    for t in range(2):
        turn(0, 0, t)
    clear()

    def front1(j, t, slot):
        elementwise(da[t], dot(dy[t], wdt[lax.rem(j, 2)]).astype(BF16).astype(F32), slot)

    @pl.loop(0, nc * per_chunk)
    def _(i):
        j, t = i // per_chunk, 2 * lax.rem(i, per_chunk)
        k = jnp.maximum(2 * i - 1, 0)
        for s in range(2):
            gu_in(2 * i + s).wait()
        jk, tk, jn = nc + k // nt, lax.rem(k, nt), jnp.minimum(j + 1, nc - 1)
        turn(0, jn, t + 1)
        back_d(jk, tk, 1)
        turn(0, jn, t)
        back_g(jk, tk, 1)
        front1(j, t, 0)
        back_d(nc + j, t, 0, t == 0)
        front1(j, t + 1, 1)
        back_g(nc + j, t, 0, t == 0)

        @pl.when(j + 1 < nc)
        def _():
            for s in range(2):
                gu_in(2 * i + s + nt).start()

        turn_round(steps + far + i, steps + far, 2 * steps + far)

    back_d(2 * nc - 1, nt - 1, 1)
    back_g(2 * nc - 1, nt - 1, 1)

    pieces = [(i, layer) for layer in (1, 0) for i in range(3)]
    d = h1.shape[2]
    deep = n // 2 * rows

    def moment_copies(k):
        i, layer = pieces[k]
        made = []
        for c, h in enumerate(((mg_h, mu_h, md_h)[i], (vg_h, vu_h, vd_h)[i])):
            if i == 2:
                made.append(pltpu.make_async_copy(h.at[layer], da.at[k, pl.ds(c * deep, deep), :], mv_sem.at[k, c]))
            else:
                for b in range(far):
                    made.append(pltpu.make_async_copy(
                        h.at[layer, :, pl.ds(b * d, d)], da.at[k, pl.ds(c * deep + b * rows, rows), :], mv_sem.at[k, c * far + b]))
        return made

    for k in range(len(pieces)):
        for copy in moment_copies(k):
            copy.start()

    for kind, u, s in LAST:
        go_on(kind, jnp.int32(u), s)

    def early_loads(k):
        made = []
        for j in range(EARLY):
            made.append(pltpu.make_async_copy(mv_h.at[j, around[k]], pd.at[k - 1, j], late_sem.at[k - 1, j, 0]))
            made.append(pltpu.make_async_copy(gs_h.at[j, around[k]], rg.at[j, (k - 1) // far, (k - 1) % far], late_sem.at[k - 1, j, 1]))
        return made

    tots[pl.ds(me, 1)] = ss[...][None]
    totals = [
        pltpu.make_async_remote_copy(ss, tots.at[me], ts_sem.at[k], tr_sem.at[n - k], device_id={"dp": around[k]}, device_id_type=MESH)
        for k in range(1, n)
    ]
    for copy in totals:
        copy.start()
    for j in range(EARLY):
        for way in range(2):
            moments_in(j, far - 1, way).wait_recv()
            moments_on(j, far - 1, way).wait_send()
            sums_in(j, far - 1, way).wait_recv()
            for s in range(far):
                sums_on(j, s, way).wait_send()
    for k in range(1, n):
        for copy in early_loads(k):
            copy.start()
    for way in range(2):
        for s in range(far):
            for u in (units - 2, units - 1):
                g_copy(u, s, way, s > 0).wait_send()
            e = around[far - s] if way == 0 else around[n - far + s]
            d_copy(lax.rem(e, far), way, s > 0).wait_send()
    for k in range(len(pieces)):
        for copy in moment_copies(k):
            copy.wait()
    for k in range(1, n):
        pltpu.make_async_remote_copy(ss, tots.at[around[k]], ts_sem.at[k], tr_sem.at[k], device_id={"dp": around[k]}, device_id_type=MESH).wait_recv()
    factor = jnp.minimum(1.0, 0.5 * lax.rsqrt(jnp.sum(tots[...], keepdims=True).reshape(1, 1) / count + 1e-30))

    def rows_of(i, origin, part=None):
        tall = full[i].shape[1] // n
        start = origin * tall
        if part is not None:
            tall //= 2
            start += part * tall
        return pl.ds(pl.multiple_of(start, tall), tall)

    early = sorted(static_block(j) + s * nc for j in range(EARLY) for s in range(2))
    between = [(p + 1, q) for p, q in zip([-1] + early, early + [2 * nc]) if q > p + 1]
    parcels = [(k, i, layer, cols) for k, (i, layer) in enumerate(pieces)
               for cols in ([pl.ds(p * LB, (q - p) * LB) for p, q in between] if layer == 1 and i < 2 else [slice(None)])]

    def pass_on(c, s, way, coming=False):
        _, i, layer, cols = parcels[c]
        back_by = s + coming
        origin = around[(n - back_by) % n] if way == 0 else around[back_by]
        here = full[i].at[layer, rows_of(i, origin, way if s == far - 1 else None), cols]
        return pltpu.make_async_remote_copy(
            here, here, ag_send.at[way, s, c], ag_recv.at[way, s, c], device_id={"dp": towards[way]}, device_id_type=MESH)

    for k, (i, layer) in enumerate(pieces):
        def adamw(here, where_g, where_w):
            m_at, v_at = here, pl.ds(here.start + deep, here.size)
            g = own_g[i][(layer, *where_g)].astype(F32) * factor
            m = 0.9 * da[k, m_at, :] + 0.1 * g
            v = 0.95 * da[k, v_at, :] + 0.05 * g * g
            w = full[i][(layer, *where_w)].astype(F32)
            step = m * lax.rsqrt(v + 1e-8) + 0.1 * w
            da[k, m_at, :] = m
            da[k, v_at, :] = v
            full[i][(layer, *where_w)] = (w - 0.02 * step).astype(BF16)

        for b in range(far):
            here = pl.ds(b * rows, rows)
            if i == 2:
                adamw(here, (here, slice(None)), (pl.ds(pl.multiple_of(me * deep + b * rows, rows), rows), slice(None)))
            else:
                cols = pl.ds(b * d, d)
                adamw(here, (slice(None), cols), (pl.ds(pl.multiple_of(me * rows, rows), rows), cols))
        for c, parcel in enumerate(parcels):
            if parcel[0] == k:
                for way in range(2):
                    pass_on(c, 0, way).start()

    for k in range(1, n):
        for copy in early_loads(k):
            copy.wait()

    @pl.loop(1, n)
    def _(k):
        origin = lax.rem(me + k, n)
        mine = pl.ds(pl.multiple_of(origin * rows, rows), rows)
        for j in range(EARLY):
            for i, f in enumerate((fg, fu)):
                for b in range(2):
                    cols = at_block(static_block(j) + b * nc)
                    g = rg[j, (k - 1) // far, lax.rem(k - 1, far), i, :, b * LB:(b + 1) * LB].astype(F32) * factor
                    m = 0.9 * pd[k - 1, j, (4 * i + b) * rows:(4 * i + b + 1) * rows, :] + 0.1 * g
                    v = 0.95 * pd[k - 1, j, (4 * i + 2 + b) * rows:(4 * i + 3 + b) * rows, :] + 0.05 * g * g
                    w = f[1, mine, cols].astype(F32)
                    f[1, mine, cols] = (w - 0.02 * (m * lax.rsqrt(v + 1e-8) + 0.1 * w)).astype(BF16)

    for s in range(far):
        for c in range(len(parcels)):
            for way in range(2):
                pass_on(c, s, way, True).wait_recv()
                if s + 1 < far:
                    pass_on(c, s + 1, way).start()
    for copy in totals:
        copy.wait_send()
    for s in range(far):
        for c in range(len(parcels)):
            for way in range(2):
                pass_on(c, s, way).wait_send()


def flush_kernel(n, fg, fu, fd, wide, *refs):
    outs, sem = refs[:9], refs[9]
    layers, d = fg.shape[0], fg.shape[1]
    rows, far = d // n, n // 2
    deep = far * rows
    copies = []
    for k, (i, layer) in enumerate((i, layer) for layer in (1, 0) for i in range(3)):
        for c in range(2):
            out = outs[3 + 3 * c + i]
            if i == 2:
                copies.append((wide.at[k, pl.ds(c * deep, deep), :], out.at[layer]))
            else:
                copies += [(wide.at[k, pl.ds(c * deep + b * rows, rows), :], out.at[layer, :, pl.ds(b * d, d)]) for b in range(far)]
    copies += [(f.at[layer], out.at[layer]) for layer in range(layers) for f, out in zip((fg, fu, fd), outs)]
    copies = [pltpu.make_async_copy(*pair, sem.at[i]) for i, pair in enumerate(copies)]
    for copy in copies:
        copy.start()
    for copy in copies:
        copy.wait()


def train_step(x, dy, w, m, v, n):
    wg, wu, wd = w
    tokens, d = x.shape[1:]
    layers, _, f = wg.shape
    nt, nc = tokens // TT, f // FC
    far, rows = n // 2, d // n
    pieces = 3 * layers
    parcels = pieces + 2 * 2 * EARLY
    hbm = pl.BlockSpec(memory_space=pl.ANY)
    vmem = pl.BlockSpec(memory_space=pltpu.VMEM)
    shape = jax.ShapeDtypeStruct
    kept = [pltpu.VMEM(one.shape, BF16) for one in w] + [pltpu.VMEM((nt, TT, d), F32)]
    v_, dma = pltpu.VMEM, pltpu.SemaphoreType.DMA
    scratch = [
        v_((2, 2 * FC, d), BF16), v_((2, d, FC), BF16),
        v_((nt, TT, d), BF16), v_((nt, d, TT), BF16), v_((nt, TT, d), BF16), v_((nt, TT, d), BF16), v_((nt, d, TT), BF16),
        v_((2 * nc, TT, LB), BF16), v_((TT, FC), BF16), v_((TT, FC), BF16), v_((TT, 2 * FC), BF16), v_((TT, 2 * FC), BF16),
        v_((UNITS_HELD, d, 2 * FC), F32), v_((UNITS_HELD, 2, d, LB), F32),
        v_((2, RECEIVED, far, 2, rows, FC), BF16), v_((2, 2, far, 2, rows, FC), BF16), v_((EARLY, 2, rows, FC), BF16),
        v_((layers, rows, f), BF16), v_((layers, rows, f), BF16), v_((layers, f // n, d), BF16), v_((8, LB), F32), v_((n, 8, LB), F32),
        dma((layers, 3)), dma((nt,)), dma((nt,)), dma((2,)), dma((2 * nc + 6,)), dma((nt,)),
        dma((2, RECEIVED, far)), dma((2, far)), dma((2, 2, far)), dma((2, far)), dma((n,)), dma((n,)),
        dma((pieces, n)), dma((2, far, parcels)), dma((2, far, parcels)),
        pltpu.SemaphoreType.REGULAR, dma((EARLY, 8)), dma((2, far, EARLY)), dma((2, far, EARLY)), dma((2, far, EARLY)), dma((2, far, EARLY)),
        dma((n - 1, EARLY, 2)),
    ]
    kept_bytes = 2 * sum(one.size for one in w) + 4 * tokens * d
    *new, wide, _, _, _, _ = pl.pallas_call(
        functools.partial(step_kernel, nt, nc, n, sum(one.size for one in w)),
        name="train_step",
        out_shape=kept + [shape((nc, nt, TT, 2 * FC), F32), shape((nt, d, TT), BF16),
                          shape((EARLY, n, d, LB), F32), shape((EARLY, n, 2, rows, FC), BF16)],
        in_specs=[hbm] * 11,
        out_specs=[vmem] * 4 + [hbm] * 4,
        scratch_shapes=scratch,
        compiler_params=pltpu.CompilerParams(vmem_limit_bytes=VMEM_BYTES - kept_bytes, collective_id=0, has_side_effects=True),
    )(x, dy, *w, *m, *v)
    copies = layers * (2 * (2 * far + 1) + 3)
    keep = lambda one: pltpu.with_memory_space_constraint(one, pltpu.VMEM)
    return tuple(pl.pallas_call(
        functools.partial(flush_kernel, n),
        name="flush",
        out_shape=[shape(one.shape, one.dtype) for group in (w, m, v) for one in group],
        in_specs=[vmem] * 4,
        out_specs=[hbm] * 9,
        scratch_shapes=[dma((copies,))],
        compiler_params=pltpu.CompilerParams(vmem_limit_bytes=1 << 20),
    )(*(keep(one) for one in (*new, wide))))


def solution(mesh):
    n = mesh.shape["dp"]

    def step(x, dy, *arrays):
        return train_step(x, dy, *(arrays[i:i + 3] for i in (0, 3, 6)), n)

    seq, rows = P(("rep", "dp"), None, None), P(None, "dp", None)
    return jax.shard_map(
        step,
        mesh=mesh,
        in_specs=(seq, seq) + (P(),) * 3 + (rows,) * 6,
        out_specs=(P("rep"),) * 3 + (P("rep", "dp"),) * 6,
        check_vma=False,
    )
```

```python
import functools

import jax
import jax.numpy as jnp
from jax import lax
from jax.experimental import pallas as pl
from jax.experimental.pallas import tpu as pltpu
from jax.sharding import PartitionSpec as P

F32, BF16 = jnp.float32, jnp.bfloat16
MESH = pl.DeviceIdType.MESH
TT = 512
LB = 128
EARLY = 2
STAGED = 4
FC = 2 * LB
RECEIVED = 6
UNITS_HELD = 7
VMEM_BYTES = 67_043_328
PLACES = tuple(tuple(int(p) for p in line.split(",")) for line in (
    "4,8,13,16,20,24,29,32,40,44,48,52,56,60,64",
    "6,11,15,22,23,27,36,41,46,47,53,57,61,66",
    "9,14,18,26,29,30,42,45,50,55,59,62,65",
    "12,17,21,31,33,37,49,51,55,61,63",
    "15,20,25,42,45,46,55,57,62",
))
LAST = tuple((what[0], *(int(p) for p in what[1:].split("."))) for line in (
    "g15.0,g11.3,d14.1,g9.4,d15.0,d9.4,g10.4,g12.3,d11.3,d12.3",
    "d10.4,g14.1,g15.1,d13.2,d15.1,d11.4,g13.2,g11.4,d14.2,g14.2",
    "g12.4,g15.2,d13.3,d12.4,d15.2,d14.3,g13.3,g14.3,g15.3,d15.3",
    "g13.4,d13.4,d14.4,g14.4,g15.4,d15.4",
) for what in line.split(","))
EARLY_PLACES = tuple((what[0], *(int(p) for p in what[1:].split("."))) for line in (
    "m1.2.1,m0.3.4,m1.3.7,s0.0.15,s0.1.19,s1.0.20,s1.1.23,s0.2.24",
    "s1.2.27,s0.3.29,s1.3.31",
) for what in line.split(","))


def dot(a, b):
    return jnp.dot(a, b, preferred_element_type=F32)


def rms(wide):
    return lax.rsqrt(jnp.mean(wide * wide, -1, keepdims=True) + 1e-6)


def sigmoid(g):
    return 0.5 * jnp.tanh(0.5 * g) + 0.5


def step_kernel(nt, nc, n, count, x_h, dy_h, wg_h, wu_h, wd_h, mg_h, mu_h, md_h, vg_h, vu_h, vd_h,
                fg, fu, fd, wide_ref, gu_h, a1t_h, mv_h, gs_h,
                wgut, wdt, a, at, h1, dy, dyt, hid, hd0, hd1, dgu0, dgu1,
                pg, pd, rg, sg, gs, og, ou, od, ss, tots,
                sem_w, sem_x, sem_dy, sem_at, sem_gu, sem_gi, rg_sem, rd_sem, sg_sem, sd_sem, ts_sem, tr_sem, mv_sem, ag_send, ag_recv,
                free_sem, early_sem, ms_sem, mr_sem, gs_sem, gr_sem, late_sem):
    half, far = nc // 2, n // 2
    units = 2 * nc
    rows = pg.shape[1] // n
    hds, dgus = (hd0, hd1), (dgu0, dgu1)
    full, own_g = (fg, fu, fd), (og, ou, od)
    da = wide_ref
    me = lax.axis_index("dp")
    around = [lax.rem(me + k, n) for k in range(n)]
    towards = (around[1], around[n - 1])

    barrier = pltpu.get_barrier_semaphore()
    for k in range(1, n):
        pl.semaphore_signal(barrier, inc=1, device_id={"dp": around[k]}, device_id_type=MESH)

    def block(j):
        return 2 * lax.rem(j, half) + j // half

    def at_block(b):
        return pl.ds(b * LB if isinstance(b, int) else pl.multiple_of(b * LB, LB), LB)

    def x_copy(t):
        return pltpu.make_async_copy(x_h.at[0, pl.ds(t * TT, TT), :], a.at[t], sem_x.at[t])

    def dy_copy(t):
        return pltpu.make_async_copy(dy_h.at[0, pl.ds(t * TT, TT), :], dy.at[t], sem_dy.at[t])

    def w_copies(layer):
        return [pltpu.make_async_copy(h.at[layer], v.at[layer], sem_w.at[layer, i]) for i, (h, v) in enumerate(zip((wg_h, wu_h, wd_h), full))]

    x_copy(0).start()
    for copy in w_copies(0):
        copy.start()
    ss[...] = jnp.zeros_like(ss)

    def staged(odd, j):
        if not odd:
            return [(da.at[j], 0, 2 * FC)]
        if j < UNITS_HELD:
            return [(pg.at[j], 0, 2 * FC)]
        return [(pd.at[UNITS_HELD - 2 + i // 2, i % 2], i * LB, LB) for i in range(2 * FC // LB)]

    def gu_out(t, odd, j):
        return [pltpu.make_async_copy(ref, gu_h.at[j, t, :, pl.ds(at_, width)], sem_gu.at[odd * (nc + 3) + j + i])
                for i, (ref, at_, width) in enumerate(staged(odd, j))]

    def gu_out_all(t, odd):
        return [copy for j in range(nc) for copy in gu_out(t, odd, j)]

    def a1t_out(t):
        p = lax.rem(t, 2)
        return pltpu.make_async_copy(wgut.at[p], a1t_h.at[t], sem_at.at[p])

    def origin_of(s, way):
        return around[(n - s) % n] if way == 0 else around[s]

    def half_of(ref, s, way):
        size = ref.shape[0] // 2
        return ref.at[pl.ds(way * size, size)] if s == far - 1 else ref

    def kept_moments(j, s, way):
        return pd.at[2 * s + j, way] if s < 2 else mv_h.at[j, origin_of(s + 1, way)]

    def moments_on(j, s, way):
        here = kept_moments(j, s - 1, way) if s else pd.at[STAGED, j]
        there = pd.at[2 * s + j, way] if s < 2 else mv_h.at[j, origin_of(s, way)]
        return pltpu.make_async_remote_copy(
            half_of(here, s, way), half_of(there, s, way), ms_sem.at[way, s, j], mr_sem.at[way, s, j],
            device_id={"dp": towards[way]}, device_id_type=MESH)

    def moments_in(j, s, way):
        here = half_of(kept_moments(j, s, way), s, way)
        return pltpu.make_async_remote_copy(
            here, here, ms_sem.at[way, s, j], mr_sem.at[way, s, j], device_id={"dp": towards[way]}, device_id_type=MESH)

    def moments_out(j, s, way):
        return pltpu.make_async_copy(kept_moments(j, s, way), mv_h.at[j, origin_of(s + 1, way)], early_sem.at[j, 2 * s + way])

    def moments_left(j, s):
        for way in range(2):
            moments_on(j, s, way).wait_send()
            if s:
                moments_out(j, s - 1, way).wait()

    def sums_on(j, s, way, coming=False):
        back_by = s + coming
        there = gs_h.at[j, origin_of(back_by, way)]
        here = there if back_by else gs.at[j]
        return pltpu.make_async_remote_copy(
            half_of(here, s, way), half_of(there, s, way), gs_sem.at[way, s, j], gr_sem.at[way, s, j],
            device_id={"dp": towards[way]}, device_id_type=MESH)

    def sums_in(j, s, way):
        return sums_on(j, s, way, True)

    def forward_on(which, j, s):
        for way in range(2):
            moments = which is moments_on
            if s > 0:
                (moments_in if moments else sums_in)(j, s - 1, way).wait_recv()
            which(j, s, way).start()
            if moments and 0 < s < 3:
                moments_out(j, s - 1, way).start()

    def early_moments():
        copies = []
        for j in range(EARLY):
            for i, pair in enumerate(((mg_h, vg_h), (mu_h, vu_h))):
                for c, h in enumerate(pair):
                    for b in range(2):
                        part = 4 * i + 2 * c + b
                        copies.append(pltpu.make_async_copy(
                            h.at[1, :, at_block(static_block(j) + b * nc)], pd.at[STAGED, j, pl.ds(part * rows, rows), :], early_sem.at[j, part]))
        return copies

    def static_block(j):
        return 2 * (j % half) + j // half

    def down():
        w = jnp.concatenate([fd[0, at_block(static_block(j) + s * nc), :] for j in range(nc) for s in range(2)], 0)
        return dot(jnp.concatenate([hid[b] for b in range(2 * nc)], 1), w)

    def gate_up(odd, j):
        cols = [at_block(static_block(j) + s * nc) for s in range(2)]
        gu = dot(dgu0[...], jnp.concatenate([f[0, :, c] for f in (fg, fu) for c in cols], 1))
        for ref, at_, width in staged(odd, j):
            ref[...] = gu[:, at_:at_ + width]
        g, u = gu[:, :FC], gu[:, FC:]
        h = (g * sigmoid(g) * u).astype(BF16)
        for s in range(2):
            hid[2 * j + s] = h[:, s * LB:(s + 1) * LB]

    def finish(t, y):
        h = (a[t].astype(F32) + y.astype(BF16).astype(F32)).astype(BF16)
        h1[t] = h
        wide = h.astype(F32)
        a2 = (wide * rms(wide)).astype(BF16)
        a[t] = a2
        at[t] = a2.T
        dyt[t] = dy[t].T

    def forward(t, odd, follows):
        x_copy(t).wait()
        if follows:
            dy_copy(t - 1).wait()

        @pl.when(t >= 2)
        def _():
            a1t_out(t - 2).wait()
            for copy in gu_out_all(t - 2, odd):
                copy.wait()

        if follows:
            y = down()
        wide = a[t].astype(F32)
        a1 = (wide * rms(wide)).astype(BF16)
        dgu0[...] = a1
        wgut[lax.rem(t, 2)] = a1.T
        for j in range(nc):
            gate_up(odd, j)
            if j == half and follows:
                finish(t - 1, y)
        for copy in gu_out_all(t, odd):
            copy.start()
        a1t_out(t).start()

    for copy in w_copies(0):
        copy.wait()
    dy_copy(0).start()
    for t in range(1, nt):
        x_copy(t).start()
        dy_copy(t).start()
    for copy in early_moments():
        copy.start()
    for copy in w_copies(1):
        copy.start()
    forward(0, 0, False)
    for copy in early_moments():
        copy.wait()
    pl.semaphore_wait(barrier, n - 1)
    for j in range(EARLY):
        forward_on(moments_on, j, 0)

    @pl.loop(0, nt // 2 - 1)
    def _(i):
        forward(2 * i + 1, 1, True)

        @pl.when(i == 2)
        def _():
            forward_on(moments_on, 1, 1)

        forward(2 * i + 2, 0, True)

        @pl.when(i == 1)
        def _():
            forward_on(moments_on, 0, 1)

    forward(nt - 1, 1, True)
    forward_on(moments_on, 0, 2)
    dy_copy(nt - 1).wait()
    finish(nt - 1, down())
    for copy in gu_out_all(nt - 2, 0):
        copy.wait()
    for t in (nt - 2, nt - 1):
        a1t_out(t).wait()
    for copy in gu_out(nt - 1, 1, 0):
        copy.wait()
    for copy in w_copies(1):
        copy.wait()

    for other in towards:
        pl.semaphore_signal(free_sem, inc=1, device_id={"dp": other}, device_id_type=MESH)

    def g_copy(u, s, way, both):
        part = (lambda ref: ref) if both else (lambda ref: ref.at[way])
        old, new = lax.rem(u, 2), lax.rem(u, RECEIVED)
        return pltpu.make_async_remote_copy(
            part(sg.at[way, old, s]), part(rg.at[way, new, s]), sg_sem.at[way, old, s], rg_sem.at[way, new, s],
            device_id={"dp": towards[way]}, device_id_type=MESH)

    tall = pd.shape[2] // 2

    def d_at(way, k, sent):
        return hid.at[(2 * sent + way) * far + k]

    def d_copy(j, way, both):
        k = lax.rem(j, far)
        part = (lambda ref: ref) if both else (lambda ref: ref.at[pl.ds(way * tall, tall), :])
        return pltpu.make_async_remote_copy(
            part(d_at(way, k, 1)), part(d_at(way, k, 0)), sd_sem.at[way, k], rd_sem.at[way, k],
            device_id={"dp": towards[way]}, device_id_type=MESH)

    def relay_g(u, s):
        slot, old, new = lax.rem(u, UNITS_HELD), lax.rem(u, 2), lax.rem(u, RECEIVED)
        for way in range(2):
            e = around[far - s] if way == 0 else around[n - far + s]

            @pl.when(u > 1)
            def _():
                g_copy(u - 2, s, way, s > 0).wait_send()

            if s > 0:
                g_copy(u, s - 1, way, s > 1).wait_recv()
            for h in range(2):
                if s == 0 and h != way:
                    continue
                own = pg[slot, pl.ds(pl.multiple_of(e * rows, rows), rows), h * FC:(h + 1) * FC]
                if s > 1 or (s == 1 and h == way):
                    own += rg[way, new, s - 1, h].astype(F32)
                sg[way, old, s, h] = own.astype(BF16)
            g_copy(u, s, way, s > 0).start()

    def relay_d(u, s):
        j, slot = lax.rem(u, nc), lax.rem(u, UNITS_HELD)
        k = lax.rem(j, far)
        for way in range(2):
            e = around[far - s] if way == 0 else around[n - far + s]

            @pl.when(lax.rem(e, far) == k)
            def _():
                @pl.when(u >= far)
                def _():
                    d_copy(j, way, s > 0).wait_send()

                if s > 0:
                    d_copy(j, way, s > 1).wait_recv()
                for h in range(2):
                    if s == 0 and h != way:
                        continue
                    part = pl.ds(h * tall, tall)
                    own = pd[slot, e // far, part, :]
                    if s > 1 or (s == 1 and h == way):
                        own += d_at(way, k, 0)[part, :].astype(F32)
                    d_at(way, k, 1)[part, :] = own.astype(BF16)
                d_copy(j, way, s > 0).start()

    def square(g):
        wide = g.astype(F32)
        ss[...] += jnp.sum((wide * wide).reshape(-1, *ss.shape), 0)

    def arrive_g(u):
        j, slot, new, layer = lax.rem(u, nc), lax.rem(u, UNITS_HELD), lax.rem(u, RECEIVED), 1 - u // nc
        for way in range(2):
            g_copy(u, far - 1, way, True).wait_recv()
        for h, out in enumerate((og, ou)):
            own = pg[slot, pl.ds(pl.multiple_of(me * rows, rows), rows), h * FC:(h + 1) * FC]
            own = (own + rg[0, new, far - 1, h].astype(F32) + rg[1, new, far - 1, h].astype(F32)).astype(BF16)
            for s in range(2):
                piece = own[:, s * LB:(s + 1) * LB]
                out[layer, :, at_block(block(j) + s * nc)] = piece
                square(piece)

            @pl.when(u < EARLY)
            def _(own=own, h=h):
                gs[jnp.minimum(u, EARLY - 1), h] = own

    def arrive_d(u):
        j, slot, layer = lax.rem(u, nc), lax.rem(u, UNITS_HELD), 1 - u // nc
        k = lax.rem(j, far)

        @pl.when(lax.rem(me, far) == k)
        def _():
            for way in range(2):
                d_copy(j, way, True).wait_recv()
            for h in range(2):
                part = pl.ds(h * tall, tall)
                own = pd[slot, me // far, part, :]
                own = own + d_at(0, k, 0)[part, :].astype(F32) + d_at(1, k, 0)[part, :].astype(F32)
                own = own.T.astype(BF16)
                od[layer, at_block(j // half), h * tall:(h + 1) * tall] = own
                for s in range(tall // LB):
                    square(own[:, s * LB:(s + 1) * LB])

    def go_on(kind, u, s):
        if s == far:
            (arrive_g if kind == "g" else arrive_d)(u)
        else:
            (relay_g if kind == "g" else relay_d)(u, s)

    def turn_round(place, first, end):
        for s in range(far, -1, -1):
            here = [p for p in PLACES[s] if first <= p < end]
            if not here:
                continue
            u = sum((place > p).astype(jnp.int32) for p in here) + PLACES[s].index(here[0])
            due = functools.reduce(jnp.logical_or, [place == p for p in here])

            @pl.when(due)
            def _(s=s, u=u):
                go_on("g", u, s)
                go_on("d", u, s)

    def elementwise(gu, dh, slot):
        g, u = gu[:, :FC], gu[:, FC:]
        sig = sigmoid(g)
        silu = g * sig
        hds[slot][...] = (silu * u).astype(BF16)
        dgus[slot][:, :FC] = (dh * u * (sig + silu * (1 - sig))).astype(BF16)
        dgus[slot][:, FC:] = (dh * silu).astype(BF16)

    def keep_from(first):
        return (lambda old: old) if first is None else (lambda old: jnp.where(first, jnp.zeros_like(old), old))

    def back_g(u, t, slot, first=None):
        k, keep = lax.rem(u, UNITS_HELD), keep_from(first)
        pg[k] = keep(pg[k]) + dot(at[t], dgus[slot][...])

    def back_d(u, t, slot, first=None):
        k, keep = lax.rem(u, UNITS_HELD), keep_from(first)
        hd = dot(dyt[t], hds[slot][...])
        for s in range(2):
            pd[k, s] = keep(pd[k, s]) + hd[:, s * LB:(s + 1) * LB]

    def to_states(u, t, slot):
        old = jnp.where(u == 0, jnp.zeros(da.shape[1:], F32), da[t])
        da[t] = old + dot(dgus[slot][...], wgut[lax.rem(u, 2)])

    def turn(layer, j, t):
        p = lax.rem(j, 2)
        if layer:
            for i, f in enumerate((fg, fu)):
                s = lax.rem(t, 2)
                wgut[p, pl.ds(pl.multiple_of(i * FC + s * LB, LB), LB), :] = f[layer, :, at_block(block(j) + s * nc)].T
        s = lax.rem(t, 2)
        wdt[p, :, at_block(s)] = fd[layer, at_block(block(j) + s * nc), :].T

    def clear():
        for h, g in zip(hds, dgus):
            h[...] = jnp.zeros_like(h)
            g[...] = jnp.zeros_like(g)

    per_chunk = nt // 2
    steps = nc * per_chunk
    pl.semaphore_wait(free_sem, 2)
    moments_left(0, 1)

    for t in range(2):
        turn(1, 0, t)
    clear()

    def front2(j, t, slot):
        cols = [at_block(block(j) + s * nc) for s in range(2)]
        gu = dot(a[t], jnp.concatenate([f[1, :, c] for f in (fg, fu) for c in cols], 1))
        elementwise(gu, dot(dy[t], wdt[lax.rem(j, 2)]).astype(BF16).astype(F32), slot)

    @pl.loop(0, nc * per_chunk)
    def _(i):
        j, t = i // per_chunk, 2 * lax.rem(i, per_chunk)
        k = jnp.maximum(2 * i - 1, 0)
        @pl.when(i == 2)
        def _():
            for copy in [c for k in range(1, nc) for c in gu_out(nt - 1, 1, k)]:
                copy.wait()

        jk, tk, jn = k // nt, lax.rem(k, nt), jnp.minimum(j + 1, nc - 1)
        back_g(jk, tk, 1)
        to_states(jk, tk, 1)
        back_d(jk, tk, 1)
        front2(j, t, 0)
        to_states(j, t, 0)
        turn(1, jn, t + 1)
        back_d(j, t, 0, t == 0)
        front2(j, t + 1, 1)
        turn(1, jn, t)
        back_g(j, t, 0, t == 0)
        turn_round(i, 0, steps)
        @pl.when((lax.rem(i, per_chunk) == per_chunk - 1) & (i < STAGED * per_chunk))
        def _():
            for chunk, whose in ((1, ((1, 1),)), (2, ((0, 2),)), (3, ((1, 2),)), (STAGED, ((0, 0), (1, 0)))):
                @pl.when(i == chunk * per_chunk - 1)
                def _(whose=whose):
                    for j, s in whose:
                        moments_left(j, s)

        for kind, which in (("m", moments_on), ("s", sums_on)):
            due = [what for what in EARLY_PLACES if what[0] == kind]

            @pl.when(functools.reduce(jnp.logical_or, [i == what[3] for what in due]))
            def _(which=which, due=due):
                for _, j, s, place in due:
                    @pl.when(i == place)
                    def _(j=j, s=s):
                        forward_on(which, j, s)

    to_states(nc - 1, nt - 1, 1)
    back_d(nc - 1, nt - 1, 1)
    back_g(nc - 1, nt - 1, 1)

    def a1t_in(t):
        return pltpu.make_async_copy(a1t_h.at[t], at.at[t], sem_dy.at[t])

    def gu_in(i):
        return pltpu.make_async_copy(gu_h.at[i // nt, lax.rem(i, nt)], da.at[lax.rem(i, nt)], sem_gi.at[lax.rem(i, nt)])

    for t in range(nt):
        a1t_in(t).start()

    @pl.loop(0, nt)
    def _(t):
        wide = h1[t].astype(F32)
        r = rms(wide)
        da_t = da[t].astype(BF16).astype(F32)
        dn = da_t * r - wide * (r * r * r * jnp.mean(da_t * wide, -1, keepdims=True))
        dh1 = (dy[t].astype(F32) + dn).astype(BF16)
        dy[t] = dh1
        dyt[t] = dh1.T
        gu_in(t).start()
        a1t_in(t).wait()

        @pl.when(lax.rem(t, 2) == 1)
        def _():
            turn_round(steps + t // 2, steps, steps + far)

    for t in range(2):
        turn(0, 0, t)
    clear()

    def front1(j, t, slot):
        elementwise(da[t], dot(dy[t], wdt[lax.rem(j, 2)]).astype(BF16).astype(F32), slot)

    @pl.loop(0, nc * per_chunk)
    def _(i):
        j, t = i // per_chunk, 2 * lax.rem(i, per_chunk)
        k = jnp.maximum(2 * i - 1, 0)
        for s in range(2):
            gu_in(2 * i + s).wait()
        jk, tk, jn = nc + k // nt, lax.rem(k, nt), jnp.minimum(j + 1, nc - 1)
        turn(0, jn, t + 1)
        back_d(jk, tk, 1)
        turn(0, jn, t)
        back_g(jk, tk, 1)
        front1(j, t, 0)
        back_d(nc + j, t, 0, t == 0)
        front1(j, t + 1, 1)
        back_g(nc + j, t, 0, t == 0)

        @pl.when(j + 1 < nc)
        def _():
            for s in range(2):
                gu_in(2 * i + s + nt).start()

        turn_round(steps + far + i, steps + far, 2 * steps + far)

    back_d(2 * nc - 1, nt - 1, 1)
    back_g(2 * nc - 1, nt - 1, 1)

    pieces = [(i, layer) for layer in (1, 0) for i in range(3)]
    d = h1.shape[2]
    deep = n // 2 * rows

    def moment_copies(k):
        i, layer = pieces[k]
        made = []
        for c, h in enumerate(((mg_h, mu_h, md_h)[i], (vg_h, vu_h, vd_h)[i])):
            if i == 2:
                made.append(pltpu.make_async_copy(h.at[layer], da.at[k, pl.ds(c * deep, deep), :], mv_sem.at[k, c]))
            else:
                for b in range(far):
                    made.append(pltpu.make_async_copy(
                        h.at[layer, :, pl.ds(b * d, d)], da.at[k, pl.ds(c * deep + b * rows, rows), :], mv_sem.at[k, c * far + b]))
        return made

    for k in range(len(pieces)):
        for copy in moment_copies(k):
            copy.start()

    for kind, u, s in LAST:
        go_on(kind, jnp.int32(u), s)

    def early_loads(k):
        made = []
        for j in range(EARLY):
            made.append(pltpu.make_async_copy(mv_h.at[j, around[k]], pd.at[k - 1, j], late_sem.at[k - 1, j, 0]))
            made.append(pltpu.make_async_copy(gs_h.at[j, around[k]], rg.at[j, (k - 1) // far, (k - 1) % far], late_sem.at[k - 1, j, 1]))
        return made

    tots[pl.ds(me, 1)] = ss[...][None]
    totals = [
        pltpu.make_async_remote_copy(ss, tots.at[me], ts_sem.at[k], tr_sem.at[n - k], device_id={"dp": around[k]}, device_id_type=MESH)
        for k in range(1, n)
    ]
    for copy in totals:
        copy.start()
    for j in range(EARLY):
        for way in range(2):
            moments_in(j, far - 1, way).wait_recv()
            moments_on(j, far - 1, way).wait_send()
            sums_in(j, far - 1, way).wait_recv()
            for s in range(far):
                sums_on(j, s, way).wait_send()
    for k in range(1, n):
        for copy in early_loads(k):
            copy.start()
    for way in range(2):
        for s in range(far):
            for u in (units - 2, units - 1):
                g_copy(u, s, way, s > 0).wait_send()
            e = around[far - s] if way == 0 else around[n - far + s]
            d_copy(lax.rem(e, far), way, s > 0).wait_send()
    for k in range(len(pieces)):
        for copy in moment_copies(k):
            copy.wait()
    for k in range(1, n):
        pltpu.make_async_remote_copy(ss, tots.at[around[k]], ts_sem.at[k], tr_sem.at[k], device_id={"dp": around[k]}, device_id_type=MESH).wait_recv()
    factor = jnp.minimum(1.0, 0.5 * lax.rsqrt(jnp.sum(tots[...], keepdims=True).reshape(1, 1) / count + 1e-30))

    def rows_of(i, origin, part=None):
        tall = full[i].shape[1] // n
        start = origin * tall
        if part is not None:
            tall //= 2
            start += part * tall
        return pl.ds(pl.multiple_of(start, tall), tall)

    early = sorted(static_block(j) + s * nc for j in range(EARLY) for s in range(2))
    between = [(p + 1, q) for p, q in zip([-1] + early, early + [2 * nc]) if q > p + 1]
    parcels = [(k, i, layer, cols) for k, (i, layer) in enumerate(pieces)
               for cols in ([pl.ds(p * LB, (q - p) * LB) for p, q in between] if layer == 1 and i < 2 else [slice(None)])]

    def pass_on(c, s, way, coming=False):
        _, i, layer, cols = parcels[c]
        back_by = s + coming
        origin = around[(n - back_by) % n] if way == 0 else around[back_by]
        here = full[i].at[layer, rows_of(i, origin, way if s == far - 1 else None), cols]
        return pltpu.make_async_remote_copy(
            here, here, ag_send.at[way, s, c], ag_recv.at[way, s, c], device_id={"dp": towards[way]}, device_id_type=MESH)

    for k, (i, layer) in enumerate(pieces):
        def adamw(here, where_g, where_w):
            m_at, v_at = here, pl.ds(here.start + deep, here.size)
            g = own_g[i][(layer, *where_g)].astype(F32) * factor
            m = 0.9 * da[k, m_at, :] + 0.1 * g
            v = 0.95 * da[k, v_at, :] + 0.05 * g * g
            w = full[i][(layer, *where_w)].astype(F32)
            step = m * lax.rsqrt(v + 1e-8) + 0.1 * w
            da[k, m_at, :] = m
            da[k, v_at, :] = v
            full[i][(layer, *where_w)] = (w - 0.02 * step).astype(BF16)

        for b in range(far):
            here = pl.ds(b * rows, rows)
            if i == 2:
                adamw(here, (here, slice(None)), (pl.ds(pl.multiple_of(me * deep + b * rows, rows), rows), slice(None)))
            else:
                cols = pl.ds(b * d, d)
                adamw(here, (slice(None), cols), (pl.ds(pl.multiple_of(me * rows, rows), rows), cols))
        for c, parcel in enumerate(parcels):
            if parcel[0] == k:
                for way in range(2):
                    pass_on(c, 0, way).start()

    for k in range(1, n):
        for copy in early_loads(k):
            copy.wait()

    @pl.loop(1, n)
    def _(k):
        origin = lax.rem(me + k, n)
        mine = pl.ds(pl.multiple_of(origin * rows, rows), rows)
        for j in range(EARLY):
            for i, f in enumerate((fg, fu)):
                for b in range(2):
                    cols = at_block(static_block(j) + b * nc)
                    g = rg[j, (k - 1) // far, lax.rem(k - 1, far), i, :, b * LB:(b + 1) * LB].astype(F32) * factor
                    m = 0.9 * pd[k - 1, j, (4 * i + b) * rows:(4 * i + b + 1) * rows, :] + 0.1 * g
                    v = 0.95 * pd[k - 1, j, (4 * i + 2 + b) * rows:(4 * i + 3 + b) * rows, :] + 0.05 * g * g
                    w = f[1, mine, cols].astype(F32)
                    f[1, mine, cols] = (w - 0.02 * (m * lax.rsqrt(v + 1e-8) + 0.1 * w)).astype(BF16)

    for s in range(far):
        for c in range(len(parcels)):
            for way in range(2):
                pass_on(c, s, way, True).wait_recv()
                if s + 1 < far:
                    pass_on(c, s + 1, way).start()
    for copy in totals:
        copy.wait_send()
    for s in range(far):
        for c in range(len(parcels)):
            for way in range(2):
                pass_on(c, s, way).wait_send()


def flush_kernel(n, fg, fu, fd, wide, *refs):
    outs, sem = refs[:9], refs[9]
    layers, d = fg.shape[0], fg.shape[1]
    rows, far = d // n, n // 2
    deep = far * rows
    copies = [(f.at[layer], out.at[layer]) for layer in range(layers) for f, out in zip((fg, fu, fd), outs)]
    for k, (i, layer) in enumerate((i, layer) for layer in (1, 0) for i in range(3)):
        for c in range(2):
            out = outs[3 + 3 * c + i]
            if i == 2:
                copies.append((wide.at[k, pl.ds(c * deep, deep), :], out.at[layer]))
            else:
                copies += [(wide.at[k, pl.ds(c * deep + b * rows, rows), :], out.at[layer, :, pl.ds(b * d, d)]) for b in range(far)]
    copies = [pltpu.make_async_copy(*pair, sem.at[i]) for i, pair in enumerate(copies)]
    for copy in copies:
        copy.start()
    for copy in copies:
        copy.wait()


def train_step(x, dy, w, m, v, n):
    wg, wu, wd = w
    tokens, d = x.shape[1:]
    layers, _, f = wg.shape
    nt, nc = tokens // TT, f // FC
    far, rows = n // 2, d // n
    pieces = 3 * layers
    parcels = pieces + 2 * 2 * EARLY
    hbm = pl.BlockSpec(memory_space=pl.ANY)
    vmem = pl.BlockSpec(memory_space=pltpu.VMEM)
    shape = jax.ShapeDtypeStruct
    kept = [pltpu.VMEM(one.shape, BF16) for one in w] + [pltpu.VMEM((nt, TT, d), F32)]
    v_, dma = pltpu.VMEM, pltpu.SemaphoreType.DMA
    scratch = [
        v_((2, 2 * FC, d), BF16), v_((2, d, FC), BF16),
        v_((nt, TT, d), BF16), v_((nt, d, TT), BF16), v_((nt, TT, d), BF16), v_((nt, TT, d), BF16), v_((nt, d, TT), BF16),
        v_((2 * nc, TT, LB), BF16), v_((TT, FC), BF16), v_((TT, FC), BF16), v_((TT, 2 * FC), BF16), v_((TT, 2 * FC), BF16),
        v_((UNITS_HELD, d, 2 * FC), F32), v_((UNITS_HELD, 2, d, LB), F32),
        v_((2, RECEIVED, far, 2, rows, FC), BF16), v_((2, 2, far, 2, rows, FC), BF16), v_((EARLY, 2, rows, FC), BF16),
        v_((layers, rows, f), BF16), v_((layers, rows, f), BF16), v_((layers, f // n, d), BF16), v_((8, LB), F32), v_((n, 8, LB), F32),
        dma((layers, 3)), dma((nt,)), dma((nt,)), dma((2,)), dma((2 * nc + 6,)), dma((nt,)),
        dma((2, RECEIVED, far)), dma((2, far)), dma((2, 2, far)), dma((2, far)), dma((n,)), dma((n,)),
        dma((pieces, n)), dma((2, far, parcels)), dma((2, far, parcels)),
        pltpu.SemaphoreType.REGULAR, dma((EARLY, 8)), dma((2, far, EARLY)), dma((2, far, EARLY)), dma((2, far, EARLY)), dma((2, far, EARLY)),
        dma((n - 1, EARLY, 2)),
    ]
    kept_bytes = 2 * sum(one.size for one in w) + 4 * tokens * d
    *new, wide, _, _, _, _ = pl.pallas_call(
        functools.partial(step_kernel, nt, nc, n, sum(one.size for one in w)),
        name="train_step",
        out_shape=kept + [shape((nc, nt, TT, 2 * FC), F32), shape((nt, d, TT), BF16),
                          shape((EARLY, n, d, LB), F32), shape((EARLY, n, 2, rows, FC), BF16)],
        in_specs=[hbm] * 11,
        out_specs=[vmem] * 4 + [hbm] * 4,
        scratch_shapes=scratch,
        compiler_params=pltpu.CompilerParams(vmem_limit_bytes=VMEM_BYTES - kept_bytes, collective_id=0, has_side_effects=True),
    )(x, dy, *w, *m, *v)
    copies = layers * (2 * (2 * far + 1) + 3)
    keep = lambda one: pltpu.with_memory_space_constraint(one, pltpu.VMEM)
    return tuple(pl.pallas_call(
        functools.partial(flush_kernel, n),
        name="flush",
        out_shape=[shape(one.shape, one.dtype) for group in (w, m, v) for one in group],
        in_specs=[vmem] * 4,
        out_specs=[hbm] * 9,
        scratch_shapes=[dma((copies,))],
        compiler_params=pltpu.CompilerParams(vmem_limit_bytes=1 << 20),
    )(*(keep(one) for one in (*new, wide))))


def solution(mesh):
    n = mesh.shape["dp"]

    def step(x, dy, *arrays):
        return train_step(x, dy, *(arrays[i:i + 3] for i in (0, 3, 6)), n)

    seq, rows = P(("rep", "dp"), None, None), P(None, "dp", None)
    return jax.shard_map(
        step,
        mesh=mesh,
        in_specs=(seq, seq) + (P(),) * 3 + (rows,) * 6,
        out_specs=(P("rep"),) * 3 + (P("rep", "dp"),) * 6,
        check_vma=False,
    )
```
